32 devices in a mesh: obs: 4 (over y, x), patch: 8 (over z, core).
Axes of the slice: x: 2, y: 2, z: 4, core: 2. Of those that a mesh axis runs over, the one named last changes fastest.
Arguments:
- green: float32 [5120, 5120], P('obs', 'patch'), may hold values from -0.078125 to 0.078125
- data: float32 [5120, 128], P('obs'), may hold values from -6 to 6
- neighbours: int32 [3, 5120], P(None, 'patch'), may hold values from 0 to 5119, as said below
- reg_weight: float32 [128], replicated, may hold values from 0.5 to 2
Outputs:
- slip: float32 [5120, 128], P('patch')
The draws below stay inside these ranges and needn't reach their ends.
Inputs may be any that keep to these rules, and one draw needn't show every extreme that they name: `neighbours`: entry (k, i) is a patch within 128 of i; an entry equal to i is padding. Distance 128 is reached in every draw.
All inputs are finite; a program needn't handle non-finite values.
Results may differ from the reference program's by a relative error of at most 0.0001.
Values sent between devices are 32-bit elements; how exact they have to be, the bound alone decides.
A program may use at most 64 MiB of HBM per device.

```python
import math
import jax
import jax.numpy as jnp
from jax import lax

EPOCHS = 128
BAND = 128
ITERS = 3
OBS = 5120
NPATCH = 5120


def draw_neighbours(key, part):
    key_offsets = jax.random.fold_in(key, 11)
    key_padding = jax.random.fold_in(key, 12)
    offsets = jax.random.randint(key_offsets, (3, NPATCH), -BAND, BAND + 1)
    padding = jax.random.randint(key_padding, (3, NPATCH), 0, 4) == 0
    offsets = jnp.where(padding, 0, offsets)
    indices = jnp.arange(NPATCH, dtype=jnp.int32)
    marked = indices % 37 == 5
    offsets = offsets.at[0].set(jnp.where(marked, -BAND, offsets[0]))
    offsets = offsets.at[1].set(jnp.where(marked, BAND, offsets[1]))
    return jnp.clip(indices[None, :] + offsets, 0, NPATCH - 1).astype(jnp.int32)


def level_of(key, extent, split, least, largest):
    level = 1.0
    for position, parts in split:
        draws = jax.random.uniform(jax.random.fold_in(jax.random.fold_in(key, 6), position), (parts,), jnp.float32, least / len(split), largest / len(split))
        level = level * jnp.repeat(jnp.exp(draws), extent[position] // parts).reshape((-1,) + (1,) * (len(extent) - 1 - position))
    return level


def gaussian(stream_key, dims, spread, most, shards=(), kind=jnp.bfloat16):
    loudness = level_of(stream_key, dims, shards, -0.22, 0.18) if shards else 1.0
    array = jax.random.normal(stream_key, dims, jnp.float32) * spread * loudness
    return jnp.minimum(jnp.maximum(array, -most), most).astype(kind)


def setup_inputs(seed: int = 0) -> dict:
    seeds = jax.random.split(jax.random.key(seed), 5)
    green = gaussian(seeds[0], (OBS, NPATCH), NPATCH ** -0.5, 0.078125, ((0, 4), (1, 8)), jnp.float32)
    data = gaussian(seeds[1], (OBS, EPOCHS), 1.0, 6.0, ((0, 4),), jnp.float32)
    neighbours = draw_neighbours(jax.random.fold_in(seeds[4], 71), 0)
    reg_weight = jnp.clip(jnp.exp(jax.random.uniform(seeds[3], (EPOCHS,), jnp.float32, math.log(0.5), math.log(2.0))), 0.5, 2.0)
    return {"green": green, "data": data, "neighbours": neighbours, "reg_weight": reg_weight}


def laplace(field, neighbours):
    return 4.0 * field - field[neighbours[0]] - field[neighbours[1]] - field[neighbours[2]]


def laplace_t(values, neighbours):
    result = 4.0 * values
    for slot in range(3):
        result = result.at[neighbours[slot]].add(-values)
    return result


def transposed(green, residual):
    return lax.dot_general(green, residual, (((0,), (0,)), ((), ())), precision=lax.Precision.HIGHEST, preferred_element_type=jnp.float32)


def reference(green, data, neighbours, reg_weight):
    slip = jnp.zeros((NPATCH, EPOCHS), jnp.float32)
    residual = data
    reg_resid = jnp.zeros((NPATCH, EPOCHS), jnp.float32)
    gradient = transposed(green, data)
    grad_norm = jnp.sum(gradient * gradient, axis=0)
    direction = gradient
    for iteration in range(ITERS):
        image = jnp.dot(green, direction, precision=lax.Precision.HIGHEST, preferred_element_type=jnp.float32)
        reg_image = reg_weight * laplace(direction, neighbours)
        curvature = jnp.sum(image * image, axis=0) + jnp.sum(reg_image * reg_image, axis=0)
        step_size = grad_norm / curvature
        slip = slip + step_size * direction
        if iteration + 1 < ITERS:
            residual = residual - step_size * image
            reg_resid = reg_resid - step_size * reg_image
            gradient = transposed(green, residual) + reg_weight * laplace_t(reg_resid, neighbours)
            next_norm = jnp.sum(gradient * gradient, axis=0)
            direction = gradient + (next_norm / grad_norm) * direction
            grad_norm = next_norm
    return slip
```

```python
import functools

import jax
import jax.numpy as jnp
from jax import lax
from jax.experimental import pallas as pl
from jax.experimental.pallas import tpu as pltpu
from jax.sharding import PartitionSpec as P

BAND = 128
ITERS = 3
MESH = pl.DeviceIdType.MESH
F32 = jnp.float32
BF16 = jnp.bfloat16
R = 64
LAG = 6


def dot(a, b):
    return lax.dot_general(a, b, (((1,), (0,)), ((), ())), preferred_element_type=F32)


def split(x):
    hi = x.astype(BF16)
    return hi, (x - hi.astype(F32)).astype(BF16)


def rowsum(x):
    return jnp.sum(x, axis=0, keepdims=True)


def kernel(n_obs, n_patch, nc, bc, green, data, nb, rw, out,
           gbuf, gpar, dbuf, ghi, glo, nbp, nbe, lm, lmt,
           cat_d, cat_e, cat_u, lt, lt0,
           d, g, a, wown, wsrc, slip, slp, dp, sq, hsrc, hd, hg, qd, qg,
           s, sr, sl, rl, rr, bb, br, nat, natp, hal, wr, scs, scr, pls, plr, tsrc, tdst,
           sem_l, sem_r, sem_b, sem_h, sem_w, sem_s, sem_p, sem_n, sem_x, sem_y, sem_g, sem_nb, sem_in):
    rows, cols = gbuf.shape
    E = dbuf.shape[1]
    H = E // 2
    CB = cols // BAND
    NB = 2 * CB
    RB = rows // (2 * BAND)
    nblk = rows // BAND
    per = BAND // R
    nz = n_patch // 2
    nbit = n_obs.bit_length() - 1
    obs = lax.axis_index("obs")
    pat = lax.axis_index("patch")
    z = pat // 2
    c = pat % 2
    other = 1 - c
    partner = z * 2 + other
    has_l, has_r = z > 0, z < nz - 1
    up, down = has_r, has_l
    n_plane = 2 * n_obs

    def lanes(n):
        return lax.broadcasted_iota(jnp.int32, (n, E), 1)

    def low(n):
        return lanes(n) < H

    def mine(n):
        i = lanes(n) - c * H
        return (i >= 0) & (i < H)

    def roll(x):
        return pltpu.roll(x, H, 1)

    def both(x):
        q = roll(x)
        m = low(x.shape[0])
        return jnp.where(m, x, q), jnp.where(m, q, x)

    def fold(x):
        return x + roll(x)

    def put_cat(ref, r0, v, third=False):
        n = v.shape[0]
        hi = v.astype(BF16)
        hf = hi.astype(F32)
        lf = v - hf
        m = low(n)
        ref[pl.ds(r0, n), 0:E] = jnp.where(m, hf, lf).astype(BF16)
        ref[pl.ds(r0, n), E:2 * E] = jnp.where(m, lf, hf).astype(BF16)
        if third:
            ref[pl.ds(r0, n), 2 * E:3 * E] = hi

    def rcopy(src, dst, sems, dev):
        return pltpu.make_async_remote_copy(
            src_ref=src, dst_ref=dst, send_sem=sems[0], recv_sem=sems[1],
            device_id=dev, device_id_type=MESH)

    def pair(sem, *idx):
        return sem.at[(0,) + idx], sem.at[(1,) + idx]

    def at(o, q):
        return (o, q)

    def plane(i):
        q = (obs * 2 + c + i) % n_plane
        return q // 2, z * 2 + q % 2

    def zpeer(i):
        return (z + i) % nz

    def load(i):
        r0 = pl.multiple_of(i * BAND, BAND)
        return pltpu.make_async_copy(green.at[pl.ds(r0, BAND)], gbuf.at[pl.ds(r0, BAND)], sem_in.at[i])

    load_data = pltpu.make_async_copy(data, dbuf, sem_in.at[nblk])
    load_data.start()

    @pl.loop(0, nblk)
    def _(i):
        load(i).start()

    barrier = pltpu.get_barrier_semaphore()

    @pl.loop(1, nz)
    def _(i):
        pl.semaphore_signal(barrier, inc=1, device_id=at(obs, zpeer(i) * 2 + c), device_id_type=MESH)

    @pl.loop(1, n_plane)
    def _(i):
        pl.semaphore_signal(barrier, inc=1, device_id=plane(i), device_id_type=MESH)

    wrow = rw[...]
    weight = jnp.where(mine(1), wrow, roll(wrow))

    scs[...] = jnp.zeros((ITERS, 8, E), F32)
    zero_c = jnp.zeros((nc, R, E), F32)
    zero_h = jnp.zeros((R, E), F32)
    zero_u = jnp.zeros((2 * BAND, 2 * E), BF16)
    cat_u[0:2 * BAND, :] = zero_u
    cat_u[(NB + 2) * BAND:(NB + 4) * BAND, :] = zero_u
    nbe[...] = jnp.full(nbe.shape, -(2 ** 24), jnp.int32)

    @pl.when(z == 0)
    def _():
        for it in range(ITERS):
            rl[it] = zero_c
            hal[it, 0] = zero_h
        for it in range(ITERS - 1):
            wr[it, 0] = zero_h

    @pl.when(z == nz - 1)
    def _():
        for it in range(ITERS):
            rr[it] = zero_c
            hal[it, 1] = zero_h
        for it in range(ITERS - 1):
            wr[it, 1] = zero_h

    load_data.wait()

    @pl.loop(0, nblk)
    def _(i):
        r0 = pl.multiple_of(i * BAND, BAND)
        hi, lo = split(dbuf[pl.ds(r0, BAND), :].T)
        lt0[0:E, pl.ds(r0, BAND)] = hi
        lt0[E:2 * E, pl.ds(r0, BAND)] = lo

    def put_green(src, i, core):
        r0 = pl.multiple_of(i * BAND, BAND)
        hi, lo = split(src[pl.ds(r0, BAND), :])
        for j in range(CB):
            c0 = pl.multiple_of((2 * j + core) * BAND, BAND)
            ghi[pl.ds(r0, BAND), pl.ds(c0, BAND)] = hi[:, j * BAND:(j + 1) * BAND]
            glo[pl.ds(r0, BAND), pl.ds(c0, BAND)] = lo[:, j * BAND:(j + 1) * BAND]

    @pl.loop(0, nblk)
    def _(i):
        load(i).wait()
        put_green(gbuf, i, c)

    pl.semaphore_wait(barrier, nz - 1 + n_plane - 1)

    ncopy = rcopy(nb, nbp, pair(sem_nb), at(obs, partner))
    ncopy.start()

    def gcopy(i):
        r0 = pl.multiple_of(i * BAND, BAND)
        return rcopy(gbuf.at[pl.ds(r0, BAND)], gpar.at[pl.ds(r0, BAND)], pair(sem_g, i), at(obs, partner))

    def build_laplace():
        ncopy.wait_recv()
        base = z * (2 * cols)
        own0 = pl.multiple_of((2 + c * CB) * BAND, BAND)
        par0 = pl.multiple_of((2 + other * CB) * BAND, BAND)
        nbe[0:3, pl.ds(own0, cols)] = nb[...] - base
        nbe[0:3, pl.ds(par0, cols)] = nbp[...] - base
        K = 3 * BAND

        @pl.loop(0, NB + 2)
        def _(j):
            r0 = pl.multiple_of(j * BAND, BAND)
            col = lax.broadcasted_iota(jnp.int32, (BAND, K), 0) + (j - 1) * BAND
            own = lax.broadcasted_iota(jnp.int32, (BAND, K), 1) + (j - 2) * BAND
            m = jnp.where(col == own, 4.0, 0.0)
            for k in range(3):
                m = m - jnp.where(col == nbe[k:k + 1, pl.ds(r0, K)], 1.0, 0.0)
            lmt[pl.ds(r0, BAND), :] = m.astype(BF16)

        @pl.loop(0, NB)
        def _(b):
            r0 = pl.multiple_of(b * BAND, BAND)
            n0 = pl.multiple_of((b + 2) * BAND, BAND)
            row = lax.broadcasted_iota(jnp.int32, (BAND, K), 0) + b * BAND
            col = lax.broadcasted_iota(jnp.int32, (BAND, K), 1) + (b - 1) * BAND
            m = jnp.where(col == row, 4.0, 0.0)
            t = nbe[0:8, pl.ds(n0, BAND)].T
            for k in range(3):
                m = m - jnp.where(col == t[:, k:k + 1], 1.0, 0.0)
            lm[pl.ds(r0, BAND), :] = m.astype(BF16)

    def bit_partner(p, j):
        b0, b1 = 1 << p, 1 << (nbit - 1 - p)
        bit = b0 + (j % 2) * (b1 - b0)
        return at(obs + bit * (1 - 2 * ((obs // bit) % 2)), pat)

    def bcopy(b, p, j):
        return rcopy(bb.at[b, p, j], br.at[b, p, j], pair(sem_b, b, p, j), bit_partner(p, j))

    def product(b, m):
        if b == 0:
            c0 = pl.multiple_of((2 * m + c) * BAND, BAND)
            y = dot(lt0[...], ghi[:, pl.ds(c0, BAND)])
            y = y[:E] + y[E:] + dot(lt0[0:E, :], glo[:, pl.ds(c0, BAND)])
            return y.T
        c0 = pl.multiple_of(m * 2 * BAND, 2 * BAND)
        y = dot(lt[...], ghi[:, pl.ds(c0, 2 * BAND)])
        y = y[:H] + y[H:] + dot(lt[0:H, :], glo[:, pl.ds(c0, 2 * BAND)])
        return jnp.concatenate([y[:, :BAND], y[:, BAND:]], axis=0).T

    def backward(b, hook, late, finish):
        @pl.loop(0, CB)
        def _(m):
            bb[b, 0, pl.ds(m * per, per)] = product(b, m).reshape(per, R, E)
            for k in range(per):
                bcopy(b, 0, m * per + k).start()

        hook()
        for p in range(1, nbit):
            @pl.loop(0, bc)
            def _(j):
                bcopy(b, p - 1, j).wait_recv()
                bb[b, p, j] = bb[b, p - 1, j] + br[b, p - 1, j]
                bcopy(b, p, j).start()

        late()

        @pl.loop(0, bc)
        def _(j):
            bcopy(b, nbit - 1, j).wait_recv()
            finish(j, bb[b, nbit - 1, j] + br[b, nbit - 1, j])

    def backward_sent(b):
        for p in range(nbit):
            @pl.loop(0, bc)
            def _(j):
                bcopy(b, p, j).wait_send()

    def rcopy_up(it, src, k):
        return rcopy(src.at[k], rl.at[it, k], pair(sem_l, it, k), at(obs, pat + 2))

    def rcopy_down(it, src, k):
        return rcopy(src.at[k], rr.at[it, k], pair(sem_r, it, k), at(obs, pat - 2))

    def hcopy_r(it):
        return rcopy(hsrc.at[it, 0], hal.at[it, 0], pair(sem_h, it, 0), at(obs, pat + 2))

    def hcopy_l(it):
        return rcopy(hsrc.at[it, 1], hal.at[it, 1], pair(sem_h, it, 1), at(obs, pat - 2))

    def put_lt(m):
        x = qd[pl.ds(m * per, per)].reshape(BAND, E)
        hi, lo = split(x.T)
        o0 = pl.multiple_of(m * 2 * BAND, 2 * BAND)
        o1 = pl.multiple_of(m * 2 * BAND + BAND, BAND)
        lt[0:H, pl.ds(o0, BAND)] = hi[:H]
        lt[H:E, pl.ds(o0, BAND)] = lo[:H]
        lt[0:H, pl.ds(o1, BAND)] = hi[H:]
        lt[H:E, pl.ds(o1, BAND)] = lo[H:]

    def forward(it, sums, hook):
        last = it == ITERS - 1
        v = a if it else g
        x = v[cols - BAND:cols, :]
        hsrc[it, 0] = jnp.where(low(R), roll(x[:R]), x[R:])
        x = v[0:BAND, :]
        hsrc[it, 1] = jnp.where(low(R), x[:R], roll(x[R:]))

        @pl.when(up & down)
        def _():
            hcopy_r(it).start()
            hcopy_l(it).start()

        @pl.loop(0, CB)
        def _(i):
            top, bot = both(v[pl.ds(pl.multiple_of(i * BAND, BAND), BAND), :])
            r0 = pl.multiple_of(i * 2 * BAND, 2 * BAND)
            put_cat(cat_d, r0, top, True)
            put_cat(cat_d, pl.multiple_of(r0 + BAND, BAND), bot, True)

        def group(m):
            r0 = pl.multiple_of(m * 2 * BAND, 2 * BAND)
            y = dot(ghi[pl.ds(r0, 2 * BAND), :], cat_d[:, 0:2 * E])
            y = y[:, :E] + y[:, E:] + dot(glo[pl.ds(r0, 2 * BAND), :], cat_d[:, 2 * E:3 * E])
            y = jnp.where(low(BAND), y[:BAND], y[BAND:])
            s[pl.ds(m * per, per)] = y.reshape(per, R, E)
            for k in range(per):
                @pl.when(z == 0)
                def _():
                    rcopy_up(it, s, m * per + k).start()

                @pl.when(z == nz - 1)
                def _():
                    rcopy_down(it, s, m * per + k).start()

        group(0)
        sums()

        @pl.when(up & (z == 0))
        def _():
            hcopy_r(it).start()

        @pl.when(down & (z == nz - 1))
        def _():
            hcopy_l(it).start()

        pl.loop(1, RB)(group)
        backward_sent(it)

        def chain(t, ends=True):
            kl = t - LAG * z
            kr = t - LAG * (nz - 1 - z)
            kt = t - LAG * jnp.maximum(z, nz - 1 - z)

            @pl.when(down & (kl >= 0) & (kl < nc))
            def _():
                rcopy_up(it, sr, kl).wait_recv()

                @pl.when(up)
                def _():
                    sr[kl] = rl[it, kl] + s[kl]
                    rcopy_up(it, sr, kl).start()

            @pl.when(up & (kr >= 0) & (kr < nc))
            def _():
                rcopy_down(it, sl, kr).wait_recv()

                @pl.when(down)
                def _():
                    sl[kr] = rr[it, kr] + s[kr]
                    rcopy_down(it, sl, kr).start()

            if not ends:
                return

            @pl.when((kt >= 0) & (kt < nc))
            def _():
                total = rl[it, kt] + s[kt] + rr[it, kt]
                if it:
                    step, ratio = scalars
                    rest = qg[kt] - step * total
                    total = rest + ratio * qd[kt]
                if last:
                    sq[...] += jnp.sum((total * total).reshape(R // 8, 8, E), axis=0)
                else:
                    qg[kt] = rest if it else total
                    qd[kt] = total

                    @pl.when(kt % per == per - 1)
                    def _():
                        put_lt(kt // per)

        if last:
            sq[...] = jnp.zeros((8, E), F32)
        pl.loop(LAG, LAG * (nz // 2))(functools.partial(chain, ends=False))
        scalars = hook()
        pl.loop(LAG * (nz // 2), nc + LAG * (nz - 1))(chain)

    def forward_sent(it):
        @pl.loop(0, nc)
        def _(k):
            @pl.when(up)
            def _():
                rcopy_up(it, sr, k).wait_send()

            @pl.when(down)
            def _():
                rcopy_down(it, sl, k).wait_send()

        @pl.when(up)
        def _():
            hcopy_r(it).wait_send()

        @pl.when(down)
        def _():
            hcopy_l(it).wait_send()

    def halo_wait(it):
        @pl.when(has_l)
        def _():
            hcopy_r(it).wait_recv()

        @pl.when(has_r)
        def _():
            hcopy_l(it).wait_recv()

    def widen(x):
        top, bot = both(x)
        return jnp.concatenate([top, bot], axis=0)

    def laplace():
        put_cat(cat_e, 0, widen(hd[0]))
        put_cat(cat_e, (NB + 1) * BAND, widen(hd[1]))

        @pl.loop(0, CB)
        def _(i):
            top, bot = both(d[pl.ds(pl.multiple_of(i * BAND, BAND), BAND), :])
            put_cat(cat_e, pl.multiple_of((i + 1) * BAND, BAND), top)
            put_cat(cat_e, pl.multiple_of((CB + i + 1) * BAND, BAND), bot)

    def banded(mat, vec, j):
        r0 = pl.multiple_of(j * BAND, BAND)
        y = dot(mat[pl.ds(r0, BAND), :], vec[pl.ds(r0, 3 * BAND), :])
        return y[:, :E] + y[:, E:]

    def lap_rows(i):
        return weight * jnp.where(low(BAND), banded(lm, cat_e, i), banded(lm, cat_e, CB + i))

    def wcopy_l(it):
        return rcopy(wsrc.at[it, 0], wr.at[it, 1], pair(sem_w, it, 1), at(obs, pat - 2))

    def wcopy_r(it):
        return rcopy(wsrc.at[it, 1], wr.at[it, 0], pair(sem_w, it, 0), at(obs, pat + 2))

    def reg_start(it):
        laplace()

        @pl.loop(0, CB)
        def _(i):
            top, bot = both(lap_rows(i))
            put_cat(cat_u, pl.multiple_of((i + 2) * BAND, BAND), top)
            put_cat(cat_u, pl.multiple_of((CB + i + 2) * BAND, BAND), bot)

        for side, j in ((0, 0), (1, NB + 1)):
            y = banded(lmt, cat_u, j)
            wsrc[it, side] = weight * jnp.where(low(R), y[:R], y[R:])

        @pl.when(has_l)
        def _():
            wcopy_l(it).start()

        @pl.when(has_r)
        def _():
            wcopy_r(it).start()

    def reg_own():
        @pl.loop(0, CB)
        def _(i):
            y = jnp.where(low(BAND), banded(lmt, cat_u, i + 1), banded(lmt, cat_u, CB + i + 1))
            wown[pl.ds(pl.multiple_of(i * BAND, BAND), BAND), :] = weight * y

    def reg_end(it):
        @pl.when(has_l)
        def _():
            wcopy_r(it).wait_recv()

        @pl.when(has_r)
        def _():
            wcopy_l(it).wait_recv()

        a[0:BAND, :] += jnp.where(low(BAND), widen(wr[it, 0]), 0.0)
        a[cols - BAND:cols, :] += jnp.where(low(BAND), 0.0, widen(wr[it, 1]))

    def reg_sent(it):
        @pl.when(has_l)
        def _():
            wcopy_l(it).wait_send()

        @pl.when(has_r)
        def _():
            wcopy_r(it).wait_send()

    def scopy(it, slot, q):
        return rcopy(scs.at[it], scr.at[it, slot], (sem_s.at[0, it, q], sem_s.at[1, it, slot]), at(obs, q * 2 + c))

    def sums_start(it):
        scr[it, z] = scs[it]

        @pl.loop(1, nz)
        def _(i):
            scopy(it, z, zpeer(i)).start()

    def sums_end(it):
        @pl.loop(1, nz)
        def _(i):
            scopy(it, zpeer(i), zpeer(i)).wait_recv()

        return fold(jnp.sum(scr[it], axis=0))

    def sums_sent(it):
        @pl.loop(1, nz)
        def _(i):
            scopy(it, z, zpeer(i)).wait_send()

    def pcopy(o, q, i):
        po, pp = plane(i)
        return rcopy(pls, plr.at[o, q], (sem_p.at[i], sem_n.at[o, q]), (po, pp))

    norms = []

    def dots(it):
        gv, dv, av = g[...], d[...], a[...]
        scs[it, 0:1, :] = rowsum(gv * gv)
        scs[it, 1:2, :] = rowsum(dv * av)
        scs[it, 2:3, :] = rowsum(gv * av)
        scs[it, 3:4, :] = rowsum(av * av)
        sums_start(it)

    def first():
        halo_wait(0)
        hg[...] = hal[0]
        hd[...] = hal[0]

    def ycopy(i):
        return rcopy((slip, d)[i], (slp, dp)[i], pair(sem_y, i), at(obs, partner))

    tcopy = rcopy(tsrc, tdst, pair(sem_y, 2), at(obs, partner))

    def advance(it):
        tot = sums_end(it - 1)
        if it == 1:
            norms.append(tot[0:1])
        norm = norms[-1]
        step = norm / tot[1:2]
        after = norm - 2.0 * step * tot[2:3] + step * step * tot[3:4]
        ratio = after / norm
        norms.append(after)
        halo_wait(it)
        if it == 1:
            slip[...] = step * d[...]
        else:
            slip[...] += step * d[...]
        g[...] = g[...] - step * a[...]
        d[...] = g[...] + ratio * d[...]
        hg[...] = hg[...] - step * hal[it]
        hd[...] = hg[...] + ratio * hd[...]
        if it == ITERS - 1:
            ycopy(0).start()
            ycopy(1).start()
            laplace()

            @pl.loop(0, CB)
            def _(i):
                u = lap_rows(i)
                scs[it] += jnp.sum((u * u).reshape(BAND // 8, 8, E), axis=0)

            sums_start(it)
        return step, ratio

    def xcopy(j):
        return rcopy(nat.at[j], natp.at[j], pair(sem_x, j), at(obs, partner))

    def first_hook():
        @pl.loop(0, nblk)
        def _(i):
            gcopy(i).start()

        build_laplace()

    def first_late():
        @pl.loop(0, nblk)
        def _(i):
            gcopy(i).wait_recv()
            put_green(gpar, i, other)

    def first_finish(j, x):
        nat[j] = x
        xcopy(j).start()

    backward(0, first_hook, first_late, first_finish)

    @pl.loop(0, bc)
    def _(j):
        xcopy(j).wait_recv()
        r0 = pl.multiple_of(j * R, R)
        x = jnp.where(mine(R), nat[j], roll(natp[j]))
        g[pl.ds(r0, R), :] = x
        d[pl.ds(r0, R), :] = x

    forward(0, lambda: None, first)
    for it in range(1, ITERS):
        def hook(it=it):
            forward_sent(it - 1)
            reg_start(it - 1)

        def finish(j, x):
            r0 = pl.multiple_of(j * R, R)
            a[pl.ds(r0, R), :] = x + wown[pl.ds(r0, R), :]

        backward(it, hook, reg_own, finish)
        reg_end(it - 1)
        forward(it, functools.partial(dots, it - 1), functools.partial(advance, it))

    last = ITERS - 1
    norm = norms[-1]
    pls[...] = sq[...]
    plr[obs, c] = sq[...]

    @pl.loop(1, n_plane)
    def _(i):
        pcopy(obs, c, i).start()

    @pl.loop(1, nz)
    def _(i):
        scopy(last, zpeer(i), zpeer(i)).wait_recv()

    tsrc[0:1, :] = norm
    tsrc[1:2, :] = fold(rowsum(jnp.sum(scr[last], axis=0)))
    tcopy.start()

    forward_sent(last)
    for it in range(ITERS):
        sums_sent(it)
    for it in range(ITERS - 1):
        reg_sent(it)
    ncopy.wait_send()

    @pl.loop(0, nblk)
    def _(i):
        gcopy(i).wait_send()

    @pl.loop(0, bc)
    def _(j):
        xcopy(j).wait_send()

    ycopy(0).wait_recv()
    ycopy(1).wait_recv()
    tcopy.wait_recv()

    @pl.loop(1, n_plane)
    def _(i):
        q = (obs * 2 + c + i) % n_plane
        pcopy(q // 2, q % 2, i).wait_recv()

    def step_of(t, q):
        return t[0:1, :] / (fold(rowsum(jnp.sum(plr[:, q], axis=0))) + t[1:2, :])

    step = jnp.where(mine(1), step_of(tsrc, c), step_of(tdst, other))

    @pl.loop(0, CB)
    def _(i):
        blk = pl.ds(pl.multiple_of(i * BAND, BAND), BAND)
        m = mine(BAND)
        out[blk, :] = jnp.where(m, slip[blk, :], roll(slp[blk, :])) + step * jnp.where(m, d[blk, :], roll(dp[blk, :]))

    ycopy(0).wait_send()
    ycopy(1).wait_send()
    tcopy.wait_send()

    @pl.loop(1, n_plane)
    def _(i):
        pcopy(obs, c, i).wait_send()


def shards(green, data, neighbours, reg_weight):
    rows, cols = green.shape
    E = data.shape[1]
    n_obs, n_patch = lax.axis_size("obs"), lax.axis_size("patch")
    nbit = n_obs.bit_length() - 1
    nz = n_patch // 2
    nc, bc = rows // 2 // R, cols // R
    NB = 2 * cols // BAND
    nblk = rows // BAND
    V = pltpu.VMEM
    D = pltpu.SemaphoreType.DMA
    scratch = [
        V((rows, cols), F32), V((rows, cols), F32), V((rows, E), F32),
        V((rows, 2 * cols), BF16), V((rows, 2 * cols), BF16),
        V(neighbours.shape, jnp.int32), V((8, (NB + 4) * BAND), jnp.int32),
        V((NB * BAND, 3 * BAND), BF16), V(((NB + 2) * BAND, 3 * BAND), BF16),
        V((2 * cols, 3 * E), BF16), V(((NB + 2) * BAND, 2 * E), BF16), V(((NB + 4) * BAND, 2 * E), BF16),
        V((E, rows), BF16), V((2 * E, rows), BF16),
        V((cols, E), F32), V((cols, E), F32), V((cols, E), F32), V((cols, E), F32), V((ITERS - 1, 2, R, E), F32),
        V((cols, E), F32), V((cols, E), F32), V((cols, E), F32), V((8, E), F32),
        V((ITERS, 2, R, E), F32), V((2, R, E), F32), V((2, R, E), F32), V((nc, R, E), F32), V((nc, R, E), F32),
        V((nc, R, E), F32), V((nc, R, E), F32), V((nc, R, E), F32),
        V((ITERS, nc, R, E), F32), V((ITERS, nc, R, E), F32),
        V((ITERS, nbit, bc, R, E), F32), V((ITERS, nbit, bc, R, E), F32),
        V((bc, R, E), F32), V((bc, R, E), F32),
        V((ITERS, 2, R, E), F32), V((ITERS - 1, 2, R, E), F32),
        V((ITERS, 8, E), F32), V((ITERS, nz, 8, E), F32),
        V((8, E), F32), V((n_obs, 2, 8, E), F32), V((8, E), F32), V((8, E), F32),
        D((2, ITERS, nc)), D((2, ITERS, nc)), D((2, ITERS, nbit, bc)), D((2, ITERS, 2)), D((2, ITERS - 1, 2)),
        D((2, ITERS, nz)), D((2 * n_obs,)), D((n_obs, 2)), D((2, bc)), D((2, 3)), D((2, nblk)), D((2,)),
        D((nblk + 1,)),
    ]
    return pl.pallas_call(
        functools.partial(kernel, n_obs, n_patch, nc, bc),
        out_shape=jax.ShapeDtypeStruct((cols, E), F32),
        in_specs=[pl.BlockSpec(memory_space=pl.ANY)] * 2 + [pl.BlockSpec(memory_space=pltpu.VMEM)] * 2,
        out_specs=pl.BlockSpec(memory_space=pltpu.VMEM),
        scratch_shapes=scratch,
        compiler_params=pltpu.CompilerParams(
            collective_id=0, has_side_effects=True, vmem_limit_bytes=56 * 1024 * 1024),
    )(green, data, neighbours, reg_weight.reshape(1, E))


def solution(mesh):
    in_specs = (P("obs", "patch"), P("obs", None), P(None, "patch"), P())
    return jax.shard_map(shards, mesh=mesh, in_specs=in_specs, out_specs=P("patch", None), check_vma=False)
```

```python
import functools

import jax
import jax.numpy as jnp
from jax import lax
from jax.experimental import pallas as pl
from jax.experimental.pallas import tpu as pltpu
from jax.sharding import PartitionSpec as P

BAND = 128
ITERS = 3
MESH = pl.DeviceIdType.MESH
F32 = jnp.float32
BF16 = jnp.bfloat16
R = 64
LAG = 6


def dot(a, b):
    return lax.dot_general(a, b, (((1,), (0,)), ((), ())), preferred_element_type=F32)


def split(x):
    hi = x.astype(BF16)
    return hi, (x - hi.astype(F32)).astype(BF16)


def rowsum(x):
    return jnp.sum(x, axis=0, keepdims=True)


def kernel(n_obs, n_patch, nc, bc, green, data, nb, rw, out,
           gbuf, gpar, dbuf, ghi, glo, nbp, nbe, lm, lmt,
           cat_d, cat_e, cat_u, lt, lt0,
           d, g, a, wown, wsrc, slip, slp, dp, sq, hsrc, hd, hg, qd, qg,
           s, sr, sl, rl, rr, bb, br, nat, natp, hal, wr, scs, scr, pls, plr, tsrc, tdst,
           sem_l, sem_r, sem_b, sem_h, sem_w, sem_s, sem_p, sem_n, sem_x, sem_y, sem_g, sem_nb, sem_in):
    rows, cols = gbuf.shape
    E = dbuf.shape[1]
    H = E // 2
    CB = cols // BAND
    NB = 2 * CB
    RB = rows // (2 * BAND)
    nblk = rows // BAND
    per = BAND // R
    nz = n_patch // 2
    nbit = n_obs.bit_length() - 1
    obs = lax.axis_index("obs")
    pat = lax.axis_index("patch")
    z = pat // 2
    c = pat % 2
    other = 1 - c
    partner = z * 2 + other
    has_l, has_r = z > 0, z < nz - 1
    up, down = has_r, has_l
    inner = up & down
    n_plane = 2 * n_obs

    def lanes(n):
        return lax.broadcasted_iota(jnp.int32, (n, E), 1)

    def low(n):
        return lanes(n) < H

    def mine(n):
        i = lanes(n) - c * H
        return (i >= 0) & (i < H)

    def roll(x):
        return pltpu.roll(x, H, 1)

    def both(x):
        q = roll(x)
        m = low(x.shape[0])
        return jnp.where(m, x, q), jnp.where(m, q, x)

    def fold(x):
        return x + roll(x)

    def put_cat(ref, r0, v, third=False):
        n = v.shape[0]
        hi = v.astype(BF16)
        hf = hi.astype(F32)
        lf = v - hf
        m = low(n)
        ref[pl.ds(r0, n), 0:E] = jnp.where(m, hf, lf).astype(BF16)
        ref[pl.ds(r0, n), E:2 * E] = jnp.where(m, lf, hf).astype(BF16)
        if third:
            ref[pl.ds(r0, n), 2 * E:3 * E] = hi

    def rcopy(src, dst, sems, dev):
        return pltpu.make_async_remote_copy(
            src_ref=src, dst_ref=dst, send_sem=sems[0], recv_sem=sems[1],
            device_id=dev, device_id_type=MESH)

    def pair(sem, *idx):
        return sem.at[(0,) + idx], sem.at[(1,) + idx]

    def at(o, q):
        return (o, q)

    def plane(i):
        q = (obs * 2 + c + i) % n_plane
        return q // 2, z * 2 + q % 2

    def zpeer(i):
        return (z + i) % nz

    def load(i):
        r0 = pl.multiple_of(i * BAND, BAND)
        return pltpu.make_async_copy(green.at[pl.ds(r0, BAND)], gbuf.at[pl.ds(r0, BAND)], sem_in.at[i])

    load_data = pltpu.make_async_copy(data, dbuf, sem_in.at[nblk])
    load_data.start()

    @pl.loop(0, nblk)
    def _(i):
        load(i).start()

    barrier = pltpu.get_barrier_semaphore()

    @pl.loop(1, nz)
    def _(i):
        pl.semaphore_signal(barrier, inc=1, device_id=at(obs, zpeer(i) * 2 + c), device_id_type=MESH)

    @pl.loop(1, n_plane)
    def _(i):
        pl.semaphore_signal(barrier, inc=1, device_id=plane(i), device_id_type=MESH)

    wrow = rw[...]
    weight = jnp.where(mine(1), wrow, roll(wrow))

    load_data.wait()

    for i in range(nblk):
        r0 = i * BAND
        hi, lo = split(dbuf[r0:r0 + BAND, :].T)
        lt0[0:E, r0:r0 + BAND] = hi
        lt0[E:2 * E, r0:r0 + BAND] = lo

    def put_green(src, i, core):
        r0 = pl.multiple_of(i * BAND, BAND)
        hi, lo = split(src[pl.ds(r0, BAND), :])
        for j in range(CB):
            c0 = pl.multiple_of((2 * j + core) * BAND, BAND)
            ghi[pl.ds(r0, BAND), pl.ds(c0, BAND)] = hi[:, j * BAND:(j + 1) * BAND]
            glo[pl.ds(r0, BAND), pl.ds(c0, BAND)] = lo[:, j * BAND:(j + 1) * BAND]

    @pl.loop(0, nblk)
    def _(i):
        load(i).wait()
        put_green(gbuf, i, c)

    pl.semaphore_wait(barrier, nz - 1 + n_plane - 1)

    ncopy = rcopy(nb, nbp, pair(sem_nb), at(obs, partner))
    ncopy.start()

    def gcopy(i):
        r0 = pl.multiple_of(i * BAND, BAND)
        return rcopy(gbuf.at[pl.ds(r0, BAND)], gpar.at[pl.ds(r0, BAND)], pair(sem_g, i), at(obs, partner))

    def build_laplace():
        ncopy.wait_recv()
        zero_u = jnp.zeros((2 * BAND, 2 * E), BF16)
        cat_u[0:2 * BAND, :] = zero_u
        cat_u[(NB + 2) * BAND:(NB + 4) * BAND, :] = zero_u
        nbe[...] = jnp.full(nbe.shape, -(2 ** 24), jnp.int32)
        base = z * (2 * cols)
        own0 = pl.multiple_of((2 + c * CB) * BAND, BAND)
        par0 = pl.multiple_of((2 + other * CB) * BAND, BAND)
        nbe[0:3, pl.ds(own0, cols)] = nb[...] - base
        nbe[0:3, pl.ds(par0, cols)] = nbp[...] - base
        K = 3 * BAND

        for j in range(NB + 2):
            r0 = j * BAND
            col = lax.broadcasted_iota(jnp.int32, (BAND, K), 0) + (j - 1) * BAND
            own = lax.broadcasted_iota(jnp.int32, (BAND, K), 1) + (j - 2) * BAND
            m = jnp.where(col == own, 4.0, 0.0)
            for k in range(3):
                m = m - jnp.where(col == nbe[k:k + 1, pl.ds(r0, K)], 1.0, 0.0)
            lmt[pl.ds(r0, BAND), :] = m.astype(BF16)

        for b in range(NB):
            r0, n0 = b * BAND, (b + 2) * BAND
            row = lax.broadcasted_iota(jnp.int32, (BAND, K), 0) + b * BAND
            col = lax.broadcasted_iota(jnp.int32, (BAND, K), 1) + (b - 1) * BAND
            m = jnp.where(col == row, 4.0, 0.0)
            t = nbe[0:8, pl.ds(n0, BAND)].T
            for k in range(3):
                m = m - jnp.where(col == t[:, k:k + 1], 1.0, 0.0)
            lm[pl.ds(r0, BAND), :] = m.astype(BF16)

    def clear():
        scs[...] = jnp.zeros((ITERS, 8, E), F32)
        zero_c = jnp.zeros((nc, R, E), F32)
        zero_h = jnp.zeros((R, E), F32)

        @pl.when(z == 0)
        def _():
            for it in range(ITERS):
                rl[it] = zero_c
                hal[it, 0] = zero_h
            for it in range(ITERS - 1):
                wr[it, 0] = zero_h

        @pl.when(z == nz - 1)
        def _():
            for it in range(ITERS):
                rr[it] = zero_c
                hal[it, 1] = zero_h
            for it in range(ITERS - 1):
                wr[it, 1] = zero_h

    def bit_partner(p, j):
        b0, b1 = 1 << p, 1 << (nbit - 1 - p)
        bit = b0 + (j % 2) * (b1 - b0)
        return at(obs + bit * (1 - 2 * ((obs // bit) % 2)), pat)

    def bcopy(b, p, j):
        return rcopy(bb.at[b, p, j], br.at[b, p, j], pair(sem_b, b, p, j), bit_partner(p, j))

    def product(b, m):
        if b == 0:
            c0 = pl.multiple_of((2 * m + c) * BAND, BAND)
            y = dot(lt0[...], ghi[:, pl.ds(c0, BAND)])
            y = y[:E] + y[E:] + dot(lt0[0:E, :], glo[:, pl.ds(c0, BAND)])
            return y.T
        c0 = pl.multiple_of(m * 2 * BAND, 2 * BAND)
        y = dot(lt[...], ghi[:, pl.ds(c0, 2 * BAND)])
        y = y[:H] + y[H:] + dot(lt[0:H, :], glo[:, pl.ds(c0, 2 * BAND)])
        return jnp.concatenate([y[:, :BAND], y[:, BAND:]], axis=0).T

    def backward(b, hook, late, finish):
        for m in range(CB):
            bb[b, 0, m * per:(m + 1) * per] = product(b, m).reshape(per, R, E)
            for k in range(per):
                bcopy(b, 0, m * per + k).start()

        hook()
        for p in range(1, nbit):
            @pl.loop(0, bc)
            def _(j):
                bcopy(b, p - 1, j).wait_recv()
                bb[b, p, j] = bb[b, p - 1, j] + br[b, p - 1, j]
                bcopy(b, p, j).start()

        late()

        @pl.loop(0, bc)
        def _(j):
            bcopy(b, nbit - 1, j).wait_recv()
            finish(j, bb[b, nbit - 1, j] + br[b, nbit - 1, j])

    def backward_sent(b):
        for p in range(nbit):
            @pl.loop(0, bc)
            def _(j):
                bcopy(b, p, j).wait_send()

    def rcopy_up(it, src, k):
        return rcopy(src.at[k], rl.at[it, k], pair(sem_l, it, k), at(obs, pat + 2))

    def rcopy_down(it, src, k):
        return rcopy(src.at[k], rr.at[it, k], pair(sem_r, it, k), at(obs, pat - 2))

    def hcopy_r(it):
        return rcopy(hsrc.at[it, 0], hal.at[it, 0], pair(sem_h, it, 0), at(obs, pat + 2))

    def hcopy_l(it):
        return rcopy(hsrc.at[it, 1], hal.at[it, 1], pair(sem_h, it, 1), at(obs, pat - 2))

    def put_lt(m):
        x = qd[pl.ds(m * per, per)].reshape(BAND, E)
        hi, lo = split(x.T)
        o0 = pl.multiple_of(m * 2 * BAND, 2 * BAND)
        o1 = pl.multiple_of(m * 2 * BAND + BAND, BAND)
        lt[0:H, pl.ds(o0, BAND)] = hi[:H]
        lt[H:E, pl.ds(o0, BAND)] = lo[:H]
        lt[0:H, pl.ds(o1, BAND)] = hi[H:]
        lt[H:E, pl.ds(o1, BAND)] = lo[H:]

    def forward(it, sums, after, hook):
        last = it == ITERS - 1
        v = a if it else g
        x = v[cols - BAND:cols, :]
        hsrc[it, 0] = jnp.where(low(R), roll(x[:R]), x[R:])
        x = v[0:BAND, :]
        hsrc[it, 1] = jnp.where(low(R), x[:R], roll(x[R:]))

        @pl.when(up & down)
        def _():
            hcopy_r(it).start()
            hcopy_l(it).start()

        def group(m):
            r0 = m * 2 * BAND
            y = dot(ghi[r0:r0 + 2 * BAND, :], cat_d[:, 0:2 * E])
            y = y[:, :E] + y[:, E:] + dot(glo[r0:r0 + 2 * BAND, :], cat_d[:, 2 * E:3 * E])
            y = jnp.where(low(BAND), y[:BAND], y[BAND:])
            s[m * per:(m + 1) * per] = y.reshape(per, R, E)
            for k in range(per):
                @pl.when(z == 0)
                def _():
                    rcopy_up(it, s, m * per + k).start()

                @pl.when(z == nz - 1)
                def _():
                    rcopy_down(it, s, m * per + k).start()

        group(0)
        sums()

        @pl.when(up & (z == 0))
        def _():
            hcopy_r(it).start()

        @pl.when(down & (z == nz - 1))
        def _():
            hcopy_l(it).start()

        for m in range(1, RB):
            group(m)
        after()
        backward_sent(it)

        def chain(t, ends=True):
            kl = t - LAG * z
            kr = t - LAG * (nz - 1 - z)
            kt = t - LAG * jnp.maximum(z, nz - 1 - z)

            @pl.when(down & (kl >= 0) & (kl < nc))
            def _():
                rcopy_up(it, sr, kl).wait_recv()

                @pl.when(up)
                def _():
                    sr[kl] = rl[it, kl] + s[kl]
                    rcopy_up(it, sr, kl).start()

            @pl.when(up & (kr >= 0) & (kr < nc))
            def _():
                rcopy_down(it, sl, kr).wait_recv()

                @pl.when(down)
                def _():
                    sl[kr] = rr[it, kr] + s[kr]
                    rcopy_down(it, sl, kr).start()

            if not ends:
                return

            @pl.when((kt >= 0) & (kt < nc))
            def _():
                total = rl[it, kt] + s[kt] + rr[it, kt]
                if it:
                    step, ratio = scalars
                    rest = qg[kt] - step * total
                    total = rest + ratio * qd[kt]
                if last:
                    sq[...] += jnp.sum((total * total).reshape(R // 8, 8, E), axis=0)
                else:
                    qg[kt] = rest if it else total
                    qd[kt] = total

                    @pl.when(kt % per == per - 1)
                    def _():
                        put_lt(kt // per)

        if last:
            sq[...] = jnp.zeros((8, E), F32)
        pl.loop(LAG, LAG * (nz // 2))(functools.partial(chain, ends=False))
        scalars = hook()

        @pl.when(jnp.logical_not(inner))
        def _():
            reg_sums() if last else reg_work(it)

        pl.loop(LAG * (nz // 2), nc + LAG * (nz - 1))(chain)
        if last:
            @pl.when(inner)
            def _():
                reg_sums()

    def forward_sent(it):
        @pl.loop(0, nc)
        def _(k):
            @pl.when(up)
            def _():
                rcopy_up(it, sr, k).wait_send()

            @pl.when(down)
            def _():
                rcopy_down(it, sl, k).wait_send()

        @pl.when(up)
        def _():
            hcopy_r(it).wait_send()

        @pl.when(down)
        def _():
            hcopy_l(it).wait_send()

    def halo_wait(it):
        @pl.when(has_l)
        def _():
            hcopy_r(it).wait_recv()

        @pl.when(has_r)
        def _():
            hcopy_l(it).wait_recv()

    def widen(x):
        top, bot = both(x)
        return jnp.concatenate([top, bot], axis=0)

    def laplace():
        put_cat(cat_e, 0, widen(hd[0]))
        put_cat(cat_e, (NB + 1) * BAND, widen(hd[1]))

        for i in range(CB):
            top, bot = both(d[i * BAND:(i + 1) * BAND, :])
            put_cat(cat_e, (i + 1) * BAND, top)
            put_cat(cat_e, (CB + i + 1) * BAND, bot)

    def banded(mat, vec, j):
        r0 = j * BAND
        y = dot(mat[r0:r0 + BAND, :], vec[r0:r0 + 3 * BAND, :])
        return y[:, :E] + y[:, E:]

    def lap_rows(i):
        return weight * jnp.where(low(BAND), banded(lm, cat_e, i), banded(lm, cat_e, CB + i))

    def wcopy_l(it):
        return rcopy(wsrc.at[it, 0], wr.at[it, 1], pair(sem_w, it, 1), at(obs, pat - 2))

    def wcopy_r(it):
        return rcopy(wsrc.at[it, 1], wr.at[it, 0], pair(sem_w, it, 0), at(obs, pat + 2))

    def reg_work(it):
        laplace()

        for i in range(CB):
            top, bot = both(lap_rows(i))
            put_cat(cat_u, (i + 2) * BAND, top)
            put_cat(cat_u, (CB + i + 2) * BAND, bot)

        for side, j in ((0, 0), (1, NB + 1)):
            y = banded(lmt, cat_u, j)
            wsrc[it, side] = weight * jnp.where(low(R), y[:R], y[R:])

        @pl.when(has_l)
        def _():
            wcopy_l(it).start()

        @pl.when(has_r)
        def _():
            wcopy_r(it).start()

        for i in range(CB):
            y = jnp.where(low(BAND), banded(lmt, cat_u, i + 1), banded(lmt, cat_u, CB + i + 1))
            wown[i * BAND:(i + 1) * BAND, :] = weight * y

    def reg_sums():
        last = ITERS - 1
        laplace()
        for i in range(CB):
            u = lap_rows(i)
            scs[last] += jnp.sum((u * u).reshape(BAND // 8, 8, E), axis=0)
        sums_start(last)

    def reg_end(it):
        @pl.when(has_l)
        def _():
            wcopy_r(it).wait_recv()

        @pl.when(has_r)
        def _():
            wcopy_l(it).wait_recv()

        wown[0:BAND, :] += jnp.where(low(BAND), widen(wr[it, 0]), 0.0)
        wown[cols - BAND:cols, :] += jnp.where(low(BAND), 0.0, widen(wr[it, 1]))

    def reg_sent(it):
        @pl.when(has_l)
        def _():
            wcopy_l(it).wait_send()

        @pl.when(has_r)
        def _():
            wcopy_r(it).wait_send()

    def scopy(it, slot, q):
        return rcopy(scs.at[it], scr.at[it, slot], (sem_s.at[0, it, q], sem_s.at[1, it, slot]), at(obs, q * 2 + c))

    def sums_start(it):
        scr[it, z] = scs[it]

        @pl.loop(1, nz)
        def _(i):
            scopy(it, z, zpeer(i)).start()

    def sums_end(it):
        @pl.loop(1, nz)
        def _(i):
            scopy(it, zpeer(i), zpeer(i)).wait_recv()

        return fold(jnp.sum(scr[it], axis=0))

    def sums_sent(it):
        @pl.loop(1, nz)
        def _(i):
            scopy(it, z, zpeer(i)).wait_send()

    def pcopy(o, q, i):
        po, pp = plane(i)
        return rcopy(pls, plr.at[o, q], (sem_p.at[i], sem_n.at[o, q]), (po, pp))

    norms = []

    def dots(it):
        gv, dv, av = g[...], d[...], a[...]
        scs[it, 0:1, :] = rowsum(gv * gv)
        scs[it, 1:2, :] = rowsum(dv * av)
        scs[it, 2:3, :] = rowsum(gv * av)
        scs[it, 3:4, :] = rowsum(av * av)
        sums_start(it)

    def first():
        halo_wait(0)
        hg[...] = hal[0]
        hd[...] = hal[0]

    def ycopy(i):
        return rcopy((slip, d)[i], (slp, dp)[i], pair(sem_y, i), at(obs, partner))

    tcopy = rcopy(tsrc, tdst, pair(sem_y, 2), at(obs, partner))

    def advance(it):
        tot = sums_end(it - 1)
        if it == 1:
            norms.append(tot[0:1])
        norm = norms[-1]
        step = norm / tot[1:2]
        after = norm - 2.0 * step * tot[2:3] + step * step * tot[3:4]
        ratio = after / norm
        norms.append(after)
        halo_wait(it)
        if it == 1:
            slip[...] = step * d[...]
        else:
            slip[...] += step * d[...]
        g[...] = g[...] - step * a[...]
        d[...] = g[...] + ratio * d[...]
        hg[...] = hg[...] - step * hal[it]
        hd[...] = hg[...] + ratio * hd[...]
        if it == ITERS - 1:
            ycopy(0).start()
            ycopy(1).start()
        return step, ratio

    def xcopy(j):
        return rcopy(nat.at[j], natp.at[j], pair(sem_x, j), at(obs, partner))

    def first_hook():
        @pl.loop(0, nblk)
        def _(i):
            gcopy(i).start()

        clear()

    def first_late():
        @pl.loop(0, nblk)
        def _(i):
            gcopy(i).wait_recv()
            put_green(gpar, i, other)

    def first_finish(j, x):
        nat[j] = x
        xcopy(j).start()

    def put_operand(ref, i):
        top, bot = both(ref[pl.ds(pl.multiple_of(i * BAND, BAND), BAND), :])
        r0 = pl.multiple_of(i * 2 * BAND, 2 * BAND)
        put_cat(cat_d, r0, top, True)
        put_cat(cat_d, pl.multiple_of(r0 + BAND, BAND), bot, True)

    backward(0, first_hook, first_late, first_finish)

    @pl.loop(0, bc)
    def _(j):
        xcopy(j).wait_recv()
        r0 = pl.multiple_of(j * R, R)
        x = jnp.where(mine(R), nat[j], roll(natp[j]))
        g[pl.ds(r0, R), :] = x
        d[pl.ds(r0, R), :] = x

        @pl.when(j % per == per - 1)
        def _():
            put_operand(g, j // per)

    pl.when(c == 0)(build_laplace)
    forward(0, lambda: None, lambda: pl.when(c == 1)(build_laplace), first)
    for it in range(1, ITERS):
        def hook(it=it):
            forward_sent(it - 1)

            @pl.when(inner)
            def _():
                reg_work(it - 1)

        def finish(j, x):
            r0 = pl.multiple_of(j * R, R)
            a[pl.ds(r0, R), :] = x + wown[pl.ds(r0, R), :]

            @pl.when(j % per == per - 1)
            def _():
                put_operand(a, j // per)

        backward(it, hook, functools.partial(reg_end, it - 1), finish)
        forward(it, functools.partial(dots, it - 1), lambda: None, functools.partial(advance, it))

    last = ITERS - 1
    norm = norms[-1]
    pls[...] = sq[...]
    plr[obs, c] = sq[...]

    @pl.loop(1, n_plane)
    def _(i):
        pcopy(obs, c, i).start()

    @pl.loop(1, nz)
    def _(i):
        scopy(last, zpeer(i), zpeer(i)).wait_recv()

    tsrc[0:1, :] = norm
    tsrc[1:2, :] = fold(rowsum(jnp.sum(scr[last], axis=0)))
    tcopy.start()

    forward_sent(last)
    for it in range(ITERS):
        sums_sent(it)
    for it in range(ITERS - 1):
        reg_sent(it)
    ncopy.wait_send()

    @pl.loop(0, nblk)
    def _(i):
        gcopy(i).wait_send()

    @pl.loop(0, bc)
    def _(j):
        xcopy(j).wait_send()

    ycopy(0).wait_recv()
    ycopy(1).wait_recv()
    ycopy(0).wait_send()
    ycopy(1).wait_send()
    for i in range(CB):
        blk = slice(i * BAND, (i + 1) * BAND)
        m = mine(BAND)
        slip[blk, :] = jnp.where(m, slip[blk, :], roll(slp[blk, :]))
        d[blk, :] = jnp.where(m, d[blk, :], roll(dp[blk, :]))
    tcopy.wait_recv()
    tcopy.wait_send()

    @pl.loop(1, n_plane)
    def _(i):
        q = (obs * 2 + c + i) % n_plane
        pcopy(q // 2, q % 2, i).wait_recv()

    def step_of(t, q):
        return t[0:1, :] / (fold(rowsum(jnp.sum(plr[:, q], axis=0))) + t[1:2, :])

    step = jnp.where(mine(1), step_of(tsrc, c), step_of(tdst, other))

    out[...] = slip[...] + step * d[...]

    @pl.loop(1, n_plane)
    def _(i):
        pcopy(obs, c, i).wait_send()


def shards(green, data, neighbours, reg_weight):
    rows, cols = green.shape
    E = data.shape[1]
    n_obs, n_patch = lax.axis_size("obs"), lax.axis_size("patch")
    nbit = n_obs.bit_length() - 1
    nz = n_patch // 2
    nc, bc = rows // 2 // R, cols // R
    NB = 2 * cols // BAND
    nblk = rows // BAND
    V = pltpu.VMEM
    D = pltpu.SemaphoreType.DMA
    scratch = [
        V((rows, cols), F32), V((rows, cols), F32), V((rows, E), F32),
        V((rows, 2 * cols), BF16), V((rows, 2 * cols), BF16),
        V(neighbours.shape, jnp.int32), V((8, (NB + 4) * BAND), jnp.int32),
        V((NB * BAND, 3 * BAND), BF16), V(((NB + 2) * BAND, 3 * BAND), BF16),
        V((2 * cols, 3 * E), BF16), V(((NB + 2) * BAND, 2 * E), BF16), V(((NB + 4) * BAND, 2 * E), BF16),
        V((E, rows), BF16), V((2 * E, rows), BF16),
        V((cols, E), F32), V((cols, E), F32), V((cols, E), F32), V((cols, E), F32), V((ITERS - 1, 2, R, E), F32),
        V((cols, E), F32), V((cols, E), F32), V((cols, E), F32), V((8, E), F32),
        V((ITERS, 2, R, E), F32), V((2, R, E), F32), V((2, R, E), F32), V((nc, R, E), F32), V((nc, R, E), F32),
        V((nc, R, E), F32), V((nc, R, E), F32), V((nc, R, E), F32),
        V((ITERS, nc, R, E), F32), V((ITERS, nc, R, E), F32),
        V((ITERS, nbit, bc, R, E), F32), V((ITERS, nbit, bc, R, E), F32),
        V((bc, R, E), F32), V((bc, R, E), F32),
        V((ITERS, 2, R, E), F32), V((ITERS - 1, 2, R, E), F32),
        V((ITERS, 8, E), F32), V((ITERS, nz, 8, E), F32),
        V((8, E), F32), V((n_obs, 2, 8, E), F32), V((8, E), F32), V((8, E), F32),
        D((2, ITERS, nc)), D((2, ITERS, nc)), D((2, ITERS, nbit, bc)), D((2, ITERS, 2)), D((2, ITERS - 1, 2)),
        D((2, ITERS, nz)), D((2 * n_obs,)), D((n_obs, 2)), D((2, bc)), D((2, 3)), D((2, nblk)), D((2,)),
        D((nblk + 1,)),
    ]
    return pl.pallas_call(
        functools.partial(kernel, n_obs, n_patch, nc, bc),
        out_shape=jax.ShapeDtypeStruct((cols, E), F32),
        in_specs=[pl.BlockSpec(memory_space=pl.ANY)] * 2 + [pl.BlockSpec(memory_space=pltpu.VMEM)] * 2,
        out_specs=pl.BlockSpec(memory_space=pltpu.VMEM),
        scratch_shapes=scratch,
        compiler_params=pltpu.CompilerParams(
            collective_id=0, has_side_effects=True, vmem_limit_bytes=56 * 1024 * 1024),
    )(green, data, neighbours, reg_weight.reshape(1, E))


def solution(mesh):
    in_specs = (P("obs", "patch"), P("obs", None), P(None, "patch"), P())
    return jax.shard_map(shards, mesh=mesh, in_specs=in_specs, out_specs=P("patch", None), check_vma=False)
```

```python
import functools

import jax
import jax.numpy as jnp
from jax import lax
from jax.experimental import pallas as pl
from jax.experimental.pallas import tpu as pltpu
from jax.sharding import PartitionSpec as P

BAND = 128
ITERS = 3
MESH = pl.DeviceIdType.MESH
F32 = jnp.float32
BF16 = jnp.bfloat16
R = 64
LAG = 8


def dot(a, b):
    return lax.dot_general(a, b, (((1,), (0,)), ((), ())), preferred_element_type=F32)


def split(x):
    hi = x.astype(BF16)
    return hi, (x - hi.astype(F32)).astype(BF16)


def rowsum(x):
    return jnp.sum(x, axis=0, keepdims=True)


def kernel(n_obs, n_patch, nc, bc, green, data, nb_in, rw_in, out,
           gbuf, gpar, dbuf, ghi, glo, nb, nbp, nbe, rw, lm, lmt,
           cat_d, cat_e, cat_u, lt, lt0,
           d, g, a, wown, wsrc, slip, slp, dp, sq, hsrc, hd, hg, qd, qg,
           s, sr, sl, rl, rr, bb, br, nat, natp, hal, wr, scs, scr, pls, plr, tsrc, tdst,
           sem_out, sem_l, sem_r, sem_b, sem_h, sem_w, sem_s, sem_p, sem_x, sem_y, sem_g, sem_nb, sem_in):
    rows, cols = gbuf.shape
    E = dbuf.shape[1]
    H = E // 2
    CB = cols // BAND
    NB = 2 * CB
    RB = rows // (2 * BAND)
    nblk = rows // BAND
    per = BAND // R
    nz = n_patch // 2
    nbit = n_obs.bit_length() - 1
    obs = lax.axis_index("obs")
    pat = lax.axis_index("patch")
    z = pat // 2
    c = pat % 2
    other = 1 - c
    partner = z * 2 + other
    has_l, has_r = z > 0, z < nz - 1
    up, down = has_r, has_l
    inner = up & down
    n_plane = 2 * n_obs

    def lanes(n):
        return lax.broadcasted_iota(jnp.int32, (n, E), 1)

    def low(n):
        return lanes(n) < H

    def mine(n):
        i = lanes(n) - c * H
        return (i >= 0) & (i < H)

    def roll(x):
        return pltpu.roll(x, H, 1)

    def both(x):
        q = roll(x)
        m = low(x.shape[0])
        return jnp.where(m, x, q), jnp.where(m, q, x)

    def fold(x):
        return x + roll(x)

    def put_cat(ref, r0, v, third=False):
        n = v.shape[0]
        hi = v.astype(BF16)
        hf = hi.astype(F32)
        lf = v - hf
        m = low(n)
        ref[pl.ds(r0, n), 0:E] = jnp.where(m, hf, lf).astype(BF16)
        ref[pl.ds(r0, n), E:2 * E] = jnp.where(m, lf, hf).astype(BF16)
        if third:
            ref[pl.ds(r0, n), 2 * E:3 * E] = hi

    def rcopy(src, dst, sems, dev):
        return pltpu.make_async_remote_copy(
            src_ref=src, dst_ref=dst, send_sem=sems[0], recv_sem=sems[1],
            device_id=dev, device_id_type=MESH)

    def pair(sem, *idx):
        return sem.at[(0,) + idx], sem.at[(1,) + idx]

    def at(o, q):
        return (o, q)

    def plane(i):
        q = (obs * 2 + c + i) % n_plane
        return q // 2, z * 2 + q % 2

    def zpeer(i):
        return (z + i) % nz

    def load(i):
        rs = pl.ds(pl.multiple_of(i * 2 * BAND, 2 * BAND), 2 * BAND)
        return pltpu.make_async_copy(green.at[rs], gbuf.at[rs], sem_in.at[i])

    load_data = pltpu.make_async_copy(data, dbuf, sem_in.at[RB])
    load_nb = pltpu.make_async_copy(nb_in, nb, sem_in.at[RB + 1])
    load_rw = pltpu.make_async_copy(rw_in, rw, sem_in.at[RB + 2])
    load_data.start()

    @pl.loop(0, RB)
    def _(i):
        load(i).start()

    load_nb.start()
    load_rw.start()

    barrier = pltpu.get_barrier_semaphore()

    @pl.loop(1, nz)
    def _(i):
        pl.semaphore_signal(barrier, inc=1, device_id=at(obs, zpeer(i) * 2 + c), device_id_type=MESH)

    @pl.loop(1, n_plane)
    def _(i):
        pl.semaphore_signal(barrier, inc=1, device_id=plane(i), device_id_type=MESH)

    load_data.wait()

    for i in range(nblk):
        r0 = i * BAND
        hi, lo = split(dbuf[r0:r0 + BAND, :].T)
        lt0[0:E, r0:r0 + BAND] = hi
        lt0[E:2 * E, r0:r0 + BAND] = lo

    def put_green(src, i, core):
        r0 = pl.multiple_of(i * BAND, BAND)
        hi, lo = split(src[pl.ds(r0, BAND), :])
        for j in range(CB):
            c0 = pl.multiple_of((2 * j + core) * BAND, BAND)
            ghi[pl.ds(r0, BAND), pl.ds(c0, BAND)] = hi[:, j * BAND:(j + 1) * BAND]
            glo[pl.ds(r0, BAND), pl.ds(c0, BAND)] = lo[:, j * BAND:(j + 1) * BAND]

    @pl.loop(0, RB)
    def _(i):
        load(i).wait()
        put_green(gbuf, 2 * i, c)
        put_green(gbuf, 2 * i + 1, c)

    load_nb.wait()
    load_rw.wait()
    wrow = rw[...]
    weight = jnp.where(mine(1), wrow, roll(wrow))

    pl.semaphore_wait(barrier, nz - 1 + n_plane - 1)

    ncopy = rcopy(nb, nbp, (sem_nb.at[0], sem_nb.at[1]), at(obs, partner))
    ncopy.start()

    def gcopy(i):
        rs = pl.ds(i * (rows // 2), rows // 2)
        return rcopy(gbuf.at[rs], gpar.at[rs], (sem_out.at[3], sem_g.at[i]), at(obs, partner))

    def build_laplace():
        ncopy.wait_recv()
        zero_u = jnp.zeros((2 * BAND, 2 * E), BF16)
        cat_u[0:2 * BAND, :] = zero_u
        cat_u[(NB + 2) * BAND:(NB + 4) * BAND, :] = zero_u
        nbe[...] = jnp.full(nbe.shape, -(2 ** 24), jnp.int32)
        base = z * (2 * cols)
        own0 = pl.multiple_of((2 + c * CB) * BAND, BAND)
        par0 = pl.multiple_of((2 + other * CB) * BAND, BAND)
        nbe[0:3, pl.ds(own0, cols)] = nb[...] - base
        nbe[0:3, pl.ds(par0, cols)] = nbp[...] - base
        K = 3 * BAND

        for j in range(NB + 2):
            r0 = j * BAND
            col = lax.broadcasted_iota(jnp.int32, (BAND, K), 0) + (j - 1) * BAND
            own = lax.broadcasted_iota(jnp.int32, (BAND, K), 1) + (j - 2) * BAND
            m = jnp.where(col == own, 4.0, 0.0)
            for k in range(3):
                m = m - jnp.where(col == nbe[k:k + 1, pl.ds(r0, K)], 1.0, 0.0)
            lmt[pl.ds(r0, BAND), :] = m.astype(BF16)

        for b in range(NB):
            r0, n0 = b * BAND, (b + 2) * BAND
            row = lax.broadcasted_iota(jnp.int32, (BAND, K), 0) + b * BAND
            col = lax.broadcasted_iota(jnp.int32, (BAND, K), 1) + (b - 1) * BAND
            m = jnp.where(col == row, 4.0, 0.0)
            t = nbe[0:8, pl.ds(n0, BAND)].T
            for k in range(3):
                m = m - jnp.where(col == t[:, k:k + 1], 1.0, 0.0)
            lm[pl.ds(r0, BAND), :] = m.astype(BF16)

    def clear():
        scs[...] = jnp.zeros((ITERS, 8, E), F32)
        zero_c = jnp.zeros((nc, R, E), F32)
        zero_h = jnp.zeros((R, E), F32)

        @pl.when(z == 0)
        def _():
            for it in range(ITERS):
                rl[it] = zero_c
                hal[it, 0] = zero_h
            for it in range(ITERS - 1):
                wr[it, 0] = zero_h

        @pl.when(z == nz - 1)
        def _():
            for it in range(ITERS):
                rr[it] = zero_c
                hal[it, 1] = zero_h
            for it in range(ITERS - 1):
                wr[it, 1] = zero_h

    def bit_partner(p, j):
        b0, b1 = 1 << p, 1 << (nbit - 1 - p)
        bit = b0 + (j % 2) * (b1 - b0)
        return at(obs + bit * (1 - 2 * ((obs // bit) % 2)), pat)

    def bcopy(b, p, j):
        return rcopy(bb.at[b, p, j], br.at[b, p, j], (sem_out.at[2], sem_b.at[b % 2, p, j]), bit_partner(p, j))

    def product(b, m):
        if b == 0:
            c0 = pl.multiple_of((2 * m + c) * BAND, BAND)
            y = dot(lt0[...], ghi[:, pl.ds(c0, BAND)])
            y = y[:E] + y[E:] + dot(lt0[0:E, :], glo[:, pl.ds(c0, BAND)])
            return y.T
        c0 = pl.multiple_of(m * 2 * BAND, 2 * BAND)
        y = dot(lt[...], ghi[:, pl.ds(c0, 2 * BAND)])
        y = y[:H] + y[H:] + dot(lt[0:H, :], glo[:, pl.ds(c0, 2 * BAND)])
        return jnp.concatenate([y[:, :BAND], y[:, BAND:]], axis=0).T

    def backward(b, hook, late, finish):
        for m in range(CB):
            bb[b, 0, m * per:(m + 1) * per] = product(b, m).reshape(per, R, E)
            for k in range(per):
                bcopy(b, 0, m * per + k).start()

        hook()
        for p in range(1, nbit):
            @pl.loop(0, bc)
            def _(j):
                bcopy(b, p - 1, j).wait_recv()
                bb[b, p, j] = bb[b, p - 1, j] + br[b, p - 1, j]
                bcopy(b, p, j).start()

        late()

        @pl.loop(0, bc)
        def _(j):
            bcopy(b, nbit - 1, j).wait_recv()
            finish(j, bb[b, nbit - 1, j] + br[b, nbit - 1, j])

    def backward_sent(b):
        rcopy(bb.at[b], br.at[b], (sem_out.at[2], sem_b.at[0, 0, 0]), at(obs, partner)).wait_send()

    def rcopy_up(it, src, k):
        return rcopy(src.at[k], rl.at[it, k], (sem_out.at[0], sem_l.at[it % 2, k]), at(obs, pat + 2))

    def rcopy_down(it, src, k):
        return rcopy(src.at[k], rr.at[it, k], (sem_out.at[1], sem_r.at[it % 2, k]), at(obs, pat - 2))

    def hcopy_r(it):
        return rcopy(hsrc.at[it, 0], hal.at[it, 0], (sem_out.at[4], sem_h.at[it % 2, 0]), at(obs, pat + 2))

    def hcopy_l(it):
        return rcopy(hsrc.at[it, 1], hal.at[it, 1], (sem_out.at[5], sem_h.at[it % 2, 1]), at(obs, pat - 2))

    def put_lt(m):
        x = qd[pl.ds(m * per, per)].reshape(BAND, E)
        hi, lo = split(x.T)
        o0 = pl.multiple_of(m * 2 * BAND, 2 * BAND)
        o1 = pl.multiple_of(m * 2 * BAND + BAND, BAND)
        lt[0:H, pl.ds(o0, BAND)] = hi[:H]
        lt[H:E, pl.ds(o0, BAND)] = lo[:H]
        lt[0:H, pl.ds(o1, BAND)] = hi[H:]
        lt[H:E, pl.ds(o1, BAND)] = lo[H:]

    def forward(it, sums, after, hook):
        last = it == ITERS - 1
        v = a if it else g
        x = v[cols - BAND:cols, :]
        hsrc[it, 0] = jnp.where(low(R), roll(x[:R]), x[R:])
        x = v[0:BAND, :]
        hsrc[it, 1] = jnp.where(low(R), x[:R], roll(x[R:]))

        @pl.when(up & down)
        def _():
            hcopy_r(it).start()
            hcopy_l(it).start()

        def group(m):
            r0 = m * 2 * BAND
            y = dot(ghi[r0:r0 + 2 * BAND, :], cat_d[:, 0:2 * E])
            y = y[:, :E] + y[:, E:] + dot(glo[r0:r0 + 2 * BAND, :], cat_d[:, 2 * E:3 * E])
            y = jnp.where(low(BAND), y[:BAND], y[BAND:])
            s[m * per:(m + 1) * per] = y.reshape(per, R, E)
            for k in range(per):
                @pl.when(z == 0)
                def _():
                    rcopy_up(it, s, m * per + k).start()

                @pl.when(z == nz - 1)
                def _():
                    rcopy_down(it, s, m * per + k).start()

        group(0)
        sums()

        @pl.when(up & (z == 0))
        def _():
            hcopy_r(it).start()

        @pl.when(down & (z == nz - 1))
        def _():
            hcopy_l(it).start()

        for m in range(1, RB):
            group(m)
        after()
        backward_sent(it)

        def chain(t, ends=True):
            kl = t - LAG * z
            kr = t - LAG * (nz - 1 - z)
            kt = t - LAG * jnp.maximum(z, nz - 1 - z)

            @pl.when(down & (kl >= 0) & (kl < nc))
            def _():
                rcopy_up(it, sr, kl).wait_recv()

                @pl.when(up)
                def _():
                    sr[kl] = rl[it, kl] + s[kl]
                    rcopy_up(it, sr, kl).start()

            @pl.when(up & (kr >= 0) & (kr < nc))
            def _():
                rcopy_down(it, sl, kr).wait_recv()

                @pl.when(down)
                def _():
                    sl[kr] = rr[it, kr] + s[kr]
                    rcopy_down(it, sl, kr).start()

            if not ends:
                return

            @pl.when((kt >= 0) & (kt < nc))
            def _():
                total = rl[it, kt] + s[kt] + rr[it, kt]
                if it:
                    step, ratio = scalars
                    rest = qg[kt] - step * total
                    total = rest + ratio * qd[kt]
                if last:
                    sq[...] += jnp.sum((total * total).reshape(R // 8, 8, E), axis=0)
                else:
                    qg[kt] = rest if it else total
                    qd[kt] = total

                    @pl.when(kt % per == per - 1)
                    def _():
                        put_lt(kt // per)

        if last:
            sq[...] = jnp.zeros((8, E), F32)
        pl.loop(LAG, LAG * (nz // 2))(functools.partial(chain, ends=False))
        scalars = hook()

        @pl.when(jnp.logical_not(inner))
        def _():
            reg_sums() if last else reg_work(it)

        pl.loop(LAG * (nz // 2), nc + LAG * (nz - 1))(chain)
        if last:
            @pl.when(inner)
            def _():
                reg_sums()

    def forward_sent(it):
        @pl.when(up)
        def _():
            rcopy(sr, rl.at[it], (sem_out.at[0], sem_l.at[0, 0]), at(obs, partner)).wait_send()

        @pl.when(down)
        def _():
            rcopy(sl, rr.at[it], (sem_out.at[1], sem_r.at[0, 0]), at(obs, partner)).wait_send()

        @pl.when(up)
        def _():
            hcopy_r(it).wait_send()

        @pl.when(down)
        def _():
            hcopy_l(it).wait_send()

    def halo_wait(it):
        @pl.when(has_l)
        def _():
            hcopy_r(it).wait_recv()

        @pl.when(has_r)
        def _():
            hcopy_l(it).wait_recv()

    def widen(x):
        top, bot = both(x)
        return jnp.concatenate([top, bot], axis=0)

    def laplace():
        put_cat(cat_e, 0, widen(hd[0]))
        put_cat(cat_e, (NB + 1) * BAND, widen(hd[1]))

        for i in range(CB):
            top, bot = both(d[i * BAND:(i + 1) * BAND, :])
            put_cat(cat_e, (i + 1) * BAND, top)
            put_cat(cat_e, (CB + i + 1) * BAND, bot)

    def banded(mat, vec, j):
        r0 = j * BAND
        y = dot(mat[r0:r0 + BAND, :], vec[r0:r0 + 3 * BAND, :])
        return y[:, :E] + y[:, E:]

    def lap_rows(i):
        return weight * jnp.where(low(BAND), banded(lm, cat_e, i), banded(lm, cat_e, CB + i))

    def wcopy_l(it):
        return rcopy(wsrc.at[it, 0], wr.at[it, 1], (sem_out.at[7], sem_w.at[it, 1]), at(obs, pat - 2))

    def wcopy_r(it):
        return rcopy(wsrc.at[it, 1], wr.at[it, 0], (sem_out.at[6], sem_w.at[it, 0]), at(obs, pat + 2))

    def reg_work(it):
        laplace()

        for i in range(CB):
            top, bot = both(lap_rows(i))
            put_cat(cat_u, (i + 2) * BAND, top)
            put_cat(cat_u, (CB + i + 2) * BAND, bot)

        for side, j in ((0, 0), (1, NB + 1)):
            y = banded(lmt, cat_u, j)
            wsrc[it, side] = weight * jnp.where(low(R), y[:R], y[R:])

        @pl.when(has_l)
        def _():
            wcopy_l(it).start()

        @pl.when(has_r)
        def _():
            wcopy_r(it).start()

        for i in range(CB):
            y = jnp.where(low(BAND), banded(lmt, cat_u, i + 1), banded(lmt, cat_u, CB + i + 1))
            wown[i * BAND:(i + 1) * BAND, :] = weight * y

    def reg_sums():
        last = ITERS - 1
        laplace()
        for i in range(CB):
            u = lap_rows(i)
            scs[last] += jnp.sum((u * u).reshape(BAND // 8, 8, E), axis=0)
        sums_start(last)

    def reg_end(it):
        @pl.when(has_l)
        def _():
            wcopy_r(it).wait_recv()

        @pl.when(has_r)
        def _():
            wcopy_l(it).wait_recv()

        wown[0:BAND, :] += jnp.where(low(BAND), widen(wr[it, 0]), 0.0)
        wown[cols - BAND:cols, :] += jnp.where(low(BAND), 0.0, widen(wr[it, 1]))
        reg_sent(it)

    def reg_sent(it):
        @pl.when(has_l)
        def _():
            wcopy_l(it).wait_send()

        @pl.when(has_r)
        def _():
            wcopy_r(it).wait_send()

    def scopy(it, q):
        return rcopy(scs.at[it], scr.at[it, z], (sem_out.at[8], sem_s.at[it]), at(obs, q * 2 + c))

    def sums_all(it):
        part = scr.at[it, pl.ds(0, nz - 1)]
        return rcopy(part, part, (sem_out.at[8], sem_s.at[it]), at(obs, partner))

    def sums_start(it):
        scr[it, z] = scs[it]

        @pl.loop(1, nz)
        def _(i):
            scopy(it, zpeer(i)).start()

    def sums_end(it):
        sums_all(it).wait_recv()
        sums_all(it).wait_send()
        return fold(jnp.sum(scr[it], axis=0))

    def pcopy(i):
        po, pp = plane(i)
        return rcopy(pls, plr.at[obs * 2 + c], (sem_p.at[0], sem_p.at[1]), (po, pp))

    norms = []

    def dots(it):
        gv, dv, av = g[...], d[...], a[...]
        scs[it, 0:1, :] = rowsum(gv * gv)
        scs[it, 1:2, :] = rowsum(dv * av)
        scs[it, 2:3, :] = rowsum(gv * av)
        scs[it, 3:4, :] = rowsum(av * av)
        sums_start(it)

    def first():
        halo_wait(0)
        hg[...] = hal[0]
        hd[...] = hal[0]

    def ycopy(i):
        return rcopy((slip, d)[i], (slp, dp)[i], pair(sem_y, i), at(obs, partner))

    tcopy = rcopy(tsrc, tdst, pair(sem_y, 2), at(obs, partner))

    def advance(it):
        tot = sums_end(it - 1)
        if it == 1:
            norms.append(tot[0:1])
        norm = norms[-1]
        step = norm / tot[1:2]
        after = norm - 2.0 * step * tot[2:3] + step * step * tot[3:4]
        ratio = after / norm
        norms.append(after)
        halo_wait(it)
        if it == 1:
            slip[...] = step * d[...]
        else:
            slip[...] += step * d[...]
        g[...] = g[...] - step * a[...]
        d[...] = g[...] + ratio * d[...]
        hg[...] = hg[...] - step * hal[it]
        hd[...] = hg[...] + ratio * hd[...]
        if it == ITERS - 1:
            ycopy(0).start()
            ycopy(1).start()
        return step, ratio

    def xcopy(j):
        return rcopy(nat.at[j], natp.at[j], (sem_out.at[9], sem_x.at[j]), at(obs, partner))

    def first_hook():
        gcopy(0).start()
        gcopy(1).start()
        clear()

    def first_late():
        for h in range(2):
            gcopy(h).wait_recv()

            @pl.loop(h * nblk // 2, (h + 1) * nblk // 2)
            def _(i):
                put_green(gpar, i, other)

    def first_finish(j, x):
        nat[j] = x
        xcopy(j).start()

    def put_operand(ref, i):
        top, bot = both(ref[pl.ds(pl.multiple_of(i * BAND, BAND), BAND), :])
        r0 = pl.multiple_of(i * 2 * BAND, 2 * BAND)
        put_cat(cat_d, r0, top, True)
        put_cat(cat_d, pl.multiple_of(r0 + BAND, BAND), bot, True)

    backward(0, first_hook, first_late, first_finish)

    @pl.loop(0, bc)
    def _(j):
        xcopy(j).wait_recv()
        r0 = pl.multiple_of(j * R, R)
        x = jnp.where(mine(R), nat[j], roll(natp[j]))
        g[pl.ds(r0, R), :] = x
        d[pl.ds(r0, R), :] = x

        @pl.when(j % per == per - 1)
        def _():
            put_operand(g, j // per)

    pl.when(c == 0)(build_laplace)
    forward(0, lambda: None, lambda: pl.when(c == 1)(build_laplace), first)
    for it in range(1, ITERS):
        def hook(it=it):
            forward_sent(it - 1)

            @pl.when(inner)
            def _():
                reg_work(it - 1)

        def finish(j, x):
            r0 = pl.multiple_of(j * R, R)
            a[pl.ds(r0, R), :] = x + wown[pl.ds(r0, R), :]

            @pl.when(j % per == per - 1)
            def _():
                put_operand(a, j // per)

        backward(it, hook, functools.partial(reg_end, it - 1), finish)
        forward(it, functools.partial(dots, it - 1), lambda: None, functools.partial(advance, it))

    last = ITERS - 1
    norm = norms[-1]
    pls[...] = sq[...]
    plr[obs * 2 + c] = sq[...]

    @pl.loop(1, n_plane)
    def _(i):
        pcopy(i).start()

    tsrc[0:1, :] = norm
    tsrc[1:2, :] = rowsum(sums_end(last))
    tcopy.start()

    forward_sent(last)
    ncopy.wait_send()
    rcopy(gbuf, gpar, (sem_out.at[3], sem_g.at[0]), at(obs, partner)).wait_send()
    rcopy(nat, natp, (sem_out.at[9], sem_x.at[0]), at(obs, partner)).wait_send()
    ycopy(0).wait_recv()
    ycopy(1).wait_recv()
    ycopy(0).wait_send()
    ycopy(1).wait_send()
    for i in range(CB):
        blk = slice(i * BAND, (i + 1) * BAND)
        m = mine(BAND)
        slip[blk, :] = jnp.where(m, slip[blk, :], roll(slp[blk, :]))
        d[blk, :] = jnp.where(m, d[blk, :], roll(dp[blk, :]))
    tcopy.wait_recv()
    tcopy.wait_send()

    part = plr.at[pl.ds(0, n_plane - 1)]
    rcopy(part, part, (sem_p.at[0], sem_p.at[1]), at(obs, partner)).wait_recv()

    def step_of(t, q):
        return t[0:1, :] / (fold(sum(rowsum(plr[2 * o + q]) for o in range(n_obs))) + t[1:2, :])

    step = jnp.where(mine(1), step_of(tsrc, c), step_of(tdst, other))

    out[...] = slip[...] + step * d[...]

    rcopy(part, part, (sem_p.at[0], sem_p.at[1]), at(obs, partner)).wait_send()


def shards(green, data, neighbours, reg_weight):
    rows, cols = green.shape
    E = data.shape[1]
    n_obs, n_patch = lax.axis_size("obs"), lax.axis_size("patch")
    nbit = n_obs.bit_length() - 1
    nz = n_patch // 2
    nc, bc = rows // 2 // R, cols // R
    NB = 2 * cols // BAND
    nblk = rows // BAND
    V = pltpu.VMEM
    D = pltpu.SemaphoreType.DMA
    scratch = [
        V((rows, cols), F32), V((rows, cols), F32), V((rows, E), F32),
        V((rows, 2 * cols), BF16), V((rows, 2 * cols), BF16),
        V(neighbours.shape, jnp.int32), V(neighbours.shape, jnp.int32), V((8, (NB + 4) * BAND), jnp.int32), V((1, E), F32),
        V((NB * BAND, 3 * BAND), BF16), V(((NB + 2) * BAND, 3 * BAND), BF16),
        V((2 * cols, 3 * E), BF16), V(((NB + 2) * BAND, 2 * E), BF16), V(((NB + 4) * BAND, 2 * E), BF16),
        V((E, rows), BF16), V((2 * E, rows), BF16),
        V((cols, E), F32), V((cols, E), F32), V((cols, E), F32), V((cols, E), F32), V((ITERS - 1, 2, R, E), F32),
        V((cols, E), F32), V((cols, E), F32), V((cols, E), F32), V((8, E), F32),
        V((ITERS, 2, R, E), F32), V((2, R, E), F32), V((2, R, E), F32), V((nc, R, E), F32), V((nc, R, E), F32),
        V((nc, R, E), F32), V((nc, R, E), F32), V((nc, R, E), F32),
        V((ITERS, nc, R, E), F32), V((ITERS, nc, R, E), F32),
        V((ITERS, nbit, bc, R, E), F32), V((ITERS, nbit, bc, R, E), F32),
        V((bc, R, E), F32), V((bc, R, E), F32),
        V((ITERS, 2, R, E), F32), V((ITERS - 1, 2, R, E), F32),
        V((ITERS, 8, E), F32), V((ITERS, nz, 8, E), F32),
        V((8, E), F32), V((2 * n_obs, 8, E), F32), V((8, E), F32), V((8, E), F32),
        D((10,)), D((2, nc)), D((2, nc)), D((2, nbit, bc)), D((2, 2)), D((ITERS - 1, 2)),
        D((ITERS,)), D((2,)), D((bc,)), D((2, 3)), D((2,)), D((2,)), D((rows // (2 * BAND) + 3,)),
    ]
    return pl.pallas_call(
        functools.partial(kernel, n_obs, n_patch, nc, bc),
        out_shape=jax.ShapeDtypeStruct((cols, E), F32),
        in_specs=[pl.BlockSpec(memory_space=pl.ANY)] * 4,
        out_specs=pl.BlockSpec(memory_space=pltpu.VMEM),
        scratch_shapes=scratch,
        compiler_params=pltpu.CompilerParams(
            collective_id=0, has_side_effects=True, vmem_limit_bytes=56 * 1024 * 1024),
    )(green, data, neighbours, reg_weight.reshape(1, E))


def solution(mesh):
    in_specs = (P("obs", "patch"), P("obs", None), P(None, "patch"), P())
    return jax.shard_map(shards, mesh=mesh, in_specs=in_specs, out_specs=P("patch", None), check_vma=False)
```

```python
import functools

import jax
import jax.numpy as jnp
from jax import lax
from jax.experimental import pallas as pl
from jax.experimental.pallas import tpu as pltpu
from jax.sharding import PartitionSpec as P

BAND = 128
ITERS = 3
MESH = pl.DeviceIdType.MESH
F32 = jnp.float32
BF16 = jnp.bfloat16
R = 64
HB = BAND // 2
LAG = 8


def dot(a, b):
    return lax.dot_general(a, b, (((1,), (0,)), ((), ())), preferred_element_type=F32)


def split(x):
    hi = x.astype(BF16)
    return hi, (x - hi.astype(F32)).astype(BF16)


def rowsum(x):
    return jnp.sum(x, axis=0, keepdims=True)


def kernel(n_obs, n_patch, nc, bc, green, data, nb_in, rw_in, out,
           gbuf, gpar, dbuf, ghi, glo, nb, nbp, nbe, rw, lm, lmt,
           cat_d, cat_e, cat_u, lt, lt0,
           d, g, a, wown, wsrc, slip, slp, dp, sq, hsrc, hd, hg, qd, qg,
           s, sr, sl, rl, rr, bb, br, nat, natp, hal, wr, scs, scr, zsq, pls, plr, tsrc, tdst,
           sem_out, sem_l, sem_r, sem_b, sem_h, sem_w, sem_s, sem_p, sem_x, sem_y, sem_g, sem_nb, sem_in, sem_zs):
    rows, cols = gbuf.shape
    E = dbuf.shape[1]
    H = E // 2
    CB = cols // BAND
    NB = 2 * CB
    RB = rows // (2 * BAND)
    nblk = rows // BAND
    per = BAND // R
    nz = n_patch // 2
    nbit = n_obs.bit_length() - 1
    obs = lax.axis_index("obs")
    pat = lax.axis_index("patch")
    z = pat // 2
    c = pat % 2
    other = 1 - c
    partner = z * 2 + other
    has_l, has_r = z > 0, z < nz - 1
    up, down = has_r, has_l
    inner = up & down
    n_plane = 2 * n_obs
    za, zb = nz // 2 - 1, nz // 2

    def lanes(n):
        return lax.broadcasted_iota(jnp.int32, (n, E), 1)

    def low(n):
        return lanes(n) < H

    def mine(n):
        i = lanes(n) - c * H
        return (i >= 0) & (i < H)

    def roll(x):
        return pltpu.roll(x, H, 1)

    def both(x):
        q = roll(x)
        m = low(x.shape[0])
        return jnp.where(m, x, q), jnp.where(m, q, x)

    def fold(x):
        return x + roll(x)

    def put_cat(ref, r0, v, third=False):
        n = v.shape[0]
        hi = v.astype(BF16)
        hf = hi.astype(F32)
        lf = v - hf
        m = low(n)
        ref[pl.ds(r0, n), 0:E] = jnp.where(m, hf, lf).astype(BF16)
        ref[pl.ds(r0, n), E:2 * E] = jnp.where(m, lf, hf).astype(BF16)
        if third:
            ref[pl.ds(r0, n), 2 * E:3 * E] = hi

    def rcopy(src, dst, sems, dev):
        return pltpu.make_async_remote_copy(
            src_ref=src, dst_ref=dst, send_sem=sems[0], recv_sem=sems[1],
            device_id=dev, device_id_type=MESH)

    def pair(sem, *idx):
        return sem.at[(0,) + idx], sem.at[(1,) + idx]

    def at(o, q):
        return (o, q)

    def plane(i):
        q = (obs * 2 + c + i) % n_plane
        return q // 2, z * 2 + q % 2

    def zpeer(i):
        return (z + i) % nz

    def load(i):
        rs = pl.ds(pl.multiple_of(i * 2 * BAND, 2 * BAND), 2 * BAND)
        return pltpu.make_async_copy(green.at[rs], gbuf.at[rs], sem_in.at[i])

    load_data = pltpu.make_async_copy(data, dbuf, sem_in.at[RB])
    load_nb = pltpu.make_async_copy(nb_in, nb, sem_in.at[RB + 1])
    load_rw = pltpu.make_async_copy(rw_in, rw, sem_in.at[RB + 2])
    load_data.start()

    @pl.loop(0, RB)
    def _(i):
        load(i).start()

    load_nb.start()
    load_rw.start()

    barrier = pltpu.get_barrier_semaphore()

    @pl.loop(1, nz)
    def _(i):
        pl.semaphore_signal(barrier, inc=1, device_id=at(obs, zpeer(i) * 2 + c), device_id_type=MESH)

    @pl.loop(1, n_plane)
    def _(i):
        pl.semaphore_signal(barrier, inc=1, device_id=plane(i), device_id_type=MESH)

    load_data.wait()

    for i in range(nblk):
        r0 = i * BAND
        hi, lo = split(dbuf[r0:r0 + BAND, :].T)
        lt0[0:E, r0:r0 + BAND] = hi
        lt0[E:2 * E, r0:r0 + BAND] = lo

    def put_green(src, i, core):
        r0 = pl.multiple_of(i * BAND, BAND)
        hi, lo = split(src[pl.ds(r0, BAND), :])
        for j in range(CB):
            c0 = pl.multiple_of((2 * j + core) * BAND, BAND)
            ghi[pl.ds(r0, BAND), pl.ds(c0, BAND)] = hi[:, j * BAND:(j + 1) * BAND]
            glo[pl.ds(r0, BAND), pl.ds(c0, BAND)] = lo[:, j * BAND:(j + 1) * BAND]

    @pl.loop(0, RB)
    def _(i):
        load(i).wait()
        put_green(gbuf, 2 * i, c)
        put_green(gbuf, 2 * i + 1, c)

    load_nb.wait()
    load_rw.wait()
    wrow = rw[...]
    weight = jnp.where(mine(1), wrow, roll(wrow))

    pl.semaphore_wait(barrier, nz - 1 + n_plane - 1)

    ncopy = rcopy(nb, nbp, (sem_nb.at[0], sem_nb.at[1]), at(obs, partner))
    ncopy.start()

    def gcopy(i):
        rs = pl.ds(i * BAND, BAND)
        return rcopy(gbuf.at[rs], gpar.at[rs], (sem_out.at[3], sem_g.at[i // (nblk // 2)]), at(obs, partner))

    def build_laplace():
        ncopy.wait_recv()
        zero_u = jnp.zeros((2 * BAND, 2 * E), BF16)
        cat_u[0:2 * BAND, :] = zero_u
        cat_u[(NB + 2) * BAND:(NB + 4) * BAND, :] = zero_u
        nbe[...] = jnp.full(nbe.shape, -(2 ** 24), jnp.int32)
        base = z * (2 * cols)
        own0 = pl.multiple_of((2 + c * CB) * BAND, BAND)
        par0 = pl.multiple_of((2 + other * CB) * BAND, BAND)
        nbe[0:3, pl.ds(own0, cols)] = nb[...] - base
        nbe[0:3, pl.ds(par0, cols)] = nbp[...] - base
        K = 3 * BAND

        for j in range(NB + 2):
            r0 = j * BAND
            col = lax.broadcasted_iota(jnp.int32, (BAND, K), 0) + (j - 1) * BAND
            own = lax.broadcasted_iota(jnp.int32, (BAND, K), 1) + (j - 2) * BAND
            m = jnp.where(col == own, 4.0, 0.0)
            for k in range(3):
                m = m - jnp.where(col == nbe[k:k + 1, pl.ds(r0, K)], 1.0, 0.0)
            lmt[pl.ds(r0, BAND), :] = m.astype(BF16)

        for b in range(NB):
            r0, n0 = b * BAND, (b + 2) * BAND
            row = lax.broadcasted_iota(jnp.int32, (BAND, K), 0) + b * BAND
            col = lax.broadcasted_iota(jnp.int32, (BAND, K), 1) + (b - 1) * BAND
            m = jnp.where(col == row, 4.0, 0.0)
            t = nbe[0:8, pl.ds(n0, BAND)].T
            for k in range(3):
                m = m - jnp.where(col == t[:, k:k + 1], 1.0, 0.0)
            lm[pl.ds(r0, BAND), :] = m.astype(BF16)

    def clear():
        scs[...] = jnp.zeros((ITERS, 8, E), F32)
        zero_c = jnp.zeros((nc, R, E), F32)
        zero_h = jnp.zeros((HB, E), F32)

        @pl.when(z == 0)
        def _():
            for it in range(ITERS):
                rl[it] = zero_c
                hal[it, 0] = zero_h
            for it in range(ITERS - 1):
                wr[it, 0] = zero_h

        @pl.when(z == nz - 1)
        def _():
            for it in range(ITERS):
                rr[it] = zero_c
                hal[it, 1] = zero_h
            for it in range(ITERS - 1):
                wr[it, 1] = zero_h

    def bit_partner(p, j):
        b0, b1 = 1 << p, 1 << (nbit - 1 - p)
        bit = b0 + (j % 2) * (b1 - b0)
        return at(obs + bit * (1 - 2 * ((obs // bit) % 2)), pat)

    def bcopy(b, p, j):
        return rcopy(bb.at[b, p, j], br.at[b, p, j], (sem_out.at[2], sem_b.at[b % 2, p, j]), bit_partner(p, j))

    def product(b, m):
        if b == 0:
            c0 = pl.multiple_of((2 * m + c) * BAND, BAND)
            y = dot(lt0[...], ghi[:, pl.ds(c0, BAND)])
            y = y[:E] + y[E:] + dot(lt0[0:E, :], glo[:, pl.ds(c0, BAND)])
            return y.T
        c0 = pl.multiple_of(m * 2 * BAND, 2 * BAND)
        y = dot(lt[...], ghi[:, pl.ds(c0, 2 * BAND)])
        y = y[:H] + y[H:] + dot(lt[0:H, :], glo[:, pl.ds(c0, 2 * BAND)])
        return jnp.concatenate([y[:, :BAND], y[:, BAND:]], axis=0).T

    def xcopy(m):
        return rcopy(nat.at[m], natp.at[m], (sem_out.at[9], sem_x.at[m]), at(obs, partner))

    gcopy(0).start()

    def backward(b, hook, late, finish):
        for m in range(CB):
            y = product(b, m)
            if b == 0:
                nat[m] = y
                xcopy(m).start()
                gcopy(m + 1).start()
                continue
            bb[b, 0, m * per:(m + 1) * per] = y.reshape(per, R, E)
            for k in range(per):
                bcopy(b, 0, m * per + k).start()

        if b == 0:
            for i in range(CB + 1, nblk):
                gcopy(i).start()
            pl.when(c == 0)(build_laplace)
            for m in range(CB):
                xcopy(m).wait_recv()
                y = jnp.where(mine(BAND), nat[m], roll(natp[m]))
                bb[b, 0, m * per:(m + 1) * per] = y.reshape(per, R, E)
                for k in range(per):
                    bcopy(b, 0, m * per + k).start()

        hook()
        for p in range(1, nbit):
            @pl.loop(0, bc)
            def _(j):
                bcopy(b, p - 1, j).wait_recv()
                bb[b, p, j] = bb[b, p - 1, j] + br[b, p - 1, j]
                bcopy(b, p, j).start()

        late()

        @pl.loop(0, bc)
        def _(j):
            bcopy(b, nbit - 1, j).wait_recv()
            finish(j, bb[b, nbit - 1, j] + br[b, nbit - 1, j])

    def backward_sent(b):
        rcopy(bb.at[b], br.at[b], (sem_out.at[2], sem_b.at[0, 0, 0]), at(obs, partner)).wait_send()

    def rcopy_up(it, src, k):
        return rcopy(src.at[k], rl.at[it, k], (sem_out.at[0], sem_l.at[it % 2, k]), at(obs, pat + 2))

    def rcopy_down(it, src, k):
        return rcopy(src.at[k], rr.at[it, k], (sem_out.at[1], sem_r.at[it % 2, k]), at(obs, pat - 2))

    def hcopy_r(it):
        return rcopy(hsrc.at[it, 0], hal.at[it, 0], (sem_out.at[4], sem_h.at[it % 2, 0]), at(obs, pat + 2))

    def hcopy_l(it):
        return rcopy(hsrc.at[it, 1], hal.at[it, 1], (sem_out.at[5], sem_h.at[it % 2, 1]), at(obs, pat - 2))

    def put_lt(m):
        x = qd[pl.ds(m * per, per)].reshape(BAND, E)
        hi, lo = split(x.T)
        o0 = pl.multiple_of(m * 2 * BAND, 2 * BAND)
        o1 = pl.multiple_of(m * 2 * BAND + BAND, BAND)
        lt[0:H, pl.ds(o0, BAND)] = hi[:H]
        lt[H:E, pl.ds(o0, BAND)] = lo[:H]
        lt[0:H, pl.ds(o1, BAND)] = hi[H:]
        lt[H:E, pl.ds(o1, BAND)] = lo[H:]

    def forward(it, sums, after, hook):
        last = it == ITERS - 1
        v = a if it else g
        x = v[cols - BAND:cols, :]
        hsrc[it, 0] = jnp.where(low(HB), roll(x[:HB]), x[HB:])
        x = v[0:BAND, :]
        hsrc[it, 1] = jnp.where(low(HB), x[:HB], roll(x[HB:]))

        @pl.when(up & down)
        def _():
            hcopy_r(it).start()
            hcopy_l(it).start()

        if last:
            forward_last(sums, hook)
            return

        def group(m):
            r0 = m * 2 * BAND
            y = dot(ghi[r0:r0 + 2 * BAND, :], cat_d[:, 0:2 * E])
            y = y[:, :E] + y[:, E:] + dot(glo[r0:r0 + 2 * BAND, :], cat_d[:, 2 * E:3 * E])
            y = jnp.where(low(BAND), y[:BAND], y[BAND:])
            s[m * per:(m + 1) * per] = y.reshape(per, R, E)
            for k in range(per):
                @pl.when(z == 0)
                def _():
                    rcopy_up(it, s, m * per + k).start()

                @pl.when(z == nz - 1)
                def _():
                    rcopy_down(it, s, m * per + k).start()

        group(0)
        sums()

        @pl.when(up & (z == 0))
        def _():
            hcopy_r(it).start()

        @pl.when(down & (z == nz - 1))
        def _():
            hcopy_l(it).start()

        for m in range(1, RB):
            group(m)
        after()
        backward_sent(it)

        def chain(t, ends=True):
            kl = t - LAG * z
            kr = t - LAG * (nz - 1 - z)
            kt = t - LAG * jnp.maximum(z, nz - 1 - z)

            @pl.when(down & (kl >= 0) & (kl < nc))
            def _():
                rcopy_up(it, sr, kl).wait_recv()

                @pl.when(up)
                def _():
                    sr[kl] = rl[it, kl] + s[kl]
                    rcopy_up(it, sr, kl).start()

            @pl.when(up & (kr >= 0) & (kr < nc))
            def _():
                rcopy_down(it, sl, kr).wait_recv()

                @pl.when(down)
                def _():
                    sl[kr] = rr[it, kr] + s[kr]
                    rcopy_down(it, sl, kr).start()

            if not ends:
                return

            @pl.when((kt >= 0) & (kt < nc))
            def _():
                total = rl[it, kt] + s[kt] + rr[it, kt]
                if it:
                    step, ratio = scalars
                    rest = qg[kt] - step * total
                    total = rest + ratio * qd[kt]
                qg[kt] = rest if it else total
                qd[kt] = total

                @pl.when(kt % per == per - 1)
                def _():
                    put_lt(kt // per)

        pl.loop(LAG, LAG * (nz // 2))(functools.partial(chain, ends=False))
        scalars = hook()

        @pl.when(jnp.logical_not(inner))
        def _():
            reg_work(it)

        pl.loop(LAG * (nz // 2), nc + LAG * (nz - 1))(chain)

    def forward_last(sums, hook):
        it = ITERS - 1
        low_side = z <= za

        def order(i, n):
            return jnp.where(low_side, n - 1 - i, i)

        def group(i):
            m = order(i, RB)
            rs = pl.ds(pl.multiple_of(m * 2 * BAND, 2 * BAND), 2 * BAND)
            y = dot(ghi[rs, :], cat_d[:, 0:2 * E])
            y = y[:, :E] + y[:, E:] + dot(glo[rs, :], cat_d[:, 2 * E:3 * E])
            y = jnp.where(low(BAND), y[:BAND], y[BAND:])
            s[pl.ds(m * per, per)] = y.reshape(per, R, E)
            for j in range(per):
                k = m * per + order(j, per)

                @pl.when((z == 0) & ((z < za) | (k >= nc // 2)))
                def _():
                    rcopy_up(it, s, k).start()

                @pl.when((z == nz - 1) & ((z > zb) | (k < nc // 2)))
                def _():
                    rcopy_down(it, s, k).start()

        group(0)
        sums()

        @pl.when(up & (z == 0))
        def _():
            hcopy_r(it).start()

        @pl.when(down & (z == nz - 1))
        def _():
            hcopy_l(it).start()

        for i in range(1, RB):
            group(i)
        backward_sent(it)
        sq[...] = jnp.zeros((8, E), F32)

        def move(n0, n1):
            @pl.loop(n0, n1)
            def _(i):
                k = order(i, nc)

                @pl.when(low_side & down)
                def _():
                    rcopy_up(it, sr, k).wait_recv()

                    @pl.when((z < za) | (k >= nc // 2))
                    def _():
                        sr[k] = rl[it, k] + s[k]
                        rcopy_up(it, sr, k).start()

                @pl.when(jnp.logical_not(low_side) & up)
                def _():
                    rcopy_down(it, sl, k).wait_recv()

                    @pl.when((z > zb) | (k < nc // 2))
                    def _():
                        sl[k] = rr[it, k] + s[k]
                        rcopy_down(it, sl, k).start()

        half = nc - nc // 2
        move(0, half)
        step, ratio = hook()
        move(half, nc)

        def ends(k):
            total = rl[it, k] + s[k] + rr[it, k]
            total = qg[k] - step * total + ratio * qd[k]
            sq[...] += jnp.sum((total * total).reshape(R // 8, 8, E), axis=0)

        @pl.when(z == za)
        def _():
            @pl.loop(0, nc // 2)
            def _(k):
                rcopy_down(it, sl, k).wait_recv()
                ends(k)

        @pl.when(z == zb)
        def _():
            @pl.loop(nc // 2, nc)
            def _(k):
                rcopy_up(it, sr, k).wait_recv()
                ends(k)

    def last_sent():
        it = ITERS - 1

        def wait(buf, sem, n):
            part = buf.at[pl.ds(0, n)]
            rcopy(part, part, (sem, sem_p.at[2]), at(obs, partner)).wait_send()

        @pl.when(z < za)
        def _():
            wait(sr, sem_out.at[0], nc)

        @pl.when(z == za)
        def _():
            wait(sr, sem_out.at[0], nc - nc // 2)

        @pl.when(z == zb)
        def _():
            wait(sl, sem_out.at[1], nc // 2)

        @pl.when(z > zb)
        def _():
            wait(sl, sem_out.at[1], nc)

        @pl.when(up)
        def _():
            hcopy_r(it).wait_send()

        @pl.when(down)
        def _():
            hcopy_l(it).wait_send()

    def forward_sent(it):
        @pl.when(up)
        def _():
            rcopy(sr, rl.at[it], (sem_out.at[0], sem_l.at[0, 0]), at(obs, partner)).wait_send()

        @pl.when(down)
        def _():
            rcopy(sl, rr.at[it], (sem_out.at[1], sem_r.at[0, 0]), at(obs, partner)).wait_send()

        @pl.when(up)
        def _():
            hcopy_r(it).wait_send()

        @pl.when(down)
        def _():
            hcopy_l(it).wait_send()

    def halo_wait(it):
        @pl.when(has_l)
        def _():
            hcopy_r(it).wait_recv()

        @pl.when(has_r)
        def _():
            hcopy_l(it).wait_recv()

    def widen(x):
        top, bot = both(x)
        return jnp.concatenate([top, bot], axis=0)

    def laplace():
        put_cat(cat_e, 0, widen(hd[0]))
        put_cat(cat_e, (NB + 1) * BAND, widen(hd[1]))

        for i in range(CB):
            top, bot = both(d[i * BAND:(i + 1) * BAND, :])
            put_cat(cat_e, (i + 1) * BAND, top)
            put_cat(cat_e, (CB + i + 1) * BAND, bot)

    def banded(mat, vec, j):
        r0 = j * BAND
        y = dot(mat[r0:r0 + BAND, :], vec[r0:r0 + 3 * BAND, :])
        return y[:, :E] + y[:, E:]

    def lap_rows(i):
        return weight * jnp.where(low(BAND), banded(lm, cat_e, i), banded(lm, cat_e, CB + i))

    def wcopy_l(it):
        return rcopy(wsrc.at[it, 0], wr.at[it, 1], (sem_out.at[7], sem_w.at[it, 1]), at(obs, pat - 2))

    def wcopy_r(it):
        return rcopy(wsrc.at[it, 1], wr.at[it, 0], (sem_out.at[6], sem_w.at[it, 0]), at(obs, pat + 2))

    def reg_work(it):
        laplace()

        for i in range(CB):
            top, bot = both(lap_rows(i))
            put_cat(cat_u, (i + 2) * BAND, top)
            put_cat(cat_u, (CB + i + 2) * BAND, bot)

        for side, j in ((0, 0), (1, NB + 1)):
            y = banded(lmt, cat_u, j)
            wsrc[it, side] = weight * jnp.where(low(HB), y[:HB], y[HB:])

        @pl.when(has_l)
        def _():
            wcopy_l(it).start()

        @pl.when(has_r)
        def _():
            wcopy_r(it).start()

        for i in range(CB):
            y = jnp.where(low(BAND), banded(lmt, cat_u, i + 1), banded(lmt, cat_u, CB + i + 1))
            wown[i * BAND:(i + 1) * BAND, :] = weight * y

    def reg_sums():
        last = ITERS - 1
        laplace()
        for i in range(CB):
            u = lap_rows(i)
            scs[last] += jnp.sum((u * u).reshape(BAND // 8, 8, E), axis=0)
        sums_start(last)

    def reg_end(it):
        @pl.when(has_l)
        def _():
            wcopy_r(it).wait_recv()

        @pl.when(has_r)
        def _():
            wcopy_l(it).wait_recv()

        wown[0:BAND, :] += jnp.where(low(BAND), widen(wr[it, 0]), 0.0)
        wown[cols - BAND:cols, :] += jnp.where(low(BAND), 0.0, widen(wr[it, 1]))
        reg_sent(it)

    def reg_sent(it):
        @pl.when(has_l)
        def _():
            wcopy_l(it).wait_send()

        @pl.when(has_r)
        def _():
            wcopy_r(it).wait_send()

    def scopy(it, q):
        return rcopy(scs.at[it], scr.at[it, z], (sem_out.at[8], sem_s.at[it]), at(obs, q * 2 + c))

    def sums_all(it):
        part = scr.at[it, pl.ds(0, nz - 1)]
        return rcopy(part, part, (sem_out.at[8], sem_s.at[it]), at(obs, partner))

    def sums_start(it):
        scr[it, z] = scs[it]

        @pl.loop(1, nz)
        def _(i):
            scopy(it, zpeer(i)).start()

    def sums_end(it):
        sums_all(it).wait_recv()
        sums_all(it).wait_send()
        return fold(jnp.sum(scr[it], axis=0))

    def pcopy(i):
        po, pp = plane(i)
        return rcopy(pls, plr.at[obs * 2 + c], (sem_p.at[0], sem_p.at[1]), (po, pp))

    norms = []

    def dots(it):
        gv, dv, av = g[...], d[...], a[...]
        scs[it, 0:1, :] = rowsum(gv * gv)
        scs[it, 1:2, :] = rowsum(dv * av)
        scs[it, 2:3, :] = rowsum(gv * av)
        scs[it, 3:4, :] = rowsum(av * av)
        sums_start(it)

    def first():
        halo_wait(0)
        hg[...] = hal[0]
        hd[...] = hal[0]

    def ycopy(i):
        return rcopy((slip, d)[i], (slp, dp)[i], pair(sem_y, i), at(obs, partner))

    tcopy = rcopy(tsrc, tdst, pair(sem_y, 2), at(obs, partner))

    def advance(it):
        tot = sums_end(it - 1)
        if it == 1:
            norms.append(tot[0:1])
        norm = norms[-1]
        step = norm / tot[1:2]
        after = norm - 2.0 * step * tot[2:3] + step * step * tot[3:4]
        ratio = after / norm
        norms.append(after)
        halo_wait(it)
        if it == 1:
            slip[...] = step * d[...]
        else:
            slip[...] += step * d[...]
        g[...] = g[...] - step * a[...]
        d[...] = g[...] + ratio * d[...]
        hg[...] = hg[...] - step * hal[it]
        hd[...] = hg[...] + ratio * hd[...]
        if it == ITERS - 1:
            ycopy(0).start()
            ycopy(1).start()
        return step, ratio

    def first_hook():
        clear()

    def first_late():
        for h in range(2):
            rs = pl.ds(h * (rows // 2), rows // 2)
            rcopy(gbuf.at[rs], gpar.at[rs], (sem_out.at[3], sem_g.at[h]), at(obs, partner)).wait_recv()

            @pl.loop(h * nblk // 2, (h + 1) * nblk // 2)
            def _(i):
                put_green(gpar, i, other)

    def put_operand(ref, i):
        top, bot = both(ref[pl.ds(pl.multiple_of(i * BAND, BAND), BAND), :])
        r0 = pl.multiple_of(i * 2 * BAND, 2 * BAND)
        put_cat(cat_d, r0, top, True)
        put_cat(cat_d, pl.multiple_of(r0 + BAND, BAND), bot, True)

    def first_finish(j, x):
        r0 = pl.multiple_of(j * R, R)
        g[pl.ds(r0, R), :] = x
        d[pl.ds(r0, R), :] = x

        @pl.when(j % per == per - 1)
        def _():
            put_operand(g, j // per)

    backward(0, first_hook, first_late, first_finish)
    forward(0, lambda: None, lambda: pl.when(c == 1)(build_laplace), first)
    for it in range(1, ITERS):
        def hook(it=it):
            forward_sent(it - 1)

            @pl.when(inner)
            def _():
                reg_work(it - 1)

        def finish(j, x):
            r0 = pl.multiple_of(j * R, R)
            a[pl.ds(r0, R), :] = x + wown[pl.ds(r0, R), :]

            @pl.when(j % per == per - 1)
            def _():
                put_operand(a, j // per)

        backward(it, hook, functools.partial(reg_end, it - 1), finish)
        forward(it, functools.partial(dots, it - 1), lambda: None, functools.partial(advance, it))

    last = ITERS - 1
    norm = norms[-1]
    mid = (z == za) | (z == zb)

    def zcopy(i):
        q = zpeer(i)
        return rcopy(sq, zsq.at[z - za], (sem_zs.at[0], sem_p.at[2 + z - za]), at(obs, q * 2 + c))

    def zwait(slot):
        rcopy(sq, zsq.at[slot], (sem_zs.at[0], sem_p.at[2 + slot]), at(obs, partner)).wait_recv()

    @pl.when(mid)
    def _():
        zsq[z - za] = sq[...]

        @pl.loop(1, nz)
        def _(i):
            zcopy(i).start()

    reg_sums()

    @pl.when(z != za)
    def _():
        zwait(0)

    @pl.when(z != zb)
    def _():
        zwait(1)

    pls[...] = zsq[0] + zsq[1]
    plr[obs * 2 + c] = pls[...]

    @pl.loop(1, n_plane)
    def _(i):
        pcopy(i).start()

    tsrc[0:1, :] = norm
    tsrc[1:2, :] = rowsum(sums_end(last))
    tcopy.start()

    last_sent()

    @pl.when(mid)
    def _():
        part = scr.at[last, pl.ds(0, nz - 1)]
        rcopy(part, part, (sem_zs.at[0], sem_p.at[2]), at(obs, partner)).wait_send()

    ncopy.wait_send()
    rcopy(gbuf, gpar, (sem_out.at[3], sem_g.at[0]), at(obs, partner)).wait_send()
    rcopy(nat, natp, (sem_out.at[9], sem_x.at[0]), at(obs, partner)).wait_send()
    ycopy(0).wait_recv()
    ycopy(1).wait_recv()
    ycopy(0).wait_send()
    ycopy(1).wait_send()
    for i in range(CB):
        blk = slice(i * BAND, (i + 1) * BAND)
        m = mine(BAND)
        slip[blk, :] = jnp.where(m, slip[blk, :], roll(slp[blk, :]))
        d[blk, :] = jnp.where(m, d[blk, :], roll(dp[blk, :]))
    tcopy.wait_recv()
    tcopy.wait_send()

    part = plr.at[pl.ds(0, n_plane - 1)]
    rcopy(part, part, (sem_p.at[0], sem_p.at[1]), at(obs, partner)).wait_recv()

    def step_of(t, q):
        return t[0:1, :] / (fold(sum(rowsum(plr[2 * o + q]) for o in range(n_obs))) + t[1:2, :])

    step = jnp.where(mine(1), step_of(tsrc, c), step_of(tdst, other))

    out[...] = slip[...] + step * d[...]

    rcopy(part, part, (sem_p.at[0], sem_p.at[1]), at(obs, partner)).wait_send()


def shards(green, data, neighbours, reg_weight):
    rows, cols = green.shape
    E = data.shape[1]
    n_obs, n_patch = lax.axis_size("obs"), lax.axis_size("patch")
    nbit = n_obs.bit_length() - 1
    nz = n_patch // 2
    nc, bc = rows // 2 // R, cols // R
    NB = 2 * cols // BAND
    nblk = rows // BAND
    V = pltpu.VMEM
    D = pltpu.SemaphoreType.DMA
    scratch = [
        V((rows, cols), F32), V((rows, cols), F32), V((rows, E), F32),
        V((rows, 2 * cols), BF16), V((rows, 2 * cols), BF16),
        V(neighbours.shape, jnp.int32), V(neighbours.shape, jnp.int32), V((8, (NB + 4) * BAND), jnp.int32), V((1, E), F32),
        V((NB * BAND, 3 * BAND), BF16), V(((NB + 2) * BAND, 3 * BAND), BF16),
        V((2 * cols, 3 * E), BF16), V(((NB + 2) * BAND, 2 * E), BF16), V(((NB + 4) * BAND, 2 * E), BF16),
        V((E, rows), BF16), V((2 * E, rows), BF16),
        V((cols, E), F32), V((cols, E), F32), V((cols, E), F32), V((cols, E), F32), V((ITERS - 1, 2, HB, E), F32),
        V((cols, E), F32), V((cols, E), F32), V((cols, E), F32), V((8, E), F32),
        V((ITERS, 2, HB, E), F32), V((2, HB, E), F32), V((2, HB, E), F32), V((nc, R, E), F32), V((nc, R, E), F32),
        V((nc, R, E), F32), V((nc, R, E), F32), V((nc, R, E), F32),
        V((ITERS, nc, R, E), F32), V((ITERS, nc, R, E), F32),
        V((ITERS, nbit, bc, R, E), F32), V((ITERS, nbit, bc, R, E), F32),
        V((cols // BAND, BAND, E), F32), V((cols // BAND, BAND, E), F32),
        V((ITERS, 2, HB, E), F32), V((ITERS - 1, 2, HB, E), F32),
        V((ITERS, 8, E), F32), V((ITERS, nz, 8, E), F32),
        V((2, 8, E), F32), V((8, E), F32), V((2 * n_obs, 8, E), F32), V((8, E), F32), V((8, E), F32),
        D((10,)), D((2, nc)), D((2, nc)), D((2, nbit, bc)), D((2, 2)), D((ITERS - 1, 2)),
        D((ITERS,)), D((4,)), D((cols // BAND,)), D((2, 3)), D((2,)), D((2,)), D((rows // (2 * BAND) + 3,)), D((1,)),
    ]
    return pl.pallas_call(
        functools.partial(kernel, n_obs, n_patch, nc, bc),
        out_shape=pltpu.VMEM((cols, E), F32),
        in_specs=[pl.BlockSpec(memory_space=pl.ANY)] * 4,
        out_specs=pl.BlockSpec(memory_space=pltpu.VMEM),
        scratch_shapes=scratch,
        compiler_params=pltpu.CompilerParams(
            collective_id=0, has_side_effects=True, vmem_limit_bytes=56 * 1024 * 1024),
    )(green, data, neighbours, reg_weight.reshape(1, E))


def solution(mesh):
    in_specs = (P("obs", "patch"), P("obs", None), P(None, "patch"), P())
    return jax.shard_map(shards, mesh=mesh, in_specs=in_specs, out_specs=P("patch", None), check_vma=False)
```

```python
import functools

import jax
import jax.numpy as jnp
from jax import lax
from jax.experimental import pallas as pl
from jax.experimental.pallas import tpu as pltpu
from jax.sharding import PartitionSpec as P

BAND = 128
ITERS = 3
MESH = pl.DeviceIdType.MESH
F32 = jnp.float32
BF16 = jnp.bfloat16
R = 64
HB = BAND // 2
LAG = 8


def dot(a, b):
    return lax.dot_general(a, b, (((1,), (0,)), ((), ())), preferred_element_type=F32)


def split(x):
    hi = x.astype(BF16)
    return hi, (x - hi.astype(F32)).astype(BF16)


def batches(n):
    return [[0]] + [list(range(i, min(i + 2, n))) for i in range(1, n, 2)]


def rowsum(x):
    return jnp.sum(x, axis=0, keepdims=True)


def kernel(n_obs, n_patch, nc, bc, green, data, nb_in, rw_in, out,
           gbuf, gpar, dbuf, ghi, glo, nb, nbp, nbe, rw, lm, lmt,
           cat_d, cat_e, cat_u, lt, lt0,
           d, g, a, wown, wsrc, slip, slp, dp, sq, hsrc, hd, hg, qd, qg,
           s, sr, sl, rl, rr, bb, br, nat, natp, hal, wr, scs, scr, zsq, pls, plr, tsrc, tdst,
           sem_out, sem_l, sem_r, sem_b, sem_h, sem_w, sem_s, sem_p, sem_x, sem_y, sem_g, sem_nb, sem_in, sem_zs):
    rows, cols = gbuf.shape
    E = dbuf.shape[1]
    H = E // 2
    CB = cols // BAND
    NB = 2 * CB
    RB = rows // (2 * BAND)
    nblk = rows // BAND
    per = BAND // R
    nz = n_patch // 2
    nbit = n_obs.bit_length() - 1
    obs = lax.axis_index("obs")
    pat = lax.axis_index("patch")
    z = pat // 2
    c = pat % 2
    other = 1 - c
    partner = z * 2 + other
    has_l, has_r = z > 0, z < nz - 1
    up, down = has_r, has_l
    inner = up & down
    n_plane = 2 * n_obs
    za, zb = nz // 2 - 1, nz // 2

    def lanes(n):
        return lax.broadcasted_iota(jnp.int32, (n, E), 1)

    def low(n):
        return lanes(n) < H

    def mine(n):
        i = lanes(n) - c * H
        return (i >= 0) & (i < H)

    def roll(x):
        return pltpu.roll(x, H, 1)

    def both(x):
        q = roll(x)
        m = low(x.shape[0])
        return jnp.where(m, x, q), jnp.where(m, q, x)

    def fold(x):
        return x + roll(x)

    def put_cat(ref, r0, v, third=False):
        n = v.shape[0]
        hi = v.astype(BF16)
        hf = hi.astype(F32)
        lf = v - hf
        m = low(n)
        ref[pl.ds(r0, n), 0:E] = jnp.where(m, hf, lf).astype(BF16)
        ref[pl.ds(r0, n), E:2 * E] = jnp.where(m, lf, hf).astype(BF16)
        if third:
            ref[pl.ds(r0, n), 2 * E:3 * E] = hi

    def rcopy(src, dst, sems, dev):
        return pltpu.make_async_remote_copy(
            src_ref=src, dst_ref=dst, send_sem=sems[0], recv_sem=sems[1],
            device_id=dev, device_id_type=MESH)

    def pair(sem, *idx):
        return sem.at[(0,) + idx], sem.at[(1,) + idx]

    def at(o, q):
        return (o, q)

    def plane(i):
        q = (obs * 2 + c + i) % n_plane
        return q // 2, z * 2 + q % 2

    def zpeer(i):
        return (z + i) % nz

    def load(i):
        rs = pl.ds(pl.multiple_of(i * 2 * BAND, 2 * BAND), 2 * BAND)
        return pltpu.make_async_copy(green.at[rs], gbuf.at[rs], sem_in.at[i])

    load_data = pltpu.make_async_copy(data, dbuf, sem_in.at[RB])
    load_nb = pltpu.make_async_copy(nb_in, nb, sem_in.at[RB + 1])
    load_rw = pltpu.make_async_copy(rw_in, rw, sem_in.at[RB + 2])
    load_data.start()

    @pl.loop(0, RB)
    def _(i):
        load(i).start()

    load_nb.start()
    load_rw.start()

    barrier = pltpu.get_barrier_semaphore()

    @pl.loop(1, nz)
    def _(i):
        pl.semaphore_signal(barrier, inc=1, device_id=at(obs, zpeer(i) * 2 + c), device_id_type=MESH)

    @pl.loop(1, n_plane)
    def _(i):
        pl.semaphore_signal(barrier, inc=1, device_id=plane(i), device_id_type=MESH)

    load_data.wait()

    for i in range(nblk):
        r0 = i * BAND
        hi, lo = split(dbuf[r0:r0 + BAND, :].T)
        lt0[0:E, r0:r0 + BAND] = hi
        lt0[E:2 * E, r0:r0 + BAND] = lo

    def put_green(src, i, core):
        r0 = pl.multiple_of(i * BAND, BAND)
        hi, lo = split(src[pl.ds(r0, BAND), :])
        for j in range(CB):
            c0 = pl.multiple_of((2 * j + core) * BAND, BAND)
            ghi[pl.ds(r0, BAND), pl.ds(c0, BAND)] = hi[:, j * BAND:(j + 1) * BAND]
            glo[pl.ds(r0, BAND), pl.ds(c0, BAND)] = lo[:, j * BAND:(j + 1) * BAND]

    @pl.loop(0, RB)
    def _(i):
        load(i).wait()
        put_green(gbuf, 2 * i, c)
        put_green(gbuf, 2 * i + 1, c)

    load_nb.wait()
    load_rw.wait()
    wrow = rw[...]
    weight = jnp.where(mine(1), wrow, roll(wrow))

    ncopy = rcopy(nb, nbp, (sem_nb.at[0], sem_nb.at[1]), at(obs, partner))
    def gcopy(i):
        rs = pl.ds(i * BAND, BAND)
        return rcopy(gbuf.at[rs], gpar.at[rs], (sem_out.at[3], sem_g.at[i // (nblk // 2)]), at(obs, partner))

    def build_laplace():
        ncopy.wait_recv()
        zero_u = jnp.zeros((2 * BAND, 2 * E), BF16)
        cat_u[0:2 * BAND, :] = zero_u
        cat_u[(NB + 2) * BAND:(NB + 4) * BAND, :] = zero_u
        nbe[...] = jnp.full(nbe.shape, -(2 ** 24), jnp.int32)
        base = z * (2 * cols)
        own0 = pl.multiple_of((2 + c * CB) * BAND, BAND)
        par0 = pl.multiple_of((2 + other * CB) * BAND, BAND)
        nbe[0:3, pl.ds(own0, cols)] = nb[...] - base
        nbe[0:3, pl.ds(par0, cols)] = nbp[...] - base
        K = 3 * BAND

        for j in range(NB + 2):
            r0 = j * BAND
            col = lax.broadcasted_iota(jnp.int32, (BAND, K), 0) + (j - 1) * BAND
            own = lax.broadcasted_iota(jnp.int32, (BAND, K), 1) + (j - 2) * BAND
            m = jnp.where(col == own, 4.0, 0.0)
            for k in range(3):
                m = m - jnp.where(col == nbe[k:k + 1, pl.ds(r0, K)], 1.0, 0.0)
            lmt[pl.ds(r0, BAND), :] = m.astype(BF16)

        for b in range(NB):
            r0, n0 = b * BAND, (b + 2) * BAND
            row = lax.broadcasted_iota(jnp.int32, (BAND, K), 0) + b * BAND
            col = lax.broadcasted_iota(jnp.int32, (BAND, K), 1) + (b - 1) * BAND
            m = jnp.where(col == row, 4.0, 0.0)
            t = nbe[0:8, pl.ds(n0, BAND)].T
            for k in range(3):
                m = m - jnp.where(col == t[:, k:k + 1], 1.0, 0.0)
            lm[pl.ds(r0, BAND), :] = m.astype(BF16)

    def clear():
        scs[...] = jnp.zeros((ITERS, 8, E), F32)
        zero_c = jnp.zeros((nc, R, E), F32)
        zero_h = jnp.zeros((HB, E), F32)

        @pl.when(z == 0)
        def _():
            for it in range(ITERS):
                rl[it] = zero_c
                hal[it, 0] = zero_h
            for it in range(ITERS - 1):
                wr[it, 0] = zero_h

        @pl.when(z == nz - 1)
        def _():
            for it in range(ITERS):
                rr[it] = zero_c
                hal[it, 1] = zero_h
            for it in range(ITERS - 1):
                wr[it, 1] = zero_h

    def bit_partner(p, j):
        b0, b1 = 1 << p, 1 << (nbit - 1 - p)
        bit = b0 + (j % 2) * (b1 - b0)
        return at(obs + bit * (1 - 2 * ((obs // bit) % 2)), pat)

    def bcopy(b, p, j):
        return rcopy(bb.at[b, p, j], br.at[b, p, j], (sem_out.at[2], sem_b.at[b % 2, p, j]), bit_partner(p, j))

    def product(b, m):
        if b == 0:
            c0 = pl.multiple_of((2 * m + c) * BAND, BAND)
            y = dot(lt0[...], ghi[:, pl.ds(c0, BAND)])
            y = y[:E] + y[E:] + dot(lt0[0:E, :], glo[:, pl.ds(c0, BAND)])
            return y.T
        c0 = pl.multiple_of(m * 2 * BAND, 2 * BAND)
        y = dot(lt[...], ghi[:, pl.ds(c0, 2 * BAND)])
        y = y[:H] + y[H:] + dot(lt[0:H, :], glo[:, pl.ds(c0, 2 * BAND)])
        return jnp.concatenate([y[:, :BAND], y[:, BAND:]], axis=0).T

    def xcopy(m):
        return rcopy(nat.at[m], natp.at[m], (sem_out.at[9], sem_x.at[m]), at(obs, partner))

    def enter():
        pl.semaphore_wait(barrier, nz - 1 + n_plane - 1)
        ncopy.start()
        gcopy(0).start()

    def backward(b, hook, late, finish):
        for ms in batches(CB) if b else ([0, 1], range(2, CB)):
            for m in ms:
                y = product(b, m)
                if b == 0:
                    nat[m] = y
                else:
                    bb[b, 0, m * per:(m + 1) * per] = y.reshape(per, R, E)
            if b == 0 and ms[0] == 0:
                enter()
            for m in ms:
                if b == 0:
                    xcopy(m).start()
                else:
                    for k in range(per):
                        bcopy(b, 0, m * per + k).start()

        if b == 0:
            for i in range(1, nblk):
                gcopy(i).start()
            pl.when(c == 0)(build_laplace)
            for m in range(CB):
                xcopy(m).wait_recv()
                y = jnp.where(mine(BAND), nat[m], roll(natp[m]))
                bb[b, 0, m * per:(m + 1) * per] = y.reshape(per, R, E)
                for k in range(per):
                    bcopy(b, 0, m * per + k).start()

        hook()
        for p in range(1, nbit):
            @pl.loop(0, bc)
            def _(j):
                bcopy(b, p - 1, j).wait_recv()
                bb[b, p, j] = bb[b, p - 1, j] + br[b, p - 1, j]
                bcopy(b, p, j).start()

        late()

        @pl.loop(0, bc)
        def _(j):
            bcopy(b, nbit - 1, j).wait_recv()
            finish(j, bb[b, nbit - 1, j] + br[b, nbit - 1, j])

    def backward_sent(b):
        rcopy(bb.at[b], br.at[b], (sem_out.at[2], sem_b.at[0, 0, 0]), at(obs, partner)).wait_send()

    def rcopy_up(it, src, k):
        return rcopy(src.at[k], rl.at[it, k], (sem_out.at[0], sem_l.at[it % 2, k]), at(obs, pat + 2))

    def rcopy_down(it, src, k):
        return rcopy(src.at[k], rr.at[it, k], (sem_out.at[1], sem_r.at[it % 2, k]), at(obs, pat - 2))

    def hcopy_r(it):
        return rcopy(hsrc.at[it, 0], hal.at[it, 0], (sem_out.at[4], sem_h.at[it % 2, 0]), at(obs, pat + 2))

    def hcopy_l(it):
        return rcopy(hsrc.at[it, 1], hal.at[it, 1], (sem_out.at[5], sem_h.at[it % 2, 1]), at(obs, pat - 2))

    def put_lt(m):
        x = qd[pl.ds(m * per, per)].reshape(BAND, E)
        hi, lo = split(x.T)
        o0 = pl.multiple_of(m * 2 * BAND, 2 * BAND)
        o1 = pl.multiple_of(m * 2 * BAND + BAND, BAND)
        lt[0:H, pl.ds(o0, BAND)] = hi[:H]
        lt[H:E, pl.ds(o0, BAND)] = lo[:H]
        lt[0:H, pl.ds(o1, BAND)] = hi[H:]
        lt[H:E, pl.ds(o1, BAND)] = lo[H:]

    def forward(it, sums, after, hook):
        last = it == ITERS - 1
        v = a if it else g
        x = v[cols - BAND:cols, :]
        hsrc[it, 0] = jnp.where(low(HB), roll(x[:HB]), x[HB:])
        x = v[0:BAND, :]
        hsrc[it, 1] = jnp.where(low(HB), x[:HB], roll(x[HB:]))

        @pl.when(up & down)
        def _():
            hcopy_r(it).start()
            hcopy_l(it).start()

        if last:
            forward_last(sums, hook)
            return

        def group(m):
            r0 = m * 2 * BAND
            y = dot(ghi[r0:r0 + 2 * BAND, :], cat_d[:, 0:2 * E])
            y = y[:, :E] + y[:, E:] + dot(glo[r0:r0 + 2 * BAND, :], cat_d[:, 2 * E:3 * E])
            y = jnp.where(low(BAND), y[:BAND], y[BAND:])
            s[m * per:(m + 1) * per] = y.reshape(per, R, E)

        def send(ms):
            @pl.when(z == 0)
            def _():
                for k in range(ms[0] * per, (ms[-1] + 1) * per):
                    rcopy_up(it, s, k).start()

            @pl.when(z == nz - 1)
            def _():
                for k in range(ms[0] * per, (ms[-1] + 1) * per):
                    rcopy_down(it, s, k).start()

        group(0)
        send([0])
        sums()

        @pl.when(up & (z == 0))
        def _():
            hcopy_r(it).start()

        @pl.when(down & (z == nz - 1))
        def _():
            hcopy_l(it).start()

        for ms in batches(RB)[1:]:
            for m in ms:
                group(m)
            send(ms)
        after()
        backward_sent(it)

        def chain(t, ends=True):
            kl = t - LAG * z
            kr = t - LAG * (nz - 1 - z)
            kt = t - LAG * jnp.maximum(z, nz - 1 - z)

            @pl.when(down & (kl >= 0) & (kl < nc))
            def _():
                rcopy_up(it, sr, kl).wait_recv()

                @pl.when(up)
                def _():
                    sr[kl] = rl[it, kl] + s[kl]
                    rcopy_up(it, sr, kl).start()

            @pl.when(up & (kr >= 0) & (kr < nc))
            def _():
                rcopy_down(it, sl, kr).wait_recv()

                @pl.when(down)
                def _():
                    sl[kr] = rr[it, kr] + s[kr]
                    rcopy_down(it, sl, kr).start()

            if not ends:
                return

            @pl.when((kt >= 0) & (kt < nc))
            def _():
                total = rl[it, kt] + s[kt] + rr[it, kt]
                if it:
                    step, ratio = scalars
                    rest = qg[kt] - step * total
                    total = rest + ratio * qd[kt]
                qg[kt] = rest if it else total
                qd[kt] = total

                @pl.when(kt % per == per - 1)
                def _():
                    put_lt(kt // per)

        pl.loop(LAG, LAG * (nz // 2))(functools.partial(chain, ends=False))
        scalars = hook()

        @pl.when(jnp.logical_not(inner))
        def _():
            reg_work(it)

        pl.loop(LAG * (nz // 2), nc + LAG * (nz - 1))(chain)

    def forward_last(sums, hook):
        it = ITERS - 1
        low_side = z <= za

        def order(i, n):
            return jnp.where(low_side, n - 1 - i, i)

        def group(i):
            m = order(i, RB)
            rs = pl.ds(pl.multiple_of(m * 2 * BAND, 2 * BAND), 2 * BAND)
            y = dot(ghi[rs, :], cat_d[:, 0:2 * E])
            y = y[:, :E] + y[:, E:] + dot(glo[rs, :], cat_d[:, 2 * E:3 * E])
            y = jnp.where(low(BAND), y[:BAND], y[BAND:])
            s[pl.ds(m * per, per)] = y.reshape(per, R, E)

        def send(ms):
            for i in range(ms[0] * per, (ms[-1] + 1) * per):
                k = order(i, nc)

                @pl.when((z == 0) & ((z < za) | (k >= nc // 2)))
                def _():
                    rcopy_up(it, s, k).start()

                @pl.when((z == nz - 1) & ((z > zb) | (k < nc // 2)))
                def _():
                    rcopy_down(it, s, k).start()

        group(0)
        send([0])
        sums()

        @pl.when(up & (z == 0))
        def _():
            hcopy_r(it).start()

        @pl.when(down & (z == nz - 1))
        def _():
            hcopy_l(it).start()

        for ms in batches(RB)[1:]:
            for i in ms:
                group(i)
            send(ms)
        backward_sent(it)
        sq[...] = jnp.zeros((8, E), F32)

        def move(n0, n1):
            @pl.loop(n0, n1)
            def _(i):
                k = order(i, nc)

                @pl.when(low_side & down)
                def _():
                    rcopy_up(it, sr, k).wait_recv()

                    @pl.when((z < za) | (k >= nc // 2))
                    def _():
                        sr[k] = rl[it, k] + s[k]
                        rcopy_up(it, sr, k).start()

                @pl.when(jnp.logical_not(low_side) & up)
                def _():
                    rcopy_down(it, sl, k).wait_recv()

                    @pl.when((z > zb) | (k < nc // 2))
                    def _():
                        sl[k] = rr[it, k] + s[k]
                        rcopy_down(it, sl, k).start()

        half = nc - nc // 2
        move(0, half)
        step, ratio = hook()
        move(half, nc)

        def ends(k):
            total = rl[it, k] + s[k] + rr[it, k]
            total = qg[k] - step * total + ratio * qd[k]
            sq[...] += jnp.sum((total * total).reshape(R // 8, 8, E), axis=0)

        @pl.when(z == za)
        def _():
            @pl.loop(0, nc // 2)
            def _(k):
                rcopy_down(it, sl, k).wait_recv()
                ends(k)

        @pl.when(z == zb)
        def _():
            @pl.loop(nc // 2, nc)
            def _(k):
                rcopy_up(it, sr, k).wait_recv()
                ends(k)

    def last_sent():
        it = ITERS - 1

        def wait(buf, sem, n):
            part = buf.at[pl.ds(0, n)]
            rcopy(part, part, (sem, sem_p.at[2]), at(obs, partner)).wait_send()

        @pl.when(z < za)
        def _():
            wait(sr, sem_out.at[0], nc)

        @pl.when(z == za)
        def _():
            wait(sr, sem_out.at[0], nc - nc // 2)

        @pl.when(z == zb)
        def _():
            wait(sl, sem_out.at[1], nc // 2)

        @pl.when(z > zb)
        def _():
            wait(sl, sem_out.at[1], nc)

        @pl.when(up)
        def _():
            hcopy_r(it).wait_send()

        @pl.when(down)
        def _():
            hcopy_l(it).wait_send()

    def forward_sent(it):
        @pl.when(up)
        def _():
            rcopy(sr, rl.at[it], (sem_out.at[0], sem_l.at[0, 0]), at(obs, partner)).wait_send()

        @pl.when(down)
        def _():
            rcopy(sl, rr.at[it], (sem_out.at[1], sem_r.at[0, 0]), at(obs, partner)).wait_send()

        @pl.when(up)
        def _():
            hcopy_r(it).wait_send()

        @pl.when(down)
        def _():
            hcopy_l(it).wait_send()

    def halo_wait(it):
        @pl.when(has_l)
        def _():
            hcopy_r(it).wait_recv()

        @pl.when(has_r)
        def _():
            hcopy_l(it).wait_recv()

    def widen(x):
        top, bot = both(x)
        return jnp.concatenate([top, bot], axis=0)

    def laplace():
        put_cat(cat_e, 0, widen(hd[0]))
        put_cat(cat_e, (NB + 1) * BAND, widen(hd[1]))

        for i in range(CB):
            top, bot = both(d[i * BAND:(i + 1) * BAND, :])
            put_cat(cat_e, (i + 1) * BAND, top)
            put_cat(cat_e, (CB + i + 1) * BAND, bot)

    def banded(mat, vec, j):
        r0 = j * BAND
        y = dot(mat[r0:r0 + BAND, :], vec[r0:r0 + 3 * BAND, :])
        return y[:, :E] + y[:, E:]

    def lap_rows(i):
        return weight * jnp.where(low(BAND), banded(lm, cat_e, i), banded(lm, cat_e, CB + i))

    def wcopy_l(it):
        return rcopy(wsrc.at[it, 0], wr.at[it, 1], (sem_out.at[7], sem_w.at[it, 1]), at(obs, pat - 2))

    def wcopy_r(it):
        return rcopy(wsrc.at[it, 1], wr.at[it, 0], (sem_out.at[6], sem_w.at[it, 0]), at(obs, pat + 2))

    def reg_work(it):
        laplace()

        for i in range(CB):
            top, bot = both(lap_rows(i))
            put_cat(cat_u, (i + 2) * BAND, top)
            put_cat(cat_u, (CB + i + 2) * BAND, bot)

        for side, j in ((0, 0), (1, NB + 1)):
            y = banded(lmt, cat_u, j)
            wsrc[it, side] = weight * jnp.where(low(HB), y[:HB], y[HB:])

        @pl.when(has_l)
        def _():
            wcopy_l(it).start()

        @pl.when(has_r)
        def _():
            wcopy_r(it).start()

        for i in range(CB):
            y = jnp.where(low(BAND), banded(lmt, cat_u, i + 1), banded(lmt, cat_u, CB + i + 1))
            wown[i * BAND:(i + 1) * BAND, :] = weight * y

    def reg_sums():
        last = ITERS - 1
        laplace()
        for i in range(CB):
            u = lap_rows(i)
            scs[last] += jnp.sum((u * u).reshape(BAND // 8, 8, E), axis=0)
        sums_start(last)

    def reg_end(it):
        @pl.when(has_l)
        def _():
            wcopy_r(it).wait_recv()

        @pl.when(has_r)
        def _():
            wcopy_l(it).wait_recv()

        wown[0:BAND, :] += jnp.where(low(BAND), widen(wr[it, 0]), 0.0)
        wown[cols - BAND:cols, :] += jnp.where(low(BAND), 0.0, widen(wr[it, 1]))
        reg_sent(it)

    def reg_sent(it):
        @pl.when(has_l)
        def _():
            wcopy_l(it).wait_send()

        @pl.when(has_r)
        def _():
            wcopy_r(it).wait_send()

    def scopy(it, q):
        return rcopy(scs.at[it], scr.at[it, z], (sem_out.at[8], sem_s.at[it]), at(obs, q * 2 + c))

    def sums_all(it):
        part = scr.at[it, pl.ds(0, nz - 1)]
        return rcopy(part, part, (sem_out.at[8], sem_s.at[it]), at(obs, partner))

    def sums_start(it):
        scr[it, z] = scs[it]

        @pl.loop(1, nz)
        def _(i):
            scopy(it, zpeer(i)).start()

    def sums_end(it):
        sums_all(it).wait_recv()
        sums_all(it).wait_send()
        return fold(jnp.sum(scr[it], axis=0))

    def pcopy(i):
        po, pp = plane(i)
        return rcopy(pls, plr.at[obs * 2 + c], (sem_p.at[0], sem_p.at[1]), (po, pp))

    norms = []

    def dots(it):
        gv, dv, av = g[...], d[...], a[...]
        scs[it, 0:1, :] = rowsum(gv * gv)
        scs[it, 1:2, :] = rowsum(dv * av)
        scs[it, 2:3, :] = rowsum(gv * av)
        scs[it, 3:4, :] = rowsum(av * av)
        sums_start(it)

    def first():
        halo_wait(0)
        hg[...] = hal[0]
        hd[...] = hal[0]

    def ycopy(i):
        return rcopy((slip, d)[i], (slp, dp)[i], pair(sem_y, i), at(obs, partner))

    tcopy = rcopy(tsrc, tdst, pair(sem_y, 2), at(obs, partner))

    def advance(it):
        tot = sums_end(it - 1)
        if it == 1:
            norms.append(tot[0:1])
        norm = norms[-1]
        step = norm / tot[1:2]
        after = norm - 2.0 * step * tot[2:3] + step * step * tot[3:4]
        ratio = after / norm
        norms.append(after)
        halo_wait(it)
        if it == 1:
            slip[...] = step * d[...]
        else:
            slip[...] += step * d[...]
        g[...] = g[...] - step * a[...]
        d[...] = g[...] + ratio * d[...]
        hg[...] = hg[...] - step * hal[it]
        hd[...] = hg[...] + ratio * hd[...]
        if it == ITERS - 1:
            ycopy(0).start()
            ycopy(1).start()
        return step, ratio

    def first_hook():
        clear()

    def first_late():
        for h in range(2):
            rs = pl.ds(h * (rows // 2), rows // 2)
            rcopy(gbuf.at[rs], gpar.at[rs], (sem_out.at[3], sem_g.at[h]), at(obs, partner)).wait_recv()

            @pl.loop(h * nblk // 2, (h + 1) * nblk // 2)
            def _(i):
                put_green(gpar, i, other)

    def put_operand(ref, i):
        top, bot = both(ref[pl.ds(pl.multiple_of(i * BAND, BAND), BAND), :])
        r0 = pl.multiple_of(i * 2 * BAND, 2 * BAND)
        put_cat(cat_d, r0, top, True)
        put_cat(cat_d, pl.multiple_of(r0 + BAND, BAND), bot, True)

    def first_finish(j, x):
        r0 = pl.multiple_of(j * R, R)
        g[pl.ds(r0, R), :] = x
        d[pl.ds(r0, R), :] = x

        @pl.when(j % per == per - 1)
        def _():
            put_operand(g, j // per)

    backward(0, first_hook, first_late, first_finish)
    forward(0, lambda: None, lambda: pl.when(c == 1)(build_laplace), first)
    for it in range(1, ITERS):
        def hook(it=it):
            forward_sent(it - 1)

            @pl.when(inner)
            def _():
                reg_work(it - 1)

        def finish(j, x):
            r0 = pl.multiple_of(j * R, R)
            a[pl.ds(r0, R), :] = x + wown[pl.ds(r0, R), :]

            @pl.when(j % per == per - 1)
            def _():
                put_operand(a, j // per)

        backward(it, hook, functools.partial(reg_end, it - 1), finish)
        forward(it, functools.partial(dots, it - 1), lambda: None, functools.partial(advance, it))

    last = ITERS - 1
    norm = norms[-1]
    mid = (z == za) | (z == zb)

    def zcopy(i):
        q = zpeer(i)
        return rcopy(sq, zsq.at[z - za], (sem_zs.at[0], sem_p.at[2 + z - za]), at(obs, q * 2 + c))

    def zwait(slot):
        rcopy(sq, zsq.at[slot], (sem_zs.at[0], sem_p.at[2 + slot]), at(obs, partner)).wait_recv()

    @pl.when(mid)
    def _():
        zsq[z - za] = sq[...]

        @pl.loop(1, nz)
        def _(i):
            zcopy(i).start()

    reg_sums()

    @pl.when(z != za)
    def _():
        zwait(0)

    @pl.when(z != zb)
    def _():
        zwait(1)

    pls[...] = zsq[0] + zsq[1]
    plr[obs * 2 + c] = pls[...]

    @pl.loop(1, n_plane)
    def _(i):
        pcopy(i).start()

    tsrc[0:1, :] = norm
    tsrc[1:2, :] = rowsum(sums_end(last))
    tcopy.start()

    last_sent()

    @pl.when(mid)
    def _():
        part = scr.at[last, pl.ds(0, nz - 1)]
        rcopy(part, part, (sem_zs.at[0], sem_p.at[2]), at(obs, partner)).wait_send()

    ncopy.wait_send()
    rcopy(gbuf, gpar, (sem_out.at[3], sem_g.at[0]), at(obs, partner)).wait_send()
    rcopy(nat, natp, (sem_out.at[9], sem_x.at[0]), at(obs, partner)).wait_send()
    ycopy(0).wait_recv()
    ycopy(1).wait_recv()
    ycopy(0).wait_send()
    ycopy(1).wait_send()
    for i in range(CB):
        blk = slice(i * BAND, (i + 1) * BAND)
        m = mine(BAND)
        slip[blk, :] = jnp.where(m, slip[blk, :], roll(slp[blk, :]))
        d[blk, :] = jnp.where(m, d[blk, :], roll(dp[blk, :]))
    tcopy.wait_recv()
    tcopy.wait_send()

    part = plr.at[pl.ds(0, n_plane - 1)]
    rcopy(part, part, (sem_p.at[0], sem_p.at[1]), at(obs, partner)).wait_recv()

    def step_of(t, q):
        return t[0:1, :] / (fold(sum(rowsum(plr[2 * o + q]) for o in range(n_obs))) + t[1:2, :])

    step = jnp.where(mine(1), step_of(tsrc, c), step_of(tdst, other))

    out[...] = slip[...] + step * d[...]

    rcopy(part, part, (sem_p.at[0], sem_p.at[1]), at(obs, partner)).wait_send()


def shards(green, data, neighbours, reg_weight):
    rows, cols = green.shape
    E = data.shape[1]
    n_obs, n_patch = lax.axis_size("obs"), lax.axis_size("patch")
    nbit = n_obs.bit_length() - 1
    nz = n_patch // 2
    nc, bc = rows // 2 // R, cols // R
    NB = 2 * cols // BAND
    nblk = rows // BAND
    V = pltpu.VMEM
    D = pltpu.SemaphoreType.DMA
    scratch = [
        V((rows, cols), F32), V((rows, cols), F32), V((rows, E), F32),
        V((rows, 2 * cols), BF16), V((rows, 2 * cols), BF16),
        V(neighbours.shape, jnp.int32), V(neighbours.shape, jnp.int32), V((8, (NB + 4) * BAND), jnp.int32), V((1, E), F32),
        V((NB * BAND, 3 * BAND), BF16), V(((NB + 2) * BAND, 3 * BAND), BF16),
        V((2 * cols, 3 * E), BF16), V(((NB + 2) * BAND, 2 * E), BF16), V(((NB + 4) * BAND, 2 * E), BF16),
        V((E, rows), BF16), V((2 * E, rows), BF16),
        V((cols, E), F32), V((cols, E), F32), V((cols, E), F32), V((cols, E), F32), V((ITERS - 1, 2, HB, E), F32),
        V((cols, E), F32), V((cols, E), F32), V((cols, E), F32), V((8, E), F32),
        V((ITERS, 2, HB, E), F32), V((2, HB, E), F32), V((2, HB, E), F32), V((nc, R, E), F32), V((nc, R, E), F32),
        V((nc, R, E), F32), V((nc, R, E), F32), V((nc, R, E), F32),
        V((ITERS, nc, R, E), F32), V((ITERS, nc, R, E), F32),
        V((ITERS, nbit, bc, R, E), F32), V((ITERS, nbit, bc, R, E), F32),
        V((cols // BAND, BAND, E), F32), V((cols // BAND, BAND, E), F32),
        V((ITERS, 2, HB, E), F32), V((ITERS - 1, 2, HB, E), F32),
        V((ITERS, 8, E), F32), V((ITERS, nz, 8, E), F32),
        V((2, 8, E), F32), V((8, E), F32), V((2 * n_obs, 8, E), F32), V((8, E), F32), V((8, E), F32),
        D((10,)), D((2, nc)), D((2, nc)), D((2, nbit, bc)), D((2, 2)), D((ITERS - 1, 2)),
        D((ITERS,)), D((4,)), D((cols // BAND,)), D((2, 3)), D((2,)), D((2,)), D((rows // (2 * BAND) + 3,)), D((1,)),
    ]
    return pl.pallas_call(
        functools.partial(kernel, n_obs, n_patch, nc, bc),
        out_shape=pltpu.VMEM((cols, E), F32),
        in_specs=[pl.BlockSpec(memory_space=pl.ANY)] * 4,
        out_specs=pl.BlockSpec(memory_space=pltpu.VMEM),
        scratch_shapes=scratch,
        compiler_params=pltpu.CompilerParams(
            collective_id=0, has_side_effects=True, vmem_limit_bytes=56 * 1024 * 1024),
    )(green, data, neighbours, reg_weight.reshape(1, E))


def solution(mesh):
    in_specs = (P("obs", "patch"), P("obs", None), P(None, "patch"), P())
    return jax.shard_map(shards, mesh=mesh, in_specs=in_specs, out_specs=P("patch", None), check_vma=False)
```

```python
import functools

import jax
import jax.numpy as jnp
from jax import lax
from jax.experimental import pallas as pl
from jax.experimental.pallas import tpu as pltpu
from jax.sharding import PartitionSpec as P

BAND = 128
ITERS = 3
MESH = pl.DeviceIdType.MESH
F32 = jnp.float32
BF16 = jnp.bfloat16
R = 64
HB = BAND // 2
LAG = 8


def dot(a, b):
    return lax.dot_general(a, b, (((1,), (0,)), ((), ())), preferred_element_type=F32)


def split(x):
    hi = x.astype(BF16)
    return hi, (x - hi.astype(F32)).astype(BF16)


def batches(n):
    return [[0]] + [list(range(i, min(i + 2, n))) for i in range(1, n, 2)]


def rowsum(x):
    return jnp.sum(x, axis=0, keepdims=True)


def kernel(n_obs, n_patch, nc, bc, green, data, nb_in, rw_in, out,
           gbuf, gpar, dbuf, ghi, glo, nb, nbp, nbe, rw, lm, lmt,
           cat_d, cat_e, cat_u, lt, lt0,
           d, g, a, wown, wsrc, slip, slp, dp, sq, hsrc, hd, hg, qd, qg,
           s, sr, sl, rl, rr, bb, br, nat, natp, hal, wr, scs, scr, zsq, pls, plr, tsrc, tdst, acc_f, acc_b,
           sem_out, sem_l, sem_r, sem_b, sem_h, sem_w, sem_s, sem_p, sem_x, sem_y, sem_g, sem_nb, sem_in, sem_zs):
    rows, cols = gbuf.shape
    E = dbuf.shape[1]
    H = E // 2
    CB = cols // BAND
    NB = 2 * CB
    RB = rows // (2 * BAND)
    nblk = rows // BAND
    per = BAND // R
    nz = n_patch // 2
    nbit = n_obs.bit_length() - 1
    obs = lax.axis_index("obs")
    pat = lax.axis_index("patch")
    z = pat // 2
    c = pat % 2
    other = 1 - c
    partner = z * 2 + other
    has_l, has_r = z > 0, z < nz - 1
    up, down = has_r, has_l
    inner = up & down
    n_plane = 2 * n_obs
    za, zb = nz // 2 - 1, nz // 2

    def lanes(n):
        return lax.broadcasted_iota(jnp.int32, (n, E), 1)

    def low(n):
        return lanes(n) < H

    def mine(n):
        i = lanes(n) - c * H
        return (i >= 0) & (i < H)

    def roll(x):
        return pltpu.roll(x, H, 1)

    def both(x):
        q = roll(x)
        m = low(x.shape[0])
        return jnp.where(m, x, q), jnp.where(m, q, x)

    def fold(x):
        return x + roll(x)

    def put_cat(ref, r0, v, third=False):
        n = v.shape[0]
        hi = v.astype(BF16)
        hf = hi.astype(F32)
        lf = v - hf
        m = low(n)
        ref[pl.ds(r0, n), 0:E] = jnp.where(m, hf, lf).astype(BF16)
        ref[pl.ds(r0, n), E:2 * E] = jnp.where(m, lf, hf).astype(BF16)
        if third:
            ref[pl.ds(r0, n), 2 * E:3 * E] = hi

    def rcopy(src, dst, sems, dev):
        return pltpu.make_async_remote_copy(
            src_ref=src, dst_ref=dst, send_sem=sems[0], recv_sem=sems[1],
            device_id=dev, device_id_type=MESH)

    def pair(sem, *idx):
        return sem.at[(0,) + idx], sem.at[(1,) + idx]

    def at(o, q):
        return (o, q)

    def plane(i):
        q = (obs * 2 + c + i) % n_plane
        return q // 2, z * 2 + q % 2

    def zpeer(i):
        return (z + i) % nz

    def load(i):
        rs = pl.ds(pl.multiple_of(i * 2 * BAND, 2 * BAND), 2 * BAND)
        return pltpu.make_async_copy(green.at[rs], gbuf.at[rs], sem_in.at[i])

    load_data = pltpu.make_async_copy(data, dbuf, sem_in.at[RB])
    load_nb = pltpu.make_async_copy(nb_in, nb, sem_in.at[RB + 1])
    load_rw = pltpu.make_async_copy(rw_in, rw, sem_in.at[RB + 2])
    load_data.start()

    @pl.loop(0, RB)
    def _(i):
        load(i).start()

    load_nb.start()
    load_rw.start()

    barrier = pltpu.get_barrier_semaphore()

    @pl.loop(1, nz)
    def _(i):
        pl.semaphore_signal(barrier, inc=1, device_id=at(obs, zpeer(i) * 2 + c), device_id_type=MESH)

    @pl.loop(1, n_plane)
    def _(i):
        pl.semaphore_signal(barrier, inc=1, device_id=plane(i), device_id_type=MESH)

    load_data.wait()

    for i in range(nblk):
        r0 = i * BAND
        hi, lo = split(dbuf[r0:r0 + BAND, :].T)
        lt0[0:E, r0:r0 + BAND] = hi
        lt0[E:2 * E, r0:r0 + BAND] = lo

    def put_green(src, i, core):
        r0 = pl.multiple_of(i * BAND, BAND)
        hi, lo = split(src[pl.ds(r0, BAND), :])
        for j in range(CB):
            c0 = pl.multiple_of((2 * j + core) * BAND, BAND)
            ghi[pl.ds(r0, BAND), pl.ds(c0, BAND)] = hi[:, j * BAND:(j + 1) * BAND]
            glo[pl.ds(r0, BAND), pl.ds(c0, BAND)] = lo[:, j * BAND:(j + 1) * BAND]

    @pl.loop(0, RB)
    def _(i):
        load(i).wait()
        put_green(gbuf, 2 * i, c)
        put_green(gbuf, 2 * i + 1, c)

    load_nb.wait()
    load_rw.wait()
    wrow = rw[...]
    weight = jnp.where(mine(1), wrow, roll(wrow))

    ncopy = rcopy(nb, nbp, (sem_nb.at[0], sem_nb.at[1]), at(obs, partner))
    def gcopy(i):
        rs = pl.ds(i * BAND, BAND)
        return rcopy(gbuf.at[rs], gpar.at[rs], (sem_out.at[3], sem_g.at[i // (nblk // 2)]), at(obs, partner))

    def build_laplace():
        ncopy.wait_recv()
        zero_u = jnp.zeros((2 * BAND, 2 * E), BF16)
        cat_u[0:2 * BAND, :] = zero_u
        cat_u[(NB + 2) * BAND:(NB + 4) * BAND, :] = zero_u
        nbe[...] = jnp.full(nbe.shape, -(2 ** 24), jnp.int32)
        base = z * (2 * cols)
        own0 = pl.multiple_of((2 + c * CB) * BAND, BAND)
        par0 = pl.multiple_of((2 + other * CB) * BAND, BAND)
        nbe[0:3, pl.ds(own0, cols)] = nb[...] - base
        nbe[0:3, pl.ds(par0, cols)] = nbp[...] - base
        K = 3 * BAND

        for j in range(NB + 2):
            r0 = j * BAND
            col = lax.broadcasted_iota(jnp.int32, (BAND, K), 0) + (j - 1) * BAND
            own = lax.broadcasted_iota(jnp.int32, (BAND, K), 1) + (j - 2) * BAND
            m = jnp.where(col == own, 4.0, 0.0)
            for k in range(3):
                m = m - jnp.where(col == nbe[k:k + 1, pl.ds(r0, K)], 1.0, 0.0)
            lmt[pl.ds(r0, BAND), :] = m.astype(BF16)

        for b in range(NB):
            r0, n0 = b * BAND, (b + 2) * BAND
            row = lax.broadcasted_iota(jnp.int32, (BAND, K), 0) + b * BAND
            col = lax.broadcasted_iota(jnp.int32, (BAND, K), 1) + (b - 1) * BAND
            m = jnp.where(col == row, 4.0, 0.0)
            t = nbe[0:8, pl.ds(n0, BAND)].T
            for k in range(3):
                m = m - jnp.where(col == t[:, k:k + 1], 1.0, 0.0)
            lm[pl.ds(r0, BAND), :] = m.astype(BF16)

    def clear():
        scs[...] = jnp.zeros((ITERS, 8, E), F32)
        zero_c = jnp.zeros((nc, R, E), F32)
        zero_h = jnp.zeros((HB, E), F32)

        @pl.when(z == 0)
        def _():
            for it in range(ITERS):
                rl[it] = zero_c
                hal[it, 0] = zero_h
            for it in range(ITERS - 1):
                wr[it, 0] = zero_h

        @pl.when(z == nz - 1)
        def _():
            for it in range(ITERS):
                rr[it] = zero_c
                hal[it, 1] = zero_h
            for it in range(ITERS - 1):
                wr[it, 1] = zero_h

    def bit_partner(p, j):
        b0, b1 = 1 << p, 1 << (nbit - 1 - p)
        bit = b0 + (j % 2) * (b1 - b0)
        return at(obs + bit * (1 - 2 * ((obs // bit) % 2)), pat)

    def bcopy(b, p, j):
        return rcopy(bb.at[b, p, j], br.at[b, p, j], (sem_out.at[2], sem_b.at[b % 2, p, j]), bit_partner(p, j))

    def product(b, m):
        if b == 0:
            c0 = pl.multiple_of((2 * m + c) * BAND, BAND)
            y = dot(lt0[...], ghi[:, pl.ds(c0, BAND)])
            y = y[:E] + y[E:] + dot(lt0[0:E, :], glo[:, pl.ds(c0, BAND)])
            return y.T
        c0 = m * 2 * BAND
        if m == 0:
            y = acc_b[...] + part_b(RB - 1)
        else:
            y = dot(lt[...], ghi[:, c0:c0 + 2 * BAND])
            y = y[:H] + y[H:] + dot(lt[0:H, :], glo[:, c0:c0 + 2 * BAND])
        return jnp.concatenate([y[:, :BAND], y[:, BAND:]], axis=0).T

    def xcopy(m):
        return rcopy(nat.at[m], natp.at[m], (sem_out.at[9], sem_x.at[m]), at(obs, partner))

    def enter():
        pl.semaphore_wait(barrier, nz - 1 + n_plane - 1)
        ncopy.start()
        gcopy(0).start()

    def backward(b, hook, late, finish):
        for ms in batches(CB) if b else ([0, 1], range(2, CB)):
            for m in ms:
                y = product(b, m)
                if b == 0:
                    nat[m] = y
                else:
                    bb[b, 0, m * per:(m + 1) * per] = y.reshape(per, R, E)
            if b == 0 and ms[0] == 0:
                enter()
            for m in ms:
                if b == 0:
                    xcopy(m).start()
                else:
                    for k in range(per):
                        bcopy(b, 0, m * per + k).start()

        if b == 0:
            for i in range(1, nblk):
                gcopy(i).start()
            pl.when(c == 0)(build_laplace)
            for m in range(CB):
                xcopy(m).wait_recv()
                y = jnp.where(mine(BAND), nat[m], roll(natp[m]))
                bb[b, 0, m * per:(m + 1) * per] = y.reshape(per, R, E)
                for k in range(per):
                    bcopy(b, 0, m * per + k).start()

        hook()
        for p in range(1, nbit):
            @pl.loop(0, bc)
            def _(j):
                bcopy(b, p - 1, j).wait_recv()
                bb[b, p, j] = bb[b, p - 1, j] + br[b, p - 1, j]
                bcopy(b, p, j).start()

        acc_f[...] = jnp.zeros(acc_f.shape, F32)
        late()

        @pl.loop(0, bc)
        def _(j):
            bcopy(b, nbit - 1, j).wait_recv()
            finish(j, bb[b, nbit - 1, j] + br[b, nbit - 1, j])

    def backward_sent(b):
        rcopy(bb.at[b], br.at[b], (sem_out.at[2], sem_b.at[0, 0, 0]), at(obs, partner)).wait_send()

    def rcopy_up(it, src, k):
        return rcopy(src.at[k], rl.at[it, k], (sem_out.at[0], sem_l.at[it % 2, k]), at(obs, pat + 2))

    def rcopy_down(it, src, k):
        return rcopy(src.at[k], rr.at[it, k], (sem_out.at[1], sem_r.at[it % 2, k]), at(obs, pat - 2))

    def hcopy_r(it):
        return rcopy(hsrc.at[it, 0], hal.at[it, 0], (sem_out.at[4], sem_h.at[it % 2, 0]), at(obs, pat + 2))

    def hcopy_l(it):
        return rcopy(hsrc.at[it, 1], hal.at[it, 1], (sem_out.at[5], sem_h.at[it % 2, 1]), at(obs, pat - 2))

    def part_b(m):
        ks = pl.ds(pl.multiple_of(m * 2 * BAND, 2 * BAND), 2 * BAND)
        y = dot(lt[:, ks], ghi[ks, 0:2 * BAND])
        return y[:H] + y[H:] + dot(lt[0:H, ks], glo[ks, 0:2 * BAND])

    def put_lt(m):
        x = qd[pl.ds(m * per, per)].reshape(BAND, E)
        hi, lo = split(x.T)
        o0 = pl.multiple_of(m * 2 * BAND, 2 * BAND)
        o1 = pl.multiple_of(m * 2 * BAND + BAND, BAND)
        lt[0:H, pl.ds(o0, BAND)] = hi[:H]
        lt[H:E, pl.ds(o0, BAND)] = lo[:H]
        lt[0:H, pl.ds(o1, BAND)] = hi[H:]
        lt[H:E, pl.ds(o1, BAND)] = lo[H:]

        @pl.when(m < RB - 1)
        def _():
            acc_b[...] += part_b(m)

    def part_f(it, i):
        m = jnp.where((it == ITERS - 1) & (z <= za), RB - 1, 0) if it == ITERS - 1 else 0
        rs = pl.ds(pl.multiple_of(m * 2 * BAND, 2 * BAND), 2 * BAND) if it == ITERS - 1 else slice(0, 2 * BAND)
        ks = pl.ds(pl.multiple_of(i * 2 * BAND, 2 * BAND), 2 * BAND)
        y = dot(ghi[rs, ks], cat_d[ks, 0:2 * E])
        return y[:, :E] + y[:, E:] + dot(glo[rs, ks], cat_d[ks, 2 * E:3 * E])

    def forward(it, sums, after, hook):
        last = it == ITERS - 1
        v = a if it else g
        x = v[cols - BAND:cols, :]
        hsrc[it, 0] = jnp.where(low(HB), roll(x[:HB]), x[HB:])
        x = v[0:BAND, :]
        hsrc[it, 1] = jnp.where(low(HB), x[:HB], roll(x[HB:]))

        @pl.when(up & down)
        def _():
            hcopy_r(it).start()
            hcopy_l(it).start()

        if last:
            forward_last(sums, hook)
            return

        acc_b[...] = jnp.zeros(acc_b.shape, F32)

        def group(m):
            r0 = m * 2 * BAND
            if m == 0:
                y = acc_f[...] + part_f(it, CB - 1)
            else:
                y = dot(ghi[r0:r0 + 2 * BAND, :], cat_d[:, 0:2 * E])
                y = y[:, :E] + y[:, E:] + dot(glo[r0:r0 + 2 * BAND, :], cat_d[:, 2 * E:3 * E])
            y = jnp.where(low(BAND), y[:BAND], y[BAND:])
            s[m * per:(m + 1) * per] = y.reshape(per, R, E)

        def send(ms):
            @pl.when(z == 0)
            def _():
                for k in range(ms[0] * per, (ms[-1] + 1) * per):
                    rcopy_up(it, s, k).start()

            @pl.when(z == nz - 1)
            def _():
                for k in range(ms[0] * per, (ms[-1] + 1) * per):
                    rcopy_down(it, s, k).start()

        group(0)
        send([0])
        sums()

        @pl.when(up & (z == 0))
        def _():
            hcopy_r(it).start()

        @pl.when(down & (z == nz - 1))
        def _():
            hcopy_l(it).start()

        for ms in batches(RB)[1:]:
            for m in ms:
                group(m)
            send(ms)
        after()
        backward_sent(it)

        def chain(t, ends=True):
            kl = t - LAG * z
            kr = t - LAG * (nz - 1 - z)
            kt = t - LAG * jnp.maximum(z, nz - 1 - z)

            @pl.when(down & (kl >= 0) & (kl < nc))
            def _():
                rcopy_up(it, sr, kl).wait_recv()

                @pl.when(up)
                def _():
                    sr[kl] = rl[it, kl] + s[kl]
                    rcopy_up(it, sr, kl).start()

            @pl.when(up & (kr >= 0) & (kr < nc))
            def _():
                rcopy_down(it, sl, kr).wait_recv()

                @pl.when(down)
                def _():
                    sl[kr] = rr[it, kr] + s[kr]
                    rcopy_down(it, sl, kr).start()

            if not ends:
                return

            @pl.when((kt >= 0) & (kt < nc))
            def _():
                total = rl[it, kt] + s[kt] + rr[it, kt]
                if it:
                    step, ratio = scalars
                    rest = qg[kt] - step * total
                    total = rest + ratio * qd[kt]
                qg[kt] = rest if it else total
                qd[kt] = total

                @pl.when(kt % per == per - 1)
                def _():
                    put_lt(kt // per)

        pl.loop(LAG, LAG * (nz // 2))(functools.partial(chain, ends=False))
        scalars = hook()

        @pl.when(jnp.logical_not(inner))
        def _():
            reg_work(it)

        pl.loop(LAG * (nz // 2), nc + LAG * (nz - 1))(chain)

    def forward_last(sums, hook):
        it = ITERS - 1
        low_side = z <= za

        def order(i, n):
            return jnp.where(low_side, n - 1 - i, i)

        def group(i):
            m = order(i, RB)
            rs = pl.ds(pl.multiple_of(m * 2 * BAND, 2 * BAND), 2 * BAND)
            if i == 0:
                y = acc_f[...] + part_f(it, CB - 1)
            else:
                y = dot(ghi[rs, :], cat_d[:, 0:2 * E])
                y = y[:, :E] + y[:, E:] + dot(glo[rs, :], cat_d[:, 2 * E:3 * E])
            y = jnp.where(low(BAND), y[:BAND], y[BAND:])
            s[pl.ds(m * per, per)] = y.reshape(per, R, E)

        def send(ms):
            for i in range(ms[0] * per, (ms[-1] + 1) * per):
                k = order(i, nc)

                @pl.when((z == 0) & ((z < za) | (k >= nc // 2)))
                def _():
                    rcopy_up(it, s, k).start()

                @pl.when((z == nz - 1) & ((z > zb) | (k < nc // 2)))
                def _():
                    rcopy_down(it, s, k).start()

        group(0)
        send([0])
        sums()

        @pl.when(up & (z == 0))
        def _():
            hcopy_r(it).start()

        @pl.when(down & (z == nz - 1))
        def _():
            hcopy_l(it).start()

        for ms in batches(RB)[1:]:
            for i in ms:
                group(i)
            send(ms)
        backward_sent(it)
        sq[...] = jnp.zeros((8, E), F32)

        def move(n0, n1):
            @pl.loop(n0, n1)
            def _(i):
                k = order(i, nc)

                @pl.when(low_side & down)
                def _():
                    rcopy_up(it, sr, k).wait_recv()

                    @pl.when((z < za) | (k >= nc // 2))
                    def _():
                        sr[k] = rl[it, k] + s[k]
                        rcopy_up(it, sr, k).start()

                @pl.when(jnp.logical_not(low_side) & up)
                def _():
                    rcopy_down(it, sl, k).wait_recv()

                    @pl.when((z > zb) | (k < nc // 2))
                    def _():
                        sl[k] = rr[it, k] + s[k]
                        rcopy_down(it, sl, k).start()

        half = nc - nc // 2
        move(0, half)
        step, ratio = hook()
        move(half, nc)

        def ends(k):
            total = rl[it, k] + s[k] + rr[it, k]
            total = qg[k] - step * total + ratio * qd[k]
            sq[...] += jnp.sum((total * total).reshape(R // 8, 8, E), axis=0)

        @pl.when(z == za)
        def _():
            @pl.loop(0, nc // 2)
            def _(k):
                rcopy_down(it, sl, k).wait_recv()
                ends(k)

        @pl.when(z == zb)
        def _():
            @pl.loop(nc // 2, nc)
            def _(k):
                rcopy_up(it, sr, k).wait_recv()
                ends(k)

    def last_sent():
        it = ITERS - 1

        def wait(buf, sem, n):
            part = buf.at[pl.ds(0, n)]
            rcopy(part, part, (sem, sem_p.at[2]), at(obs, partner)).wait_send()

        @pl.when(z < za)
        def _():
            wait(sr, sem_out.at[0], nc)

        @pl.when(z == za)
        def _():
            wait(sr, sem_out.at[0], nc - nc // 2)

        @pl.when(z == zb)
        def _():
            wait(sl, sem_out.at[1], nc // 2)

        @pl.when(z > zb)
        def _():
            wait(sl, sem_out.at[1], nc)

        @pl.when(up)
        def _():
            hcopy_r(it).wait_send()

        @pl.when(down)
        def _():
            hcopy_l(it).wait_send()

    def forward_sent(it):
        @pl.when(up)
        def _():
            rcopy(sr, rl.at[it], (sem_out.at[0], sem_l.at[0, 0]), at(obs, partner)).wait_send()

        @pl.when(down)
        def _():
            rcopy(sl, rr.at[it], (sem_out.at[1], sem_r.at[0, 0]), at(obs, partner)).wait_send()

        @pl.when(up)
        def _():
            hcopy_r(it).wait_send()

        @pl.when(down)
        def _():
            hcopy_l(it).wait_send()

    def halo_wait(it):
        @pl.when(has_l)
        def _():
            hcopy_r(it).wait_recv()

        @pl.when(has_r)
        def _():
            hcopy_l(it).wait_recv()

    def widen(x):
        top, bot = both(x)
        return jnp.concatenate([top, bot], axis=0)

    def laplace():
        put_cat(cat_e, 0, widen(hd[0]))
        put_cat(cat_e, (NB + 1) * BAND, widen(hd[1]))

        for i in range(CB):
            top, bot = both(d[i * BAND:(i + 1) * BAND, :])
            put_cat(cat_e, (i + 1) * BAND, top)
            put_cat(cat_e, (CB + i + 1) * BAND, bot)

    def banded(mat, vec, j):
        r0 = j * BAND
        y = dot(mat[r0:r0 + BAND, :], vec[r0:r0 + 3 * BAND, :])
        return y[:, :E] + y[:, E:]

    def lap_rows(i):
        return weight * jnp.where(low(BAND), banded(lm, cat_e, i), banded(lm, cat_e, CB + i))

    def wcopy_l(it):
        return rcopy(wsrc.at[it, 0], wr.at[it, 1], (sem_out.at[7], sem_w.at[it, 1]), at(obs, pat - 2))

    def wcopy_r(it):
        return rcopy(wsrc.at[it, 1], wr.at[it, 0], (sem_out.at[6], sem_w.at[it, 0]), at(obs, pat + 2))

    def reg_work(it):
        laplace()

        for i in range(CB):
            top, bot = both(lap_rows(i))
            put_cat(cat_u, (i + 2) * BAND, top)
            put_cat(cat_u, (CB + i + 2) * BAND, bot)

        for side, j in ((0, 0), (1, NB + 1)):
            y = banded(lmt, cat_u, j)
            wsrc[it, side] = weight * jnp.where(low(HB), y[:HB], y[HB:])

        @pl.when(has_l)
        def _():
            wcopy_l(it).start()

        @pl.when(has_r)
        def _():
            wcopy_r(it).start()

        for i in range(CB):
            y = jnp.where(low(BAND), banded(lmt, cat_u, i + 1), banded(lmt, cat_u, CB + i + 1))
            wown[i * BAND:(i + 1) * BAND, :] = weight * y

    def reg_sums():
        last = ITERS - 1
        laplace()
        for i in range(CB):
            u = lap_rows(i)
            scs[last] += jnp.sum((u * u).reshape(BAND // 8, 8, E), axis=0)
        sums_start(last)

    def reg_end(it):
        @pl.when(has_l)
        def _():
            wcopy_r(it).wait_recv()

        @pl.when(has_r)
        def _():
            wcopy_l(it).wait_recv()

        wown[0:BAND, :] += jnp.where(low(BAND), widen(wr[it, 0]), 0.0)
        wown[cols - BAND:cols, :] += jnp.where(low(BAND), 0.0, widen(wr[it, 1]))
        reg_sent(it)

    def reg_sent(it):
        @pl.when(has_l)
        def _():
            wcopy_l(it).wait_send()

        @pl.when(has_r)
        def _():
            wcopy_r(it).wait_send()

    def scopy(it, q):
        return rcopy(scs.at[it], scr.at[it, z], (sem_out.at[8], sem_s.at[it]), at(obs, q * 2 + c))

    def sums_all(it):
        part = scr.at[it, pl.ds(0, nz - 1)]
        return rcopy(part, part, (sem_out.at[8], sem_s.at[it]), at(obs, partner))

    def sums_start(it):
        scr[it, z] = scs[it]

        @pl.loop(1, nz)
        def _(i):
            scopy(it, zpeer(i)).start()

    def sums_end(it):
        sums_all(it).wait_recv()
        sums_all(it).wait_send()
        return fold(jnp.sum(scr[it], axis=0))

    def pcopy(i):
        po, pp = plane(i)
        return rcopy(pls, plr.at[obs * 2 + c], (sem_p.at[0], sem_p.at[1]), (po, pp))

    norms = []

    def dots(it):
        gv, dv, av = g[...], d[...], a[...]
        scs[it, 0:1, :] = rowsum(gv * gv)
        scs[it, 1:2, :] = rowsum(dv * av)
        scs[it, 2:3, :] = rowsum(gv * av)
        scs[it, 3:4, :] = rowsum(av * av)
        sums_start(it)

    def first():
        halo_wait(0)
        hg[...] = hal[0]
        hd[...] = hal[0]

    def ycopy(i):
        return rcopy((slip, d)[i], (slp, dp)[i], pair(sem_y, i), at(obs, partner))

    tcopy = rcopy(tsrc, tdst, pair(sem_y, 2), at(obs, partner))

    def advance(it):
        tot = sums_end(it - 1)
        if it == 1:
            norms.append(tot[0:1])
        norm = norms[-1]
        step = norm / tot[1:2]
        after = norm - 2.0 * step * tot[2:3] + step * step * tot[3:4]
        ratio = after / norm
        norms.append(after)
        halo_wait(it)
        if it == 1:
            slip[...] = step * d[...]
        else:
            slip[...] += step * d[...]
        g[...] = g[...] - step * a[...]
        d[...] = g[...] + ratio * d[...]
        hg[...] = hg[...] - step * hal[it]
        hd[...] = hg[...] + ratio * hd[...]
        if it == ITERS - 1:
            ycopy(0).start()
            ycopy(1).start()
        return step, ratio

    def first_hook():
        clear()

    def first_late():
        for h in range(2):
            rs = pl.ds(h * (rows // 2), rows // 2)
            rcopy(gbuf.at[rs], gpar.at[rs], (sem_out.at[3], sem_g.at[h]), at(obs, partner)).wait_recv()

            @pl.loop(h * nblk // 2, (h + 1) * nblk // 2)
            def _(i):
                put_green(gpar, i, other)

    def put_operand(ref, i, it):
        top, bot = both(ref[pl.ds(pl.multiple_of(i * BAND, BAND), BAND), :])
        r0 = pl.multiple_of(i * 2 * BAND, 2 * BAND)
        put_cat(cat_d, r0, top, True)
        put_cat(cat_d, pl.multiple_of(r0 + BAND, BAND), bot, True)

        @pl.when(i < CB - 1)
        def _():
            acc_f[...] += part_f(it, i)

    def first_finish(j, x):
        r0 = pl.multiple_of(j * R, R)
        g[pl.ds(r0, R), :] = x
        d[pl.ds(r0, R), :] = x

        @pl.when(j % per == per - 1)
        def _():
            put_operand(g, j // per, 0)

    backward(0, first_hook, first_late, first_finish)
    forward(0, lambda: None, lambda: pl.when(c == 1)(build_laplace), first)
    for it in range(1, ITERS):
        def hook(it=it):
            forward_sent(it - 1)

            @pl.when(inner)
            def _():
                reg_work(it - 1)

        def finish(j, x, it=it):
            r0 = pl.multiple_of(j * R, R)
            a[pl.ds(r0, R), :] = x + wown[pl.ds(r0, R), :]

            @pl.when(j % per == per - 1)
            def _():
                put_operand(a, j // per, it)

        backward(it, hook, functools.partial(reg_end, it - 1), finish)
        forward(it, functools.partial(dots, it - 1), lambda: None, functools.partial(advance, it))

    last = ITERS - 1
    norm = norms[-1]
    mid = (z == za) | (z == zb)

    def zcopy(i):
        q = zpeer(i)
        return rcopy(sq, zsq.at[z - za], (sem_zs.at[0], sem_p.at[2 + z - za]), at(obs, q * 2 + c))

    def zwait(slot):
        rcopy(sq, zsq.at[slot], (sem_zs.at[0], sem_p.at[2 + slot]), at(obs, partner)).wait_recv()

    @pl.when(mid)
    def _():
        zsq[z - za] = sq[...]

        @pl.loop(1, nz)
        def _(i):
            zcopy(i).start()

    reg_sums()

    @pl.when(z != za)
    def _():
        zwait(0)

    @pl.when(z != zb)
    def _():
        zwait(1)

    pls[...] = zsq[0] + zsq[1]
    plr[obs * 2 + c] = pls[...]

    @pl.loop(1, n_plane)
    def _(i):
        pcopy(i).start()

    tsrc[0:1, :] = norm
    tsrc[1:2, :] = rowsum(sums_end(last))
    tcopy.start()

    last_sent()

    @pl.when(mid)
    def _():
        part = scr.at[last, pl.ds(0, nz - 1)]
        rcopy(part, part, (sem_zs.at[0], sem_p.at[2]), at(obs, partner)).wait_send()

    ncopy.wait_send()
    rcopy(gbuf, gpar, (sem_out.at[3], sem_g.at[0]), at(obs, partner)).wait_send()
    rcopy(nat, natp, (sem_out.at[9], sem_x.at[0]), at(obs, partner)).wait_send()
    ycopy(0).wait_recv()
    ycopy(1).wait_recv()
    ycopy(0).wait_send()
    ycopy(1).wait_send()
    for i in range(CB):
        blk = slice(i * BAND, (i + 1) * BAND)
        m = mine(BAND)
        slip[blk, :] = jnp.where(m, slip[blk, :], roll(slp[blk, :]))
        d[blk, :] = jnp.where(m, d[blk, :], roll(dp[blk, :]))
    tcopy.wait_recv()
    tcopy.wait_send()

    part = plr.at[pl.ds(0, n_plane - 1)]
    rcopy(part, part, (sem_p.at[0], sem_p.at[1]), at(obs, partner)).wait_recv()

    def step_of(t, q):
        return t[0:1, :] / (fold(sum(rowsum(plr[2 * o + q]) for o in range(n_obs))) + t[1:2, :])

    step = jnp.where(mine(1), step_of(tsrc, c), step_of(tdst, other))

    out[...] = slip[...] + step * d[...]

    rcopy(part, part, (sem_p.at[0], sem_p.at[1]), at(obs, partner)).wait_send()


def shards(green, data, neighbours, reg_weight):
    rows, cols = green.shape
    E = data.shape[1]
    n_obs, n_patch = lax.axis_size("obs"), lax.axis_size("patch")
    nbit = n_obs.bit_length() - 1
    nz = n_patch // 2
    nc, bc = rows // 2 // R, cols // R
    NB = 2 * cols // BAND
    nblk = rows // BAND
    V = pltpu.VMEM
    D = pltpu.SemaphoreType.DMA
    scratch = [
        V((rows, cols), F32), V((rows, cols), F32), V((rows, E), F32),
        V((rows, 2 * cols), BF16), V((rows, 2 * cols), BF16),
        V(neighbours.shape, jnp.int32), V(neighbours.shape, jnp.int32), V((8, (NB + 4) * BAND), jnp.int32), V((1, E), F32),
        V((NB * BAND, 3 * BAND), BF16), V(((NB + 2) * BAND, 3 * BAND), BF16),
        V((2 * cols, 3 * E), BF16), V(((NB + 2) * BAND, 2 * E), BF16), V(((NB + 4) * BAND, 2 * E), BF16),
        V((E, rows), BF16), V((2 * E, rows), BF16),
        V((cols, E), F32), V((cols, E), F32), V((cols, E), F32), V((cols, E), F32), V((ITERS - 1, 2, HB, E), F32),
        V((cols, E), F32), V((cols, E), F32), V((cols, E), F32), V((8, E), F32),
        V((ITERS, 2, HB, E), F32), V((2, HB, E), F32), V((2, HB, E), F32), V((nc, R, E), F32), V((nc, R, E), F32),
        V((nc, R, E), F32), V((nc, R, E), F32), V((nc, R, E), F32),
        V((ITERS, nc, R, E), F32), V((ITERS, nc, R, E), F32),
        V((ITERS, nbit, bc, R, E), F32), V((ITERS, nbit, bc, R, E), F32),
        V((cols // BAND, BAND, E), F32), V((cols // BAND, BAND, E), F32),
        V((ITERS, 2, HB, E), F32), V((ITERS - 1, 2, HB, E), F32),
        V((ITERS, 8, E), F32), V((ITERS, nz, 8, E), F32),
        V((2, 8, E), F32), V((8, E), F32), V((2 * n_obs, 8, E), F32), V((8, E), F32), V((8, E), F32),
        V((2 * BAND, E), F32), V((E // 2, 2 * BAND), F32),
        D((10,)), D((2, nc)), D((2, nc)), D((2, nbit, bc)), D((2, 2)), D((ITERS - 1, 2)),
        D((ITERS,)), D((4,)), D((cols // BAND,)), D((2, 3)), D((2,)), D((2,)), D((rows // (2 * BAND) + 3,)), D((1,)),
    ]
    return pl.pallas_call(
        functools.partial(kernel, n_obs, n_patch, nc, bc),
        out_shape=pltpu.VMEM((cols, E), F32),
        in_specs=[pl.BlockSpec(memory_space=pl.ANY)] * 4,
        out_specs=pl.BlockSpec(memory_space=pltpu.VMEM),
        scratch_shapes=scratch,
        compiler_params=pltpu.CompilerParams(
            collective_id=0, has_side_effects=True, vmem_limit_bytes=56 * 1024 * 1024),
    )(green, data, neighbours, reg_weight.reshape(1, E))


def solution(mesh):
    in_specs = (P("obs", "patch"), P("obs", None), P(None, "patch"), P())
    return jax.shard_map(shards, mesh=mesh, in_specs=in_specs, out_specs=P("patch", None), check_vma=False)
```

```python
import functools

import jax
import jax.numpy as jnp
from jax import lax
from jax.experimental import pallas as pl
from jax.experimental.pallas import tpu as pltpu
from jax.sharding import PartitionSpec as P

BAND = 128
ITERS = 3
MESH = pl.DeviceIdType.MESH
F32 = jnp.float32
BF16 = jnp.bfloat16
R = 64
HB = BAND // 2
LAG = 8


def dot(a, b):
    return lax.dot_general(a, b, (((1,), (0,)), ((), ())), preferred_element_type=F32)


def split(x):
    hi = x.astype(BF16)
    return hi, (x - hi.astype(F32)).astype(BF16)


def batches(n):
    return [[0]] + [list(range(i, min(i + 2, n))) for i in range(1, n, 2)]


def rowsum(x):
    return jnp.sum(x, axis=0, keepdims=True)


def kernel(n_obs, n_patch, nc, bc, green, data, nb_in, rw_in, out,
           gbuf, gpar, dbuf, ghi, glo, nb, nbp, nbe, rw, lm, lmt,
           cat_d, cat_e, cat_u, lt, lt0,
           d, g, a, wown, wsrc, slip, slp, dp, sq, hsrc, hd, hg, qd, qg,
           s, sr, sl, rl, rr, bb, br, nat, natp, hal, wr, scs, scr, zsq, pls, plr, tsrc, tdst, acc_f, acc_b,
           sem_out, sem_l, sem_r, sem_b, sem_h, sem_w, sem_s, sem_p, sem_x, sem_y, sem_g, sem_nb, sem_in, sem_zs):
    rows, cols = gbuf.shape
    E = dbuf.shape[1]
    H = E // 2
    CB = cols // BAND
    NB = 2 * CB
    RB = rows // (2 * BAND)
    nblk = rows // BAND
    per = BAND // R
    nz = n_patch // 2
    nbit = n_obs.bit_length() - 1
    obs = lax.axis_index("obs")
    pat = lax.axis_index("patch")
    z = pat // 2
    c = pat % 2
    other = 1 - c
    partner = z * 2 + other
    has_l, has_r = z > 0, z < nz - 1
    up, down = has_r, has_l
    inner = up & down
    n_plane = 2 * n_obs
    za, zb = nz // 2 - 1, nz // 2

    def lanes(n):
        return lax.broadcasted_iota(jnp.int32, (n, E), 1)

    def low(n):
        return lanes(n) < H

    def mine(n):
        i = lanes(n) - c * H
        return (i >= 0) & (i < H)

    def roll(x):
        return pltpu.roll(x, H, 1)

    def both(x):
        q = roll(x)
        m = low(x.shape[0])
        return jnp.where(m, x, q), jnp.where(m, q, x)

    def fold(x):
        return x + roll(x)

    def put_cat(ref, r0, v, third=False):
        n = v.shape[0]
        hi = v.astype(BF16)
        hf = hi.astype(F32)
        lf = v - hf
        m = low(n)
        ref[pl.ds(r0, n), 0:E] = jnp.where(m, hf, lf).astype(BF16)
        ref[pl.ds(r0, n), E:2 * E] = jnp.where(m, lf, hf).astype(BF16)
        if third:
            ref[pl.ds(r0, n), 2 * E:3 * E] = hi

    def rcopy(src, dst, sems, dev):
        return pltpu.make_async_remote_copy(
            src_ref=src, dst_ref=dst, send_sem=sems[0], recv_sem=sems[1],
            device_id=dev, device_id_type=MESH)

    def pair(sem, *idx):
        return sem.at[(0,) + idx], sem.at[(1,) + idx]

    def at(o, q):
        return (o, q)

    def plane(i):
        q = (obs * 2 + c + i) % n_plane
        return q // 2, z * 2 + q % 2

    def zpeer(i):
        return (z + i) % nz

    def load(i):
        rs = pl.ds(pl.multiple_of(i * 2 * BAND, 2 * BAND), 2 * BAND)
        return pltpu.make_async_copy(green.at[rs], gbuf.at[rs], sem_in.at[i])

    load_data = pltpu.make_async_copy(data, dbuf, sem_in.at[RB])
    load_nb = pltpu.make_async_copy(nb_in, nb, sem_in.at[RB + 1])
    load_rw = pltpu.make_async_copy(rw_in, rw, sem_in.at[RB + 2])
    load_data.start()

    @pl.loop(0, RB)
    def _(i):
        load(i).start()

    load_nb.start()
    load_rw.start()

    barrier = pltpu.get_barrier_semaphore()

    @pl.loop(1, nz)
    def _(i):
        pl.semaphore_signal(barrier, inc=1, device_id=at(obs, zpeer(i) * 2 + c), device_id_type=MESH)

    @pl.loop(1, n_plane)
    def _(i):
        pl.semaphore_signal(barrier, inc=1, device_id=plane(i), device_id_type=MESH)

    load_data.wait()

    for i in range(nblk):
        r0 = i * BAND
        hi, lo = split(dbuf[r0:r0 + BAND, :].T)
        lt0[0:E, r0:r0 + BAND] = hi
        lt0[E:2 * E, r0:r0 + BAND] = lo

    def put_green(src, i, core):
        r0 = pl.multiple_of(i * BAND, BAND)
        hi, lo = split(src[pl.ds(r0, BAND), :])
        for j in range(CB):
            c0 = pl.multiple_of((2 * j + core) * BAND, BAND)
            ghi[pl.ds(r0, BAND), pl.ds(c0, BAND)] = hi[:, j * BAND:(j + 1) * BAND]
            glo[pl.ds(r0, BAND), pl.ds(c0, BAND)] = lo[:, j * BAND:(j + 1) * BAND]

    @pl.loop(0, RB)
    def _(i):
        load(i).wait()
        put_green(gbuf, 2 * i, c)
        put_green(gbuf, 2 * i + 1, c)

    load_nb.wait()
    load_rw.wait()
    wrow = rw[...]
    weight = jnp.where(mine(1), wrow, roll(wrow))

    ncopy = rcopy(nb, nbp, (sem_nb.at[0], sem_nb.at[1]), at(obs, partner))
    def gcopy(i):
        rs = pl.ds(i * BAND, BAND)
        return rcopy(gbuf.at[rs], gpar.at[rs], (sem_out.at[3], sem_g.at[i // (nblk // 2)]), at(obs, partner))

    def build_laplace():
        ncopy.wait_recv()
        zero_u = jnp.zeros((2 * BAND, 2 * E), BF16)
        cat_u[0:2 * BAND, :] = zero_u
        cat_u[(NB + 2) * BAND:(NB + 4) * BAND, :] = zero_u
        nbe[...] = jnp.full(nbe.shape, -(2 ** 24), jnp.int32)
        base = z * (2 * cols)
        own0 = pl.multiple_of((2 + c * CB) * BAND, BAND)
        par0 = pl.multiple_of((2 + other * CB) * BAND, BAND)
        nbe[0:3, pl.ds(own0, cols)] = nb[...] - base
        nbe[0:3, pl.ds(par0, cols)] = nbp[...] - base
        K = 3 * BAND

        for j in range(NB + 2):
            r0 = j * BAND
            col = lax.broadcasted_iota(jnp.int32, (BAND, K), 0) + (j - 1) * BAND
            own = lax.broadcasted_iota(jnp.int32, (BAND, K), 1) + (j - 2) * BAND
            m = jnp.where(col == own, 4.0, 0.0)
            for k in range(3):
                m = m - jnp.where(col == nbe[k:k + 1, pl.ds(r0, K)], 1.0, 0.0)
            lmt[pl.ds(r0, BAND), :] = m.astype(BF16)

        for b in range(NB):
            r0, n0 = b * BAND, (b + 2) * BAND
            row = lax.broadcasted_iota(jnp.int32, (BAND, K), 0) + b * BAND
            col = lax.broadcasted_iota(jnp.int32, (BAND, K), 1) + (b - 1) * BAND
            m = jnp.where(col == row, 4.0, 0.0)
            t = nbe[0:8, pl.ds(n0, BAND)].T
            for k in range(3):
                m = m - jnp.where(col == t[:, k:k + 1], 1.0, 0.0)
            lm[pl.ds(r0, BAND), :] = m.astype(BF16)

    def clear():
        scs[...] = jnp.zeros((ITERS, 8, E), F32)
        zero_c = jnp.zeros((nc, R, E), F32)
        zero_h = jnp.zeros((HB, E), F32)

        @pl.when(z == 0)
        def _():
            for it in range(ITERS):
                rl[it] = zero_c
                hal[it, 0] = zero_h
            for it in range(ITERS - 1):
                wr[it, 0] = zero_h

        @pl.when(z == nz - 1)
        def _():
            for it in range(ITERS):
                rr[it] = zero_c
                hal[it, 1] = zero_h
            for it in range(ITERS - 1):
                wr[it, 1] = zero_h

    def bit_partner(p, j):
        b0, b1 = 1 << p, 1 << (nbit - 1 - p)
        bit = b0 + (j % 2) * (b1 - b0)
        return at(obs + bit * (1 - 2 * ((obs // bit) % 2)), pat)

    def bcopy(b, p, j):
        return rcopy(bb.at[b, p, j], br.at[b, p, j], (sem_out.at[2], sem_b.at[b % 2, p, j]), bit_partner(p, j))

    def product(b, m):
        if b == 0:
            c0 = pl.multiple_of((2 * m + c) * BAND, BAND)
            y = dot(lt0[...], ghi[:, pl.ds(c0, BAND)])
            y = y[:E] + y[E:] + dot(lt0[0:E, :], glo[:, pl.ds(c0, BAND)])
            return y.T
        c0 = m * 2 * BAND
        if m == 0:
            y = acc_b[...] + part_b(RB - 1)
        else:
            y = dot(lt[...], ghi[:, c0:c0 + 2 * BAND])
            y = y[:H] + y[H:] + dot(lt[0:H, :], glo[:, c0:c0 + 2 * BAND])
        return jnp.concatenate([y[:, :BAND], y[:, BAND:]], axis=0).T

    def xcopy(m):
        return rcopy(nat.at[m], natp.at[m], (sem_out.at[9], sem_x.at[m]), at(obs, partner))

    def enter():
        pl.semaphore_wait(barrier, nz - 1 + n_plane - 1)
        ncopy.start()
        gcopy(0).start()

    def backward(b, hook, late, finish):
        for ms in batches(CB) if b else ([0, 1], range(2, CB)):
            for m in ms:
                y = product(b, m)
                if b == 0:
                    nat[m] = y
                else:
                    bb[b, 0, m * per:(m + 1) * per] = y.reshape(per, R, E)
            if b == 0 and ms[0] == 0:
                enter()
            for m in ms:
                if b == 0:
                    xcopy(m).start()
                else:
                    for k in range(per):
                        bcopy(b, 0, m * per + k).start()

        if b == 0:
            for i in range(1, nblk):
                gcopy(i).start()
            pl.when(c == 0)(build_laplace)
            for m in range(CB):
                xcopy(m).wait_recv()
                y = jnp.where(mine(BAND), nat[m], roll(natp[m]))
                bb[b, 0, m * per:(m + 1) * per] = y.reshape(per, R, E)
                for k in range(per):
                    bcopy(b, 0, m * per + k).start()

        hook()
        for p in range(1, nbit):
            @pl.loop(0, bc)
            def _(j):
                bcopy(b, p - 1, j).wait_recv()
                bb[b, p, j] = bb[b, p - 1, j] + br[b, p - 1, j]
                bcopy(b, p, j).start()

        acc_f[...] = jnp.zeros(acc_f.shape, F32)
        late()

        @pl.loop(0, bc)
        def _(j):
            bcopy(b, nbit - 1, j).wait_recv()
            finish(j, bb[b, nbit - 1, j] + br[b, nbit - 1, j])

    def backward_sent(b):
        rcopy(bb.at[b], br.at[b], (sem_out.at[2], sem_b.at[0, 0, 0]), at(obs, partner)).wait_send()

    def rcopy_up(it, src, k):
        return rcopy(src.at[k], rl.at[it, k], (sem_out.at[0], sem_l.at[it % 2, k]), at(obs, pat + 2))

    def rcopy_down(it, src, k):
        return rcopy(src.at[k], rr.at[it, k], (sem_out.at[1], sem_r.at[it % 2, k]), at(obs, pat - 2))

    def hcopy_r(it):
        return rcopy(hsrc.at[it, 0], hal.at[it, 0], (sem_out.at[4], sem_h.at[it % 2, 0]), at(obs, pat + 2))

    def hcopy_l(it):
        return rcopy(hsrc.at[it, 1], hal.at[it, 1], (sem_out.at[5], sem_h.at[it % 2, 1]), at(obs, pat - 2))

    def part_b(m):
        ks = pl.ds(pl.multiple_of(m * 2 * BAND, 2 * BAND), 2 * BAND)
        y = dot(lt[:, ks], ghi[ks, 0:2 * BAND])
        return y[:H] + y[H:] + dot(lt[0:H, ks], glo[ks, 0:2 * BAND])

    def put_lt(m):
        x = qd[pl.ds(m * per, per)].reshape(BAND, E)
        hi, lo = split(x.T)
        o0 = pl.multiple_of(m * 2 * BAND, 2 * BAND)
        o1 = pl.multiple_of(m * 2 * BAND + BAND, BAND)
        lt[0:H, pl.ds(o0, BAND)] = hi[:H]
        lt[H:E, pl.ds(o0, BAND)] = lo[:H]
        lt[0:H, pl.ds(o1, BAND)] = hi[H:]
        lt[H:E, pl.ds(o1, BAND)] = lo[H:]

        @pl.when(m < RB - 1)
        def _():
            acc_b[...] += part_b(m)

    def part_f(it, i):
        m = jnp.where((it == ITERS - 1) & (z <= za), RB - 1, 0) if it == ITERS - 1 else 0
        rs = pl.ds(pl.multiple_of(m * 2 * BAND, 2 * BAND), 2 * BAND) if it == ITERS - 1 else slice(0, 2 * BAND)
        ks = pl.ds(pl.multiple_of(i * 2 * BAND, 2 * BAND), 2 * BAND)
        y = dot(ghi[rs, ks], cat_d[ks, 0:2 * E])
        return y[:, :E] + y[:, E:] + dot(glo[rs, ks], cat_d[ks, 2 * E:3 * E])

    def forward(it, sums, after, hook):
        last = it == ITERS - 1
        v = a if it else g
        x = v[cols - BAND:cols, :]
        hsrc[it, 0] = jnp.where(low(HB), roll(x[:HB]), x[HB:])
        x = v[0:BAND, :]
        hsrc[it, 1] = jnp.where(low(HB), x[:HB], roll(x[HB:]))

        @pl.when(up & down)
        def _():
            hcopy_r(it).start()
            hcopy_l(it).start()

        if last:
            forward_last(sums, hook)
            return

        acc_b[...] = jnp.zeros(acc_b.shape, F32)

        def group(m):
            r0 = m * 2 * BAND
            if m == 0:
                y = acc_f[...] + part_f(it, CB - 1)
            else:
                y = dot(ghi[r0:r0 + 2 * BAND, :], cat_d[:, 0:2 * E])
                y = y[:, :E] + y[:, E:] + dot(glo[r0:r0 + 2 * BAND, :], cat_d[:, 2 * E:3 * E])
            y = jnp.where(low(BAND), y[:BAND], y[BAND:])
            s[m * per:(m + 1) * per] = y.reshape(per, R, E)

        def send(ms):
            @pl.when(z == 0)
            def _():
                for k in range(ms[0] * per, (ms[-1] + 1) * per):
                    rcopy_up(it, s, k).start()

            @pl.when(z == nz - 1)
            def _():
                for k in range(ms[0] * per, (ms[-1] + 1) * per):
                    rcopy_down(it, s, k).start()

        group(0)
        send([0])
        sums()

        @pl.when(up & (z == 0))
        def _():
            hcopy_r(it).start()

        @pl.when(down & (z == nz - 1))
        def _():
            hcopy_l(it).start()

        for ms in batches(RB)[1:]:
            for m in ms:
                group(m)
            send(ms)
        after()
        backward_sent(it)

        def chain(t, ends=True):
            kl = t - LAG * z
            kr = t - LAG * (nz - 1 - z)
            kt = t - LAG * jnp.maximum(z, nz - 1 - z)

            @pl.when(down & (kl >= 0) & (kl < nc))
            def _():
                rcopy_up(it, sr, kl).wait_recv()

                @pl.when(up)
                def _():
                    sr[kl] = rl[it, kl] + s[kl]
                    rcopy_up(it, sr, kl).start()

            @pl.when(up & (kr >= 0) & (kr < nc))
            def _():
                rcopy_down(it, sl, kr).wait_recv()

                @pl.when(down)
                def _():
                    sl[kr] = rr[it, kr] + s[kr]
                    rcopy_down(it, sl, kr).start()

            if not ends:
                return

            @pl.when((kt >= 0) & (kt < nc))
            def _():
                total = rl[it, kt] + s[kt] + rr[it, kt]
                if it:
                    step, ratio = scalars
                    rest = qg[kt] - step * total
                    total = rest + ratio * qd[kt]
                qg[kt] = rest if it else total
                qd[kt] = total

                @pl.when(kt % per == per - 1)
                def _():
                    put_lt(kt // per)

        pl.loop(LAG, LAG * (nz // 2))(functools.partial(chain, ends=False))
        scalars = hook()

        @pl.when(jnp.logical_not(inner))
        def _():
            reg_work(it)

        pl.loop(LAG * (nz // 2), nc + LAG * (nz - 1))(chain)

    def forward_last(sums, hook):
        it = ITERS - 1
        low_side = z <= za

        def order(i, n):
            return jnp.where(low_side, n - 1 - i, i)

        def group(i):
            m = order(i, RB)
            rs = pl.ds(pl.multiple_of(m * 2 * BAND, 2 * BAND), 2 * BAND)
            if i == 0:
                y = acc_f[...] + part_f(it, CB - 1)
            else:
                y = dot(ghi[rs, :], cat_d[:, 0:2 * E])
                y = y[:, :E] + y[:, E:] + dot(glo[rs, :], cat_d[:, 2 * E:3 * E])
            y = jnp.where(low(BAND), y[:BAND], y[BAND:])
            s[pl.ds(m * per, per)] = y.reshape(per, R, E)

        def send(ms):
            for i in range(ms[0] * per, (ms[-1] + 1) * per):
                k = order(i, nc)

                @pl.when((z == 0) & ((z < za) | (k >= nc // 2)))
                def _():
                    rcopy_up(it, s, k).start()

                @pl.when((z == nz - 1) & ((z > zb) | (k < nc // 2)))
                def _():
                    rcopy_down(it, s, k).start()

        group(0)
        send([0])
        first, *others = batches(RB)[1:]
        for i in first:
            group(i)
        send(first)
        sums()

        @pl.when(up & (z == 0))
        def _():
            hcopy_r(it).start()

        @pl.when(down & (z == nz - 1))
        def _():
            hcopy_l(it).start()

        for ms in others:
            for i in ms:
                group(i)
            send(ms)
        backward_sent(it)
        sq[...] = jnp.zeros((8, E), F32)

        def move(n0, n1):
            @pl.loop(n0, n1)
            def _(i):
                k = order(i, nc)

                @pl.when(low_side & down)
                def _():
                    rcopy_up(it, sr, k).wait_recv()

                    @pl.when((z < za) | (k >= nc // 2))
                    def _():
                        sr[k] = rl[it, k] + s[k]
                        rcopy_up(it, sr, k).start()

                @pl.when(jnp.logical_not(low_side) & up)
                def _():
                    rcopy_down(it, sl, k).wait_recv()

                    @pl.when((z > zb) | (k < nc // 2))
                    def _():
                        sl[k] = rr[it, k] + s[k]
                        rcopy_down(it, sl, k).start()

        half = nc - nc // 2
        move(0, half)
        step, ratio = hook()
        move(half, nc)

        def ends(k):
            total = rl[it, k] + s[k] + rr[it, k]
            total = qg[k] - step * total + ratio * qd[k]
            sq[...] += jnp.sum((total * total).reshape(R // 8, 8, E), axis=0)

        @pl.when(z == za)
        def _():
            @pl.loop(0, nc // 2)
            def _(k):
                rcopy_down(it, sl, k).wait_recv()
                ends(k)

        @pl.when(z == zb)
        def _():
            @pl.loop(nc // 2, nc)
            def _(k):
                rcopy_up(it, sr, k).wait_recv()
                ends(k)

    def last_sent():
        it = ITERS - 1

        def wait(buf, sem, n):
            part = buf.at[pl.ds(0, n)]
            rcopy(part, part, (sem, sem_p.at[2]), at(obs, partner)).wait_send()

        @pl.when(z < za)
        def _():
            wait(sr, sem_out.at[0], nc)

        @pl.when(z == za)
        def _():
            wait(sr, sem_out.at[0], nc - nc // 2)

        @pl.when(z == zb)
        def _():
            wait(sl, sem_out.at[1], nc // 2)

        @pl.when(z > zb)
        def _():
            wait(sl, sem_out.at[1], nc)

        @pl.when(up)
        def _():
            hcopy_r(it).wait_send()

        @pl.when(down)
        def _():
            hcopy_l(it).wait_send()

    def forward_sent(it):
        @pl.when(up)
        def _():
            rcopy(sr, rl.at[it], (sem_out.at[0], sem_l.at[0, 0]), at(obs, partner)).wait_send()

        @pl.when(down)
        def _():
            rcopy(sl, rr.at[it], (sem_out.at[1], sem_r.at[0, 0]), at(obs, partner)).wait_send()

        @pl.when(up)
        def _():
            hcopy_r(it).wait_send()

        @pl.when(down)
        def _():
            hcopy_l(it).wait_send()

    def halo_wait(it):
        @pl.when(has_l)
        def _():
            hcopy_r(it).wait_recv()

        @pl.when(has_r)
        def _():
            hcopy_l(it).wait_recv()

    def widen(x):
        top, bot = both(x)
        return jnp.concatenate([top, bot], axis=0)

    def laplace():
        put_cat(cat_e, 0, widen(hd[0]))
        put_cat(cat_e, (NB + 1) * BAND, widen(hd[1]))

        for i in range(CB):
            top, bot = both(d[i * BAND:(i + 1) * BAND, :])
            put_cat(cat_e, (i + 1) * BAND, top)
            put_cat(cat_e, (CB + i + 1) * BAND, bot)

    def banded(mat, vec, j):
        r0 = j * BAND
        y = dot(mat[r0:r0 + BAND, :], vec[r0:r0 + 3 * BAND, :])
        return y[:, :E] + y[:, E:]

    def lap_rows(i):
        return weight * jnp.where(low(BAND), banded(lm, cat_e, i), banded(lm, cat_e, CB + i))

    def wcopy_l(it):
        return rcopy(wsrc.at[it, 0], wr.at[it, 1], (sem_out.at[7], sem_w.at[it, 1]), at(obs, pat - 2))

    def wcopy_r(it):
        return rcopy(wsrc.at[it, 1], wr.at[it, 0], (sem_out.at[6], sem_w.at[it, 0]), at(obs, pat + 2))

    def reg_work(it):
        laplace()

        for i in range(CB):
            top, bot = both(lap_rows(i))
            put_cat(cat_u, (i + 2) * BAND, top)
            put_cat(cat_u, (CB + i + 2) * BAND, bot)

        for side, j in ((0, 0), (1, NB + 1)):
            y = banded(lmt, cat_u, j)
            wsrc[it, side] = weight * jnp.where(low(HB), y[:HB], y[HB:])

        @pl.when(has_l)
        def _():
            wcopy_l(it).start()

        @pl.when(has_r)
        def _():
            wcopy_r(it).start()

        for i in range(CB):
            y = jnp.where(low(BAND), banded(lmt, cat_u, i + 1), banded(lmt, cat_u, CB + i + 1))
            wown[i * BAND:(i + 1) * BAND, :] = weight * y

    def reg_sums():
        last = ITERS - 1
        laplace()
        for i in range(CB):
            u = lap_rows(i)
            scs[last] += jnp.sum((u * u).reshape(BAND // 8, 8, E), axis=0)
        sums_start(last)

    def reg_end(it):
        @pl.when(has_l)
        def _():
            wcopy_r(it).wait_recv()

        @pl.when(has_r)
        def _():
            wcopy_l(it).wait_recv()

        wown[0:BAND, :] += jnp.where(low(BAND), widen(wr[it, 0]), 0.0)
        wown[cols - BAND:cols, :] += jnp.where(low(BAND), 0.0, widen(wr[it, 1]))
        reg_sent(it)

    def reg_sent(it):
        @pl.when(has_l)
        def _():
            wcopy_l(it).wait_send()

        @pl.when(has_r)
        def _():
            wcopy_r(it).wait_send()

    def scopy(it, q):
        return rcopy(scs.at[it], scr.at[it, z], (sem_out.at[8], sem_s.at[it]), at(obs, q * 2 + c))

    def sums_all(it):
        part = scr.at[it, pl.ds(0, nz - 1)]
        return rcopy(part, part, (sem_out.at[8], sem_s.at[it]), at(obs, partner))

    def sums_start(it):
        scr[it, z] = scs[it]

        @pl.loop(1, nz)
        def _(i):
            scopy(it, zpeer(i)).start()

    def sums_end(it):
        sums_all(it).wait_recv()
        sums_all(it).wait_send()
        return fold(jnp.sum(scr[it], axis=0))

    def pcopy(i):
        po, pp = plane(i)
        return rcopy(pls, plr.at[obs * 2 + c], (sem_p.at[0], sem_p.at[1]), (po, pp))

    norms = []

    def dots(it):
        gv, dv, av = g[...], d[...], a[...]
        scs[it, 0:1, :] = rowsum(gv * gv)
        scs[it, 1:2, :] = rowsum(dv * av)
        scs[it, 2:3, :] = rowsum(gv * av)
        scs[it, 3:4, :] = rowsum(av * av)
        sums_start(it)

    def first():
        halo_wait(0)
        hg[...] = hal[0]
        hd[...] = hal[0]

    def ycopy(i):
        return rcopy((slip, d)[i], (slp, dp)[i], pair(sem_y, i), at(obs, partner))

    tcopy = rcopy(tsrc, tdst, pair(sem_y, 2), at(obs, partner))

    def advance(it):
        tot = sums_end(it - 1)
        if it == 1:
            norms.append(tot[0:1])
        norm = norms[-1]
        step = norm / tot[1:2]
        after = norm - 2.0 * step * tot[2:3] + step * step * tot[3:4]
        ratio = after / norm
        norms.append(after)
        halo_wait(it)
        if it == 1:
            slip[...] = step * d[...]
        else:
            slip[...] += step * d[...]
        g[...] = g[...] - step * a[...]
        d[...] = g[...] + ratio * d[...]
        hg[...] = hg[...] - step * hal[it]
        hd[...] = hg[...] + ratio * hd[...]
        if it == ITERS - 1:
            ycopy(0).start()
            ycopy(1).start()
        return step, ratio

    def first_hook():
        clear()

    def first_late():
        for h in range(2):
            rs = pl.ds(h * (rows // 2), rows // 2)
            rcopy(gbuf.at[rs], gpar.at[rs], (sem_out.at[3], sem_g.at[h]), at(obs, partner)).wait_recv()

            @pl.loop(h * nblk // 2, (h + 1) * nblk // 2)
            def _(i):
                put_green(gpar, i, other)

    def put_operand(ref, i, it):
        top, bot = both(ref[pl.ds(pl.multiple_of(i * BAND, BAND), BAND), :])
        r0 = pl.multiple_of(i * 2 * BAND, 2 * BAND)
        put_cat(cat_d, r0, top, True)
        put_cat(cat_d, pl.multiple_of(r0 + BAND, BAND), bot, True)

        @pl.when(i < CB - 1)
        def _():
            acc_f[...] += part_f(it, i)

    def first_finish(j, x):
        r0 = pl.multiple_of(j * R, R)
        g[pl.ds(r0, R), :] = x
        d[pl.ds(r0, R), :] = x

        @pl.when(j % per == per - 1)
        def _():
            put_operand(g, j // per, 0)

    backward(0, first_hook, first_late, first_finish)
    forward(0, lambda: None, lambda: pl.when(c == 1)(build_laplace), first)
    for it in range(1, ITERS):
        def hook(it=it):
            forward_sent(it - 1)

            @pl.when(inner)
            def _():
                reg_work(it - 1)

        def finish(j, x, it=it):
            r0 = pl.multiple_of(j * R, R)
            a[pl.ds(r0, R), :] = x + wown[pl.ds(r0, R), :]

            @pl.when(j % per == per - 1)
            def _():
                put_operand(a, j // per, it)

        backward(it, hook, functools.partial(reg_end, it - 1), finish)
        forward(it, functools.partial(dots, it - 1), lambda: None, functools.partial(advance, it))

    last = ITERS - 1
    norm = norms[-1]
    mid = (z == za) | (z == zb)

    def zcopy(i):
        q = zpeer(i)
        return rcopy(sq, zsq.at[z - za], (sem_zs.at[0], sem_p.at[2 + z - za]), at(obs, q * 2 + c))

    def zwait(slot):
        rcopy(sq, zsq.at[slot], (sem_zs.at[0], sem_p.at[2 + slot]), at(obs, partner)).wait_recv()

    @pl.when(mid)
    def _():
        zsq[z - za] = sq[...]

        @pl.loop(1, nz)
        def _(i):
            zcopy(i).start()

    reg_sums()

    @pl.when(z != za)
    def _():
        zwait(0)

    @pl.when(z != zb)
    def _():
        zwait(1)

    pls[...] = zsq[0] + zsq[1]
    plr[obs * 2 + c] = pls[...]

    @pl.loop(1, n_plane)
    def _(i):
        pcopy(i).start()

    tsrc[0:1, :] = norm
    tsrc[1:2, :] = rowsum(sums_end(last))
    tcopy.start()

    last_sent()

    @pl.when(mid)
    def _():
        part = scr.at[last, pl.ds(0, nz - 1)]
        rcopy(part, part, (sem_zs.at[0], sem_p.at[2]), at(obs, partner)).wait_send()

    ncopy.wait_send()
    rcopy(gbuf, gpar, (sem_out.at[3], sem_g.at[0]), at(obs, partner)).wait_send()
    rcopy(nat, natp, (sem_out.at[9], sem_x.at[0]), at(obs, partner)).wait_send()
    ycopy(0).wait_recv()
    ycopy(1).wait_recv()
    ycopy(0).wait_send()
    ycopy(1).wait_send()
    for i in range(CB):
        blk = slice(i * BAND, (i + 1) * BAND)
        m = mine(BAND)
        slip[blk, :] = jnp.where(m, slip[blk, :], roll(slp[blk, :]))
        d[blk, :] = jnp.where(m, d[blk, :], roll(dp[blk, :]))
    tcopy.wait_recv()
    tcopy.wait_send()

    part = plr.at[pl.ds(0, n_plane - 1)]
    rcopy(part, part, (sem_p.at[0], sem_p.at[1]), at(obs, partner)).wait_recv()

    def step_of(t, q):
        return t[0:1, :] / (fold(sum(rowsum(plr[2 * o + q]) for o in range(n_obs))) + t[1:2, :])

    step = jnp.where(mine(1), step_of(tsrc, c), step_of(tdst, other))

    out[...] = slip[...] + step * d[...]

    rcopy(part, part, (sem_p.at[0], sem_p.at[1]), at(obs, partner)).wait_send()


def shards(green, data, neighbours, reg_weight):
    rows, cols = green.shape
    E = data.shape[1]
    n_obs, n_patch = lax.axis_size("obs"), lax.axis_size("patch")
    nbit = n_obs.bit_length() - 1
    nz = n_patch // 2
    nc, bc = rows // 2 // R, cols // R
    NB = 2 * cols // BAND
    nblk = rows // BAND
    V = pltpu.VMEM
    D = pltpu.SemaphoreType.DMA
    scratch = [
        V((rows, cols), F32), V((rows, cols), F32), V((rows, E), F32),
        V((rows, 2 * cols), BF16), V((rows, 2 * cols), BF16),
        V(neighbours.shape, jnp.int32), V(neighbours.shape, jnp.int32), V((8, (NB + 4) * BAND), jnp.int32), V((1, E), F32),
        V((NB * BAND, 3 * BAND), BF16), V(((NB + 2) * BAND, 3 * BAND), BF16),
        V((2 * cols, 3 * E), BF16), V(((NB + 2) * BAND, 2 * E), BF16), V(((NB + 4) * BAND, 2 * E), BF16),
        V((E, rows), BF16), V((2 * E, rows), BF16),
        V((cols, E), F32), V((cols, E), F32), V((cols, E), F32), V((cols, E), F32), V((ITERS - 1, 2, HB, E), F32),
        V((cols, E), F32), V((cols, E), F32), V((cols, E), F32), V((8, E), F32),
        V((ITERS, 2, HB, E), F32), V((2, HB, E), F32), V((2, HB, E), F32), V((nc, R, E), F32), V((nc, R, E), F32),
        V((nc, R, E), F32), V((nc, R, E), F32), V((nc, R, E), F32),
        V((ITERS, nc, R, E), F32), V((ITERS, nc, R, E), F32),
        V((ITERS, nbit, bc, R, E), F32), V((ITERS, nbit, bc, R, E), F32),
        V((cols // BAND, BAND, E), F32), V((cols // BAND, BAND, E), F32),
        V((ITERS, 2, HB, E), F32), V((ITERS - 1, 2, HB, E), F32),
        V((ITERS, 8, E), F32), V((ITERS, nz, 8, E), F32),
        V((2, 8, E), F32), V((8, E), F32), V((2 * n_obs, 8, E), F32), V((8, E), F32), V((8, E), F32),
        V((2 * BAND, E), F32), V((E // 2, 2 * BAND), F32),
        D((10,)), D((2, nc)), D((2, nc)), D((2, nbit, bc)), D((2, 2)), D((ITERS - 1, 2)),
        D((ITERS,)), D((4,)), D((cols // BAND,)), D((2, 3)), D((2,)), D((2,)), D((rows // (2 * BAND) + 3,)), D((1,)),
    ]
    return pl.pallas_call(
        functools.partial(kernel, n_obs, n_patch, nc, bc),
        out_shape=pltpu.VMEM((cols, E), F32),
        in_specs=[pl.BlockSpec(memory_space=pl.ANY)] * 4,
        out_specs=pl.BlockSpec(memory_space=pltpu.VMEM),
        scratch_shapes=scratch,
        compiler_params=pltpu.CompilerParams(
            collective_id=0, has_side_effects=True, vmem_limit_bytes=56 * 1024 * 1024),
    )(green, data, neighbours, reg_weight.reshape(1, E))


def solution(mesh):
    in_specs = (P("obs", "patch"), P("obs", None), P(None, "patch"), P())
    return jax.shard_map(shards, mesh=mesh, in_specs=in_specs, out_specs=P("patch", None), check_vma=False)
```
